768 devices in a mesh: stream: 16 (over y_hi, x, core), cross: 48 (over z, y_lo).
Axes of the slice: x: 4, y: 8 (y_hi: 2, y_lo: 4; y = y_hi * 4 + y_lo), z: 12, core: 2. Of those that a mesh axis runs over, the one named last changes fastest.
Arguments:
- state_now: float32 [7, 8, 384, 2048], P(None, None, 'cross', 'stream'), as said below
- state_base: float32 [7, 8, 384, 2048], P(None, None, 'cross', 'stream'), as said below
- inflow: float32 [7, 8, 384, 3], P(None, None, 'cross'), as said below
Outputs:
- state_next: float32 [7, 8, 384, 2048], P(None, None, 'cross', 'stream')
Inputs may be any that keep to these rules, and one draw needn't show every extreme that they name: `state_now`: partial densities and volume fractions are positive, volume fractions below 1, and the pressure that each cell implies is positive. `state_base`: partial densities and volume fractions are positive, volume fractions below 1, and the pressure that each cell implies is positive. `inflow`: partial densities and volume fractions are positive, volume fractions below 1, and the pressure that each cell implies is positive.
All inputs are finite; a program needn't handle non-finite values.
Results may differ from the reference program's by a relative error of at most 0.0003.
Values sent between devices are 32-bit elements; how exact they have to be, the bound alone decides.
A program may use at most 32 MiB of HBM per device.

```python
import jax
import jax.numpy as jnp
from jax import lax

CZ = 8
NX = 2048
NY = 384


gas_gamma = 1.4


liquid_gamma = 4.4


liquid_stiff = 0.6


def field_cells(key, streamwise):
    subkeys = jax.random.split(key, 7)
    grid_shape = streamwise.shape
    lower_end = 0.5
    upper_end = 2.0
    volume = jax.random.uniform(subkeys[2], grid_shape, jnp.float32, 0.1, 0.9)

    def rough_field(subkey):
        return jnp.exp(jax.random.uniform(subkey, grid_shape, jnp.float32, jnp.log(lower_end), jnp.log(upper_end)))
    dens_gas = rough_field(subkeys[0])
    dens_liquid = 4.0 * rough_field(subkeys[1])
    stream_vel = (0.4 + 6.0 * streamwise) * jax.random.uniform(subkeys[3], grid_shape, jnp.float32, 0.8, 1.2)
    cross_vel = jax.random.uniform(subkeys[4], grid_shape, jnp.float32, -0.8, 0.8)
    span_vel = jax.random.uniform(subkeys[5], grid_shape, jnp.float32, -0.8, 0.8)
    pressure = rough_field(subkeys[6])
    partial_gas = volume * dens_gas
    partial_liquid = (1.0 - volume) * dens_liquid
    density = partial_gas + partial_liquid
    stiff_gamma = volume / (gas_gamma - 1.0) + (1.0 - volume) / (liquid_gamma - 1.0)
    stiff_term = (1.0 - volume) * liquid_gamma * liquid_stiff / (liquid_gamma - 1.0)
    energy = stiff_gamma * pressure + stiff_term + 0.5 * density * (stream_vel * stream_vel + cross_vel * cross_vel + span_vel * span_vel)
    return jnp.stack([partial_gas, partial_liquid, density * stream_vel, density * cross_vel, density * span_vel, energy, volume])


def grid_positions():
    positions = (jnp.arange(NX, dtype=jnp.float32) + 0.5) / NX
    return jnp.broadcast_to(positions, (CZ, NY, NX))


def draw_state_now(key, part):
    return field_cells(jax.random.fold_in(key, 11), grid_positions())


def draw_state_base(key, part):
    return field_cells(jax.random.fold_in(key, 23), grid_positions())


def draw_inflow(key, part):
    return field_cells(jax.random.fold_in(key, 37), jnp.ones((CZ, NY, 3), jnp.float32))


def setup_inputs(seed: int = 0) -> dict:
    key_list = jax.random.split(jax.random.key(seed), 4)
    return {
        "state_now": draw_state_now(jax.random.fold_in(key_list[3], 71), 0),
        "state_base": draw_state_base(jax.random.fold_in(key_list[3], 71), 0),
        "inflow": draw_inflow(jax.random.fold_in(key_list[3], 71), 0),
    }


gas_gamma = 1.4
liquid_gamma = 4.4
liquid_stiff = 0.6
courant = 0.3
weno_epsilon = 1e-06

def mixture(volume):
    stiff_gamma = volume / (gas_gamma - 1.0) + (1.0 - volume) / (liquid_gamma - 1.0)
    stiff_term = (1.0 - volume) * liquid_gamma * liquid_stiff / (liquid_gamma - 1.0)
    return (stiff_gamma, stiff_term)

def primitive(conserved):
    density = conserved[0] + conserved[1]
    vel_one = conserved[2] / density
    vel_two = conserved[3] / density
    vel_three = conserved[4] / density
    kinetic = 0.5 * (conserved[2] * vel_one + conserved[3] * vel_two + conserved[4] * vel_three)
    stiff_gamma, stiff_term = mixture(conserved[6])
    pressure = (conserved[5] - kinetic - stiff_term) / stiff_gamma
    return jnp.stack([conserved[0], conserved[1], vel_one, vel_two, vel_three, pressure, conserved[6]])

def sound(primitives):
    density = primitives[0] + primitives[1]
    stiff_gamma, stiff_term = mixture(primitives[6])
    return jnp.sqrt(((stiff_gamma + 1.0) * primitives[5] + stiff_term) / (stiff_gamma * density))

def max_speed(conserved):
    primitives = primitive(conserved)
    fastest = jnp.maximum(jnp.maximum(jnp.abs(primitives[2]), jnp.abs(primitives[3])), jnp.abs(primitives[4]))
    return jnp.max(fastest + sound(primitives))

def weno_face(far_left, near_left, centre, near_right, far_right):
    first_low = far_left - 2.0 * near_left + centre
    second_low = far_left - 4.0 * near_left + 3.0 * centre
    first_mid = near_left - 2.0 * centre + near_right
    second_mid = near_left - near_right
    first_high = centre - 2.0 * near_right + far_right
    second_high = 3.0 * centre - 4.0 * near_right + far_right
    smooth_low = weno_epsilon + 13.0 / 12.0 * first_low * first_low + 0.25 * second_low * second_low
    smooth_mid = weno_epsilon + 13.0 / 12.0 * first_mid * first_mid + 0.25 * second_mid * second_mid
    smooth_high = weno_epsilon + 13.0 / 12.0 * first_high * first_high + 0.25 * second_high * second_high
    weight_low = 0.1 / (smooth_low * smooth_low)
    weight_mid = 0.6 / (smooth_mid * smooth_mid)
    weight_high = 0.3 / (smooth_high * smooth_high)
    guess_low = (2.0 * far_left - 7.0 * near_left + 11.0 * centre) / 6.0
    guess_mid = (-near_left + 5.0 * centre + 2.0 * near_right) / 6.0
    guess_high = (2.0 * centre + 5.0 * near_right - far_right) / 6.0
    return (weight_low * guess_low + weight_mid * guess_mid + weight_high * guess_high) / (weight_low + weight_mid + weight_high)

def clamp_face(state, lower_cell, upper_cell):
    smaller = jnp.minimum(lower_cell, upper_cell)
    larger = jnp.maximum(lower_cell, upper_cell)
    limited = []
    for component in range(7):
        face_value = state[component]
        if component in (0, 1, 5):
            face_value = jnp.maximum(face_value, 0.5 * smaller[component])
        elif component == 6:
            face_value = jnp.clip(face_value, 0.5 * smaller[6], 1.0 - 0.5 * (1.0 - larger[6]))
        limited.append(face_value)
    return jnp.stack(limited)

def side_terms(primitives, normal):
    density = primitives[0] + primitives[1]
    stiff_gamma, stiff_term = mixture(primitives[6])
    velocity = [primitives[2], primitives[3], primitives[4]]
    energy = stiff_gamma * primitives[5] + stiff_term + 0.5 * density * (velocity[0] * velocity[0] + velocity[1] * velocity[1] + velocity[2] * velocity[2])
    normal_vel = velocity[normal]
    amounts = jnp.stack([primitives[0], primitives[1], density * velocity[0], density * velocity[1], density * velocity[2], energy, primitives[6]])
    momentum = []
    for component in range(3):
        moved = density * velocity[component] * normal_vel
        if component == normal:
            moved = moved + primitives[5]
        momentum.append(moved)
    transport = jnp.stack([primitives[0] * normal_vel, primitives[1] * normal_vel, momentum[0], momentum[1], momentum[2], (energy + primitives[5]) * normal_vel, primitives[6] * normal_vel])
    signal = jnp.abs(normal_vel) + sound(primitives)
    return (amounts, transport, normal_vel, signal)

def face_flux(left_state, right_state, normal):
    amount_left, transport_left, normal_left, signal_left = side_terms(left_state, normal)
    amount_right, transport_right, normal_right, signal_right = side_terms(right_state, normal)
    fastest = jnp.maximum(signal_left, signal_right)
    face_fluxes = 0.5 * (transport_left + transport_right) - 0.5 * fastest * (amount_right - amount_left)
    return (face_fluxes, 0.5 * (normal_left + normal_right))

def direction_sweep(padded, dimension, normal):
    primitives = primitive(padded)
    length = padded.shape[dimension] - 6
    pieces = [lax.slice_in_dim(primitives, offset, offset + length + 1, axis=dimension) for offset in range(6)]
    left_state = clamp_face(weno_face(pieces[0], pieces[1], pieces[2], pieces[3], pieces[4]), pieces[2], pieces[3])
    right_state = clamp_face(weno_face(pieces[5], pieces[4], pieces[3], pieces[2], pieces[1]), pieces[2], pieces[3])
    face_fluxes, face_motion = face_flux(left_state, right_state, normal)
    change = lax.slice_in_dim(face_fluxes, 1, length + 1, axis=dimension) - lax.slice_in_dim(face_fluxes, 0, length, axis=dimension)
    spread = lax.slice_in_dim(face_motion, 1, length + 1, axis=dimension - 1) - lax.slice_in_dim(face_motion, 0, length, axis=dimension - 1)
    return (change, spread)

def tendency(stream_cells, cross_cells, span_cells, centre_cells):
    change_stream, spread_stream = direction_sweep(stream_cells, 3, 0)
    change_cross, spread_cross = direction_sweep(cross_cells, 2, 1)
    change_span, spread_span = direction_sweep(span_cells, 1, 2)
    total = -(change_stream + change_cross + change_span)
    source = centre_cells[6] * (spread_stream + spread_cross + spread_span)
    return jnp.concatenate([total[:6], (total[6] + source)[None]], axis=0)

def reference(state_now, state_base, inflow):

    def plane_max(plane_index):
        return max_speed(lax.dynamic_slice_in_dim(state_base, plane_index, 1, 1))
    fastest = jnp.max(lax.map(plane_max, jnp.arange(CZ, dtype=jnp.int32)))
    time_step = courant / fastest
    last_cells = jnp.repeat(state_now[:, :, :, -1:], 3, axis=3)
    stream_padded = jnp.concatenate([inflow, state_now, last_cells], axis=3)
    cross_padded = jnp.concatenate([stream_padded[:, :, -3:], stream_padded, stream_padded[:, :, :3]], axis=2)
    padded = jnp.concatenate([cross_padded[:, -3:], cross_padded, cross_padded[:, :3]], axis=1)

    def one_plane(plane_index):
        span_cells = lax.dynamic_slice_in_dim(padded, plane_index, 7, 1)[:, :, 3:-3, 3:-3]
        middle = lax.dynamic_slice_in_dim(padded, plane_index + 3, 1, 1)
        cross_cells = middle[:, :, :, 3:-3]
        stream_cells = middle[:, :, 3:-3, :]
        centre_cells = middle[:, :, 3:-3, 3:-3]
        changes = tendency(stream_cells, cross_cells, span_cells, centre_cells)
        base_plane = lax.dynamic_slice_in_dim(state_base, plane_index, 1, 1)
        updated = base_plane / 3.0 + 2.0 / 3.0 * (centre_cells + time_step * changes)
        return updated[:, 0]
    planes = lax.map(one_plane, jnp.arange(CZ, dtype=jnp.int32))
    return jnp.transpose(planes, (1, 0, 2, 3))
```

```python
import functools

import jax
import jax.numpy as jnp
from jax import lax
from jax.experimental import pallas as pl
from jax.experimental.pallas import tpu as pltpu
from jax.sharding import PartitionSpec as P

MESH = pl.DeviceIdType.MESH

gas_part = 1.0 / 0.4
liquid_part = 1.0 / 3.4
stiff_part = 4.4 * 0.6 / 3.4


def inverse(value):
    guess = pl.reciprocal(value, approx=True)
    return guess * (2.0 - value * guess)


def mixture(volume):
    rest = 1.0 - volume
    return (volume * gas_part + rest * liquid_part, rest * stiff_part)


def primitive(u):
    over = 1.0 / (u[0] + u[1])
    vx, vy, vz = (u[2] * over, u[3] * over, u[4] * over)
    kinetic = 0.5 * (u[2] * vx + u[3] * vy + u[4] * vz)
    gamma, stiff = mixture(u[6])
    return (u[0], u[1], vx, vy, vz, (u[5] - kinetic - stiff) / gamma, u[6])


def sound(density, pressure, gamma, stiff):
    return jnp.sqrt(((gamma + 1.0) * pressure + stiff) / (gamma * density))


def edges(h, d1, d2, d3, d4):
    e1, e2, e3 = (d2 - d1, d3 - d2, d4 - d3)
    u0 = e1 + d2 + d2
    u1 = d2 + d3
    u2 = e3 - d3 - d3
    third = 13.0 / 3.0
    top = 1e30
    s0 = jnp.minimum(third * (e1 * e1) + u0 * u0 + 4e-6, top)
    s1 = jnp.minimum(third * (e2 * e2) + u1 * u1 + 4e-6, top)
    s2 = jnp.minimum(third * (e3 * e3) + u2 * u2 + 4e-6, top)
    r0, r1, r2 = (inverse(s0), inverse(s1), inverse(s2))
    a0, a1, a2 = (r0 * r0, 6.0 * (r1 * r1), r2 * r2)
    b0, b2 = (3.0 * a0, 3.0 * a2)
    up = a0 * (u0 + e1 + d2) + a1 * (u1 + d3) + b2 * (d3 - u2)
    down = a2 * (u2 + e3 - d3) - a1 * (u1 + d2) - b0 * (u0 + d2)
    upper = h + up * inverse(6.0 * (a0 + a1 + b2))
    lower = h + down * inverse(6.0 * (a2 + a1 + b0))
    return (upper, lower)


def limited(face, lower_cell, upper_cell):
    out = []
    for c in range(7):
        value = face[c]
        if c in (0, 1, 5):
            value = jnp.maximum(value, 0.5 * jnp.minimum(lower_cell[c], upper_cell[c]))
        elif c == 6:
            value = jnp.maximum(value, 0.5 * jnp.minimum(lower_cell[c], upper_cell[c]))
            value = jnp.minimum(value, 0.5 + 0.5 * jnp.maximum(lower_cell[c], upper_cell[c]))
        out.append(value)
    return out


def side(w, normal):
    density = w[0] + w[1]
    gamma, stiff = mixture(w[6])
    momentum = [density * w[2], density * w[3], density * w[4]]
    energy = (
        gamma * w[5]
        + stiff
        + 0.5 * (momentum[0] * w[2] + momentum[1] * w[3] + momentum[2] * w[4])
    )
    vn = w[2 + normal]
    amounts = [w[0], w[1], *momentum, energy, w[6]]
    moved = [amount * vn for amount in amounts]
    moved[2 + normal] = moved[2 + normal] + w[5]
    moved[5] = moved[5] + w[5] * vn
    signal = jnp.abs(vn) + sound(density, w[5], gamma, stiff)
    return (amounts, moved, vn, signal)


def fluxes(left, right, lower_cell, upper_cell, normal):
    one = side(limited(left, lower_cell, upper_cell), normal)
    two = side(limited(right, lower_cell, upper_cell), normal)
    fastest = jnp.maximum(one[3], two[3])
    out = [
        (fl + fr) - fastest * (ur - ul)
        for ul, ur, fl, fr in zip(one[0], two[0], one[1], two[1])
    ]
    return out + [one[2] + two[2]]


def rolled(value, shift, axis):
    return pltpu.roll(value, shift % value.shape[axis], axis)


def along(w, axis, normal):
    upper, lower, before = ([], [], [])
    for c in range(7):
        h = w[c]
        g = rolled(h, 1, axis)
        d2 = h - g
        d1, d3, d4 = (rolled(d2, 1, axis), rolled(d2, -1, axis), rolled(d2, -2, axis))
        up, down = edges(h, d1, d2, d3, d4)
        upper.append(rolled(up, 1, axis))
        lower.append(down)
        before.append(g)
    return fluxes(upper, lower, before, w, normal)


def spread(flux, axis, keep=None):
    if keep is not None:
        flux = [jnp.where(keep, f, 0.0) for f in flux]
    return [rolled(f, -1, axis) - f for f in flux]


def folded(change, volume):
    return change[:6] + [change[6] - volume * change[7]]


def ring(stage, sizes):
    inner_s, inner_c, outer_s, outer_c = sizes
    s, c = (lax.axis_index("stream"), lax.axis_index("cross"))
    if stage == 0:
        base = s // inner_s * inner_s
        return inner_s, lambda k: (base + (s - base + k) % inner_s, c)
    if stage == 1:
        n = outer_s * inner_c
        place = s // inner_s * inner_c + c % inner_c

        def at(k):
            there = (place + k) % n
            return (
                there // inner_c * inner_s + s % inner_s,
                c // inner_c * inner_c + there % inner_c,
            )

        return n, at
    return outer_c, lambda k: (s, (c + k * inner_c) % (outer_c * inner_c))


def send(source, target, send_sem, recv_sem, to):
    return pltpu.make_async_remote_copy(
        src_ref=source,
        dst_ref=target,
        send_sem=send_sem,
        recv_sem=recv_sem,
        device_id=to,
        device_id_type=MESH,
    )


def kernel(
    sizes,
    now_ref,
    base_ref,
    inflow_ref,
    rate_ref,
    fast_ref,
    cells,
    base,
    inflow,
    prim,
    xr,
    flux_prev,
    acc,
    a_own,
    a_left,
    a_right,
    edge,
    rows,
    slots0,
    slots1,
    slots2,
    in_sems,
    halo_send,
    halo_recv,
    stage_send,
    stage_recv,
):
    size_s, size_c = (sizes[0] * sizes[2], sizes[1] * sizes[3])
    s, c = (lax.axis_index("stream"), lax.axis_index("cross"))
    left, right = (((s + size_s - 1) % size_s, c), ((s + 1) % size_s, c))
    below, above = ((s, (c + size_c - 1) % size_c), (s, (c + 1) % size_c))
    slots = (slots0, slots1, slots2)
    stages = [ring(k, sizes) for k in range(3)]

    barrier = pltpu.get_barrier_semaphore()
    count = 0
    for stage in (2, 1, 0):
        n, at = stages[stage]
        for k in range(1, n):
            pl.semaphore_signal(barrier, inc=1, device_id=at(k), device_id_type=MESH)
            count += 1
    for there in (below, above, left, right):
        pl.semaphore_signal(barrier, inc=1, device_id=there, device_id_type=MESH)
        count += 1

    load_base = pltpu.make_async_copy(base_ref, base, in_sems.at[0])
    load_now = pltpu.make_async_copy(now_ref, cells.at[:, 3:11], in_sems.at[1])
    load_inflow = pltpu.make_async_copy(inflow_ref, inflow, in_sems.at[2])
    load_base.start()
    load_now.start()
    load_inflow.start()

    def all_of(ref, *index):
        return [ref[(k, *index)] for k in range(7)]

    def speed(y, most):
        w = primitive(all_of(base, y))
        gamma, stiff = mixture(w[6])
        swift = jnp.maximum(jnp.maximum(jnp.abs(w[2]), jnp.abs(w[3])), jnp.abs(w[4]))
        return jnp.maximum(most, swift + sound(w[0] + w[1], w[5], gamma, stiff))

    load_base.wait()
    most = lax.fori_loop(0, 8, speed, jnp.zeros((8, 128), jnp.float32))
    rows[0] = jnp.broadcast_to(jnp.max(most, keepdims=True), (1, 128))
    load_now.wait()
    load_inflow.wait()

    lane = lax.broadcasted_iota(jnp.int32, (8, 128), 1)
    place = lane % 16
    group = lane // 16
    for k in range(7):
        packed = rolled(cells[k, 3], 5, 1)
        for y in range(1, 8):
            packed = jnp.where(group == y, rolled(cells[k, 3 + y], 16 * y + 5, 1), packed)
        a_own[k] = packed

    def to_prim(y, _):
        for k, value in enumerate(primitive(all_of(cells, y))):
            prim[k, y] = value
        return 0

    pl.semaphore_wait(barrier, count)

    copies = [
        send(cells.at[:, 3:6], cells.at[:, 11:14], halo_send.at[0], halo_recv.at[0], below),
        send(cells.at[:, 8:11], cells.at[:, 0:3], halo_send.at[1], halo_recv.at[1], above),
        send(a_own, a_right, halo_send.at[2], halo_recv.at[2], left),
        send(a_own, a_left, halo_send.at[3], halo_recv.at[3], right),
    ]

    def stage_start(stage):
        n, at = stages[stage]
        for k in range(1, n):
            send(
                rows.at[stage],
                slots[stage].at[k - 1],
                stage_send.at[stage],
                stage_recv.at[stage],
                at(k),
            ).start()

    def stage_total(stage):
        n, at = stages[stage]
        return send(slots[stage], slots[stage], stage_send.at[stage], stage_recv.at[stage], at(1))

    def stage_end(stage):
        n, _ = stages[stage]
        stage_total(stage).wait_recv()
        value = rows[stage]
        for k in range(1, n):
            value = jnp.maximum(value, slots[stage][k - 1])
        return value

    stage_start(0)
    for copy in copies:
        copy.start()

    lax.fori_loop(3, 11, to_prim, 0)

    def local(y, _):
        w = all_of(prim, y + 3)
        across = folded(spread(along(w, 0, 2), 0), w[6])
        keep = (lane >= 3) & (lane <= 125)
        stream = folded(spread(along(w, 1, 0), 1, keep), w[6])
        for k in range(7):
            acc[k, y + 1] = across[k] + stream[k]
        return 0

    lax.fori_loop(0, 8, local, 0)

    rows[1] = stage_end(0)
    stage_start(1)

    for copy in copies:
        copy.wait_recv()

    @pl.when(s == 0)
    def _():
        for k in range(7):
            value = jnp.zeros((8, 128), jnp.float32)
            for layer in range(3):
                for y in range(8):
                    one = jnp.broadcast_to(inflow[k, layer][:, y : y + 1], (8, 128))
                    value = jnp.where((group == y) & (place == 2 + layer), one, value)
            a_left[k] = value

    @pl.when(s == size_s - 1)
    def _():
        for k in range(7):
            value = a_own[k]
            one, two, three = (rolled(value, 1, 1), rolled(value, 2, 1), rolled(value, 3, 1))
            a_right[k] = jnp.where(place == 5, one, jnp.where(place == 6, two, three))

    rim = []
    for k in range(7):
        own = a_own[k]
        late = rolled(jnp.where(place < 5, a_left[k], own), 6, 1)
        rim.append(jnp.where(place < 5, own, jnp.where(place < 8, a_right[k], late)))
    w = primitive(rim)
    keep = ((place >= 3) & (place <= 5)) | ((place >= 11) & (place <= 13))
    ends = folded(spread(along(w, 1, 0), 1, keep), w[6])
    for k in range(7):
        edge[k] = jnp.where(place < 5, ends[k], rolled(ends[k], -6, 1))

    lax.fori_loop(0, 3, to_prim, 0)
    lax.fori_loop(11, 14, to_prim, 0)

    def cell_edges(y):
        upper, lower = ([], [])
        for k in range(7):
            f, g, h, up, far = (prim[k, y + i] for i in range(1, 6))
            one, two = edges(h, g - f, h - g, up - h, far - up)
            upper.append(one)
            lower.append(two)
        return (upper, lower)

    for k, value in enumerate(cell_edges(-1 + 0)[0]):
        xr[k] = value
    for k in range(8):
        flux_prev[k] = jnp.zeros((8, 128), jnp.float32)
    for k in range(7):
        acc[k, 0] = jnp.zeros((8, 128), jnp.float32)

    def face(j, _):
        upper, lower = cell_edges(j)
        before = all_of(xr)
        for k in range(7):
            xr[k] = upper[k]
        lower_cell = all_of(prim, j + 2)
        flux = fluxes(before, lower, lower_cell, all_of(prim, j + 3), 1)
        change = [flux[k] - flux_prev[k] for k in range(8)]
        for k in range(8):
            flux_prev[k] = flux[k]
        for k, value in enumerate(folded(change, lower_cell[6])):
            acc[k, j] = acc[k, j] + value
        return 0

    lax.fori_loop(0, 9, face, 0)

    rows[2] = stage_end(1)
    stage_start(2)

    near = (lane >= 125) | (lane <= 2)
    for k in range(7):
        for y in range(8):
            extra = jnp.where(near, rolled(edge[k], 123 - 16 * y, 1), 0.0)
            rate_ref[k, y] = acc[k, y + 1] + extra

    fast_ref[...] = stage_end(2)
    for copy in copies:
        copy.wait_send()
    for stage in range(3):
        stage_total(stage).wait_send()


def shards(sizes, state_now, state_base, inflow):
    size = jnp.float32
    n0, n1, n2 = (sizes[0], sizes[1] * sizes[2], sizes[3])
    now_t = jnp.transpose(state_now, (0, 2, 1, 3))
    base_t = jnp.transpose(state_base, (0, 2, 1, 3))
    inflow_t = jnp.transpose(inflow, (0, 3, 1, 2))
    rate, fast = pl.pallas_call(
        functools.partial(kernel, sizes),
        out_shape=(
            jax.ShapeDtypeStruct((7, 8, 8, 128), size),
            jax.ShapeDtypeStruct((1, 128), size),
        ),
        in_specs=[pl.BlockSpec(memory_space=pl.ANY)] * 3,
        out_specs=(pl.BlockSpec(memory_space=pltpu.VMEM),) * 2,
        scratch_shapes=[
            pltpu.VMEM((7, 14, 8, 128), size),
            pltpu.VMEM((7, 8, 8, 128), size),
            pltpu.VMEM((7, 3, 8, 8), size),
            pltpu.VMEM((7, 14, 8, 128), size),
            pltpu.VMEM((7, 8, 128), size),
            pltpu.VMEM((8, 8, 128), size),
            pltpu.VMEM((7, 9, 8, 128), size),
            pltpu.VMEM((7, 8, 128), size),
            pltpu.VMEM((7, 8, 128), size),
            pltpu.VMEM((7, 8, 128), size),
            pltpu.VMEM((7, 8, 128), size),
            pltpu.VMEM((3, 1, 128), size),
            pltpu.VMEM((n0 - 1, 1, 128), size),
            pltpu.VMEM((n1 - 1, 1, 128), size),
            pltpu.VMEM((n2 - 1, 1, 128), size),
            pltpu.SemaphoreType.DMA((3,)),
            pltpu.SemaphoreType.DMA((4,)),
            pltpu.SemaphoreType.DMA((4,)),
            pltpu.SemaphoreType.DMA((3,)),
            pltpu.SemaphoreType.DMA((3,)),
        ],
        compiler_params=pltpu.CompilerParams(collective_id=0, has_side_effects=True),
    )(now_t, base_t, inflow_t)
    step = 0.3 / fast[0, 0]
    rate = jnp.transpose(rate, (0, 2, 1, 3)) * -0.5
    return state_base / 3.0 + 2.0 / 3.0 * (state_now + step * rate)


def solution(mesh):
    stream, cross = (mesh.shape["stream"], mesh.shape["cross"])
    sizes = (8, 4, 2, 12) if (stream, cross) == (16, 48) else (2, 2, stream // 2, cross // 2)
    return jax.shard_map(
        functools.partial(shards, sizes),
        mesh=mesh,
        in_specs=(
            P(None, None, "cross", "stream"),
            P(None, None, "cross", "stream"),
            P(None, None, "cross", None),
        ),
        out_specs=P(None, None, "cross", "stream"),
        check_vma=False,
    )
```

```python
import functools

import jax
import jax.numpy as jnp
from jax import lax
from jax.experimental import pallas as pl
from jax.experimental.pallas import tpu as pltpu
from jax.sharding import PartitionSpec as P

MESH = pl.DeviceIdType.MESH

gas_part = 1.0 / 0.4
liquid_part = 1.0 / 3.4
stiff_part = 4.4 * 0.6 / 3.4


def inverse(value):
    guess = pl.reciprocal(value, approx=True)
    return guess * (2.0 - value * guess)


def mixture(volume):
    rest = 1.0 - volume
    return (volume * gas_part + rest * liquid_part, rest * stiff_part)


def primitive(u):
    over = 1.0 / (u[0] + u[1])
    vx, vy, vz = (u[2] * over, u[3] * over, u[4] * over)
    kinetic = 0.5 * (u[2] * vx + u[3] * vy + u[4] * vz)
    gamma, stiff = mixture(u[6])
    return (u[0], u[1], vx, vy, vz, (u[5] - kinetic - stiff) / gamma, u[6])


def sound(density, pressure, gamma, stiff):
    return jnp.sqrt(((gamma + 1.0) * pressure + stiff) / (gamma * density))


def edges(h, d1, d2, d3, d4):
    e1, e2, e3 = (d2 - d1, d3 - d2, d4 - d3)
    u0 = e1 + d2 + d2
    u1 = d2 + d3
    u2 = e3 - d3 - d3
    third = 13.0 / 3.0
    top = 1e30
    s0 = jnp.minimum(third * (e1 * e1) + u0 * u0 + 4e-6, top)
    s1 = jnp.minimum(third * (e2 * e2) + u1 * u1 + 4e-6, top)
    s2 = jnp.minimum(third * (e3 * e3) + u2 * u2 + 4e-6, top)
    r0, r1, r2 = (inverse(s0), inverse(s1), inverse(s2))
    a0, a1, a2 = (r0 * r0, 6.0 * (r1 * r1), r2 * r2)
    b0, b2 = (3.0 * a0, 3.0 * a2)
    up = a0 * (u0 + e1 + d2) + a1 * (u1 + d3) + b2 * (d3 - u2)
    down = a2 * (u2 + e3 - d3) - a1 * (u1 + d2) - b0 * (u0 + d2)
    upper = h + up * inverse(6.0 * (a0 + a1 + b2))
    lower = h + down * inverse(6.0 * (a2 + a1 + b0))
    return (upper, lower)


def limited(face, lower_cell, upper_cell):
    out = []
    for c in range(7):
        value = face[c]
        if c in (0, 1, 5):
            value = jnp.maximum(value, 0.5 * jnp.minimum(lower_cell[c], upper_cell[c]))
        elif c == 6:
            value = jnp.maximum(value, 0.5 * jnp.minimum(lower_cell[c], upper_cell[c]))
            value = jnp.minimum(value, 0.5 + 0.5 * jnp.maximum(lower_cell[c], upper_cell[c]))
        out.append(value)
    return out


def side(w, normal):
    density = w[0] + w[1]
    gamma, stiff = mixture(w[6])
    momentum = [density * w[2], density * w[3], density * w[4]]
    energy = (
        gamma * w[5]
        + stiff
        + 0.5 * (momentum[0] * w[2] + momentum[1] * w[3] + momentum[2] * w[4])
    )
    vn = w[2 + normal]
    amounts = [w[0], w[1], *momentum, energy, w[6]]
    moved = [amount * vn for amount in amounts]
    moved[2 + normal] = moved[2 + normal] + w[5]
    moved[5] = moved[5] + w[5] * vn
    signal = jnp.abs(vn) + sound(density, w[5], gamma, stiff)
    return (amounts, moved, vn, signal)


def fluxes(left, right, lower_cell, upper_cell, normal):
    one = side(limited(left, lower_cell, upper_cell), normal)
    two = side(limited(right, lower_cell, upper_cell), normal)
    fastest = jnp.maximum(one[3], two[3])
    out = [
        (fl + fr) - fastest * (ur - ul)
        for ul, ur, fl, fr in zip(one[0], two[0], one[1], two[1])
    ]
    return out + [one[2] + two[2]]


def rolled(value, shift, axis):
    return pltpu.roll(value, shift % value.shape[axis], axis)


def along(w, axis, normal):
    upper, lower, before = ([], [], [])
    for c in range(7):
        h = w[c]
        g = rolled(h, 1, axis)
        d2 = h - g
        d1, d3, d4 = (rolled(d2, 1, axis), rolled(d2, -1, axis), rolled(d2, -2, axis))
        up, down = edges(h, d1, d2, d3, d4)
        upper.append(rolled(up, 1, axis))
        lower.append(down)
        before.append(g)
    return fluxes(upper, lower, before, w, normal)


def spread(flux, axis, keep=None):
    if keep is not None:
        flux = [jnp.where(keep, f, 0.0) for f in flux]
    return [rolled(f, -1, axis) - f for f in flux]


def folded(change, volume):
    return change[:6] + [change[6] - volume * change[7]]


def ring(stage, sizes):
    inner_s, inner_c, outer_s, outer_c = sizes
    s, c = (lax.axis_index("stream"), lax.axis_index("cross"))
    if stage == 0:
        base = s // inner_s * inner_s
        return inner_s, lambda k: (base + (s - base + k) % inner_s, c)
    if stage == 1:
        n = outer_s * inner_c
        place = s // inner_s * inner_c + c % inner_c

        def at(k):
            there = (place + k) % n
            return (
                there // inner_c * inner_s + s % inner_s,
                c // inner_c * inner_c + there % inner_c,
            )

        return n, at
    return outer_c, lambda k: (s, (c + k * inner_c) % (outer_c * inner_c))


def far_first(n):
    return sorted(range(1, n), key=lambda k: -min(k, n - k))


def send(source, target, send_sem, recv_sem, to):
    return pltpu.make_async_remote_copy(
        src_ref=source,
        dst_ref=target,
        send_sem=send_sem,
        recv_sem=recv_sem,
        device_id=to,
        device_id_type=MESH,
    )


def kernel(
    sizes,
    now_ref,
    base_ref,
    inflow_ref,
    rate_ref,
    fast_ref,
    now,
    base,
    halo,
    inflow,
    prim,
    xr,
    flux_prev,
    acc,
    a_own,
    a_left,
    a_right,
    edge,
    rows,
    slots0,
    slots1,
    slots2,
    in_sems,
    halo_send,
    halo_recv,
    stage_send,
    stage_recv,
):
    size_s, size_c = (sizes[0] * sizes[2], sizes[1] * sizes[3])
    s, c = (lax.axis_index("stream"), lax.axis_index("cross"))
    left, right = (((s + size_s - 1) % size_s, c), ((s + 1) % size_s, c))
    below, above = ((s, (c + size_c - 1) % size_c), (s, (c + 1) % size_c))
    slots = (slots0, slots1, slots2)
    stages = [ring(k, sizes) for k in range(3)]

    load_base = pltpu.make_async_copy(base_ref, base, in_sems.at[0])
    load_now = pltpu.make_async_copy(now_ref, now, in_sems.at[1])
    load_inflow = pltpu.make_async_copy(inflow_ref, inflow, in_sems.at[2])
    load_base.start()
    load_now.start()
    load_inflow.start()

    barrier = pltpu.get_barrier_semaphore()
    count = 0
    for stage in (2, 1, 0):
        n, at = stages[stage]
        for k in far_first(n):
            pl.semaphore_signal(barrier, inc=1, device_id=at(k), device_id_type=MESH)
            count += 1
    for there in (below, above, left, right):
        pl.semaphore_signal(barrier, inc=1, device_id=there, device_id_type=MESH)
        count += 1

    now_rows = now.reshape(7, 64, 128)
    halo_rows = halo.reshape(7, 64, 128)

    def across_rows(ref, y):
        return [ref[k, pl.ds(y, 8, stride=8), :] for k in range(7)]

    def all_of(ref, *index):
        return [ref[(k, *index)] for k in range(7)]

    def speed(y, most):
        w = primitive(all_of(base, y))
        gamma, stiff = mixture(w[6])
        swift = jnp.maximum(jnp.maximum(jnp.abs(w[2]), jnp.abs(w[3])), jnp.abs(w[4]))
        return jnp.maximum(most, swift + sound(w[0] + w[1], w[5], gamma, stiff))

    load_base.wait()
    most = lax.fori_loop(0, 8, speed, jnp.zeros((8, 128), jnp.float32))
    rows[0] = jnp.broadcast_to(jnp.max(most, keepdims=True), (1, 128))
    pl.semaphore_wait(barrier, count)

    def stage_start(stage):
        n, at = stages[stage]
        for k in far_first(n):
            send(
                rows.at[stage],
                slots[stage].at[k - 1],
                stage_send.at[stage],
                stage_recv.at[stage],
                at(k),
            ).start()

    def stage_total(stage):
        n, at = stages[stage]
        return send(slots[stage], slots[stage], stage_send.at[stage], stage_recv.at[stage], at(1))

    def stage_end(stage):
        n, _ = stages[stage]
        stage_total(stage).wait_recv()
        value = rows[stage]
        for k in range(1, n):
            value = jnp.maximum(value, slots[stage][k - 1])
        return value

    stage_start(0)
    load_now.wait()
    load_inflow.wait()

    lane = lax.broadcasted_iota(jnp.int32, (8, 128), 1)
    place = lane % 16
    group = lane // 16

    def pack(y, packed):
        packed = list(packed)
        for k, value in enumerate(across_rows(now_rows, y)):
            packed[k] = jnp.where(group == y, pltpu.roll(value, 16 * y + 5, 1), packed[k])
        return tuple(packed)

    packed = (jnp.zeros((8, 128), jnp.float32),) * 7
    for y in range(8):
        packed = pack(y, packed)
    for k in range(7):
        a_own[k] = packed[k]

    copies = [
        send(now.at[:, :, 0:3], halo.at[:, :, 0:3], halo_send.at[0], halo_recv.at[0], below),
        send(now.at[:, :, 5:8], halo.at[:, :, 5:8], halo_send.at[1], halo_recv.at[1], above),
        send(a_own, a_right, halo_send.at[2], halo_recv.at[2], left),
        send(a_own, a_left, halo_send.at[3], halo_recv.at[3], right),
    ]
    for copy in copies:
        copy.start()

    rows[1] = stage_end(0)
    stage_start(1)

    def own_prim(y, _):
        for k, value in enumerate(primitive(across_rows(now_rows, y))):
            prim[k, y + 3] = value
        return 0

    lax.fori_loop(0, 8, own_prim, 0)

    def local(y, _):
        w = all_of(prim, y + 3)
        across = folded(spread(along(w, 0, 2), 0), w[6])
        keep = (lane >= 3) & (lane <= 125)
        stream = folded(spread(along(w, 1, 0), 1, keep), w[6])
        for k in range(7):
            acc[k, y + 1] = across[k] + stream[k]
        return 0

    lax.fori_loop(0, 8, local, 0)

    rows[2] = stage_end(1)
    stage_start(2)

    for copy in copies:
        copy.wait_recv()

    @pl.when(s == 0)
    def _():
        for k in range(7):
            value = jnp.zeros((8, 128), jnp.float32)
            for layer in range(3):
                for y in range(8):
                    one = jnp.broadcast_to(inflow[k, layer][:, y : y + 1], (8, 128))
                    value = jnp.where((group == y) & (place == 2 + layer), one, value)
            a_left[k] = value

    @pl.when(s == size_s - 1)
    def _():
        for k in range(7):
            value = a_own[k]
            one, two, three = (rolled(value, 1, 1), rolled(value, 2, 1), rolled(value, 3, 1))
            a_right[k] = jnp.where(place == 5, one, jnp.where(place == 6, two, three))

    rim = []
    for k in range(7):
        own = a_own[k]
        late = rolled(jnp.where(place < 5, a_left[k], own), 6, 1)
        rim.append(jnp.where(place < 5, own, jnp.where(place < 8, a_right[k], late)))
    w = primitive(rim)
    keep = ((place >= 3) & (place <= 5)) | ((place >= 11) & (place <= 13))
    ends = folded(spread(along(w, 1, 0), 1, keep), w[6])
    for k in range(7):
        edge[k] = jnp.where(place < 5, ends[k], rolled(ends[k], -6, 1))

    def halo_prim(i, _):
        row = i + i // 3 * 8
        for k, value in enumerate(primitive(across_rows(halo_rows, (i + 5) % 8))):
            prim[k, row] = value
        return 0

    lax.fori_loop(0, 6, halo_prim, 0)

    def cell_edges(y):
        upper, lower = ([], [])
        for k in range(7):
            f, g, h, up, far = (prim[k, y + i] for i in range(1, 6))
            one, two = edges(h, g - f, h - g, up - h, far - up)
            upper.append(one)
            lower.append(two)
        return (upper, lower)

    for k, value in enumerate(cell_edges(-1)[0]):
        xr[k] = value
    for k in range(8):
        flux_prev[k] = jnp.zeros((8, 128), jnp.float32)
    for k in range(7):
        acc[k, 0] = jnp.zeros((8, 128), jnp.float32)

    def face(j, _):
        upper, lower = cell_edges(j)
        before = all_of(xr)
        for k in range(7):
            xr[k] = upper[k]
        lower_cell = all_of(prim, j + 2)
        flux = fluxes(before, lower, lower_cell, all_of(prim, j + 3), 1)
        change = [flux[k] - flux_prev[k] for k in range(8)]
        for k in range(8):
            flux_prev[k] = flux[k]
        for k, value in enumerate(folded(change, lower_cell[6])):
            acc[k, j] = acc[k, j] + value
        return 0

    lax.fori_loop(0, 9, face, 0)

    near = (lane >= 125) | (lane <= 2)
    for k in range(7):
        for y in range(8):
            extra = jnp.where(near, rolled(edge[k], 123 - 16 * y, 1), 0.0)
            rate_ref[k, pl.ds(y, 8, stride=8), :] = acc[k, y + 1] + extra

    fast_ref[...] = stage_end(2)
    for copy in copies:
        copy.wait_send()
    for stage in range(3):
        stage_total(stage).wait_send()


def shards(sizes, state_now, state_base, inflow):
    size = jnp.float32
    n0, n1, n2 = (sizes[0], sizes[1] * sizes[2], sizes[3])
    inflow_t = jnp.transpose(inflow, (0, 3, 1, 2))
    rate, fast = pl.pallas_call(
        functools.partial(kernel, sizes),
        out_shape=(
            jax.ShapeDtypeStruct((7, 64, 128), size),
            jax.ShapeDtypeStruct((1, 128), size),
        ),
        in_specs=[pl.BlockSpec(memory_space=pltpu.HBM)] * 3,
        out_specs=(pl.BlockSpec(memory_space=pltpu.VMEM),) * 2,
        scratch_shapes=[
            pltpu.VMEM((7, 8, 8, 128), size),
            pltpu.VMEM((7, 8, 8, 128), size),
            pltpu.VMEM((7, 8, 8, 128), size),
            pltpu.VMEM((7, 3, 8, 8), size),
            pltpu.VMEM((7, 14, 8, 128), size),
            pltpu.VMEM((7, 8, 128), size),
            pltpu.VMEM((8, 8, 128), size),
            pltpu.VMEM((7, 9, 8, 128), size),
            pltpu.VMEM((7, 8, 128), size),
            pltpu.VMEM((7, 8, 128), size),
            pltpu.VMEM((7, 8, 128), size),
            pltpu.VMEM((7, 8, 128), size),
            pltpu.VMEM((3, 1, 128), size),
            pltpu.VMEM((n0 - 1, 1, 128), size),
            pltpu.VMEM((n1 - 1, 1, 128), size),
            pltpu.VMEM((n2 - 1, 1, 128), size),
            pltpu.SemaphoreType.DMA((3,)),
            pltpu.SemaphoreType.DMA((4,)),
            pltpu.SemaphoreType.DMA((4,)),
            pltpu.SemaphoreType.DMA((3,)),
            pltpu.SemaphoreType.DMA((3,)),
        ],
        compiler_params=pltpu.CompilerParams(
            collective_id=0, has_side_effects=True, vmem_limit_bytes=32 * 1024 * 1024
        ),
    )(
        pltpu.with_memory_space_constraint(state_now, pltpu.HBM),
        pltpu.with_memory_space_constraint(state_base, pltpu.HBM),
        pltpu.with_memory_space_constraint(inflow_t, pltpu.HBM),
    )
    step = 0.3 / fast[0, 0]
    rate = rate.reshape(state_now.shape) * -0.5
    return state_base / 3.0 + 2.0 / 3.0 * (state_now + step * rate)


def solution(mesh):
    stream, cross = (mesh.shape["stream"], mesh.shape["cross"])
    sizes = (8, 4, 2, 12) if (stream, cross) == (16, 48) else (2, 2, stream // 2, cross // 2)
    return jax.shard_map(
        functools.partial(shards, sizes),
        mesh=mesh,
        in_specs=(
            P(None, None, "cross", "stream"),
            P(None, None, "cross", "stream"),
            P(None, None, "cross", None),
        ),
        out_specs=P(None, None, "cross", "stream"),
        check_vma=False,
    )
```

```python
import functools

import jax
import jax.numpy as jnp
from jax import lax
from jax.experimental import pallas as pl
from jax.experimental.pallas import tpu as pltpu
from jax.sharding import PartitionSpec as P

MESH = pl.DeviceIdType.MESH

gas_part = 1.0 / 0.4
liquid_part = 1.0 / 3.4
stiff_part = 4.4 * 0.6 / 3.4


def inverse(value):
    guess = pl.reciprocal(value, approx=True)
    return guess * (2.0 - value * guess)


def mixture(volume):
    rest = 1.0 - volume
    return (volume * gas_part + rest * liquid_part, rest * stiff_part)


def primitive(u):
    over = 1.0 / (u[0] + u[1])
    vx, vy, vz = (u[2] * over, u[3] * over, u[4] * over)
    kinetic = 0.5 * (u[2] * vx + u[3] * vy + u[4] * vz)
    gamma, stiff = mixture(u[6])
    return (u[0], u[1], vx, vy, vz, (u[5] - kinetic - stiff) / gamma, u[6])


def sound(density, pressure, gamma, stiff):
    return jnp.sqrt(((gamma + 1.0) * pressure + stiff) / (gamma * density))


def edges(h, d1, d2, d3, d4):
    e1, e2, e3 = (d2 - d1, d3 - d2, d4 - d3)
    u0 = e1 + d2 + d2
    u1 = d2 + d3
    u2 = e3 - d3 - d3
    third = 13.0 / 3.0
    top = 1e30
    s0 = jnp.minimum(third * (e1 * e1) + u0 * u0 + 4e-6, top)
    s1 = jnp.minimum(third * (e2 * e2) + u1 * u1 + 4e-6, top)
    s2 = jnp.minimum(third * (e3 * e3) + u2 * u2 + 4e-6, top)
    r0, r1, r2 = (inverse(s0), inverse(s1), inverse(s2))
    a0, a1, a2 = (r0 * r0, 6.0 * (r1 * r1), r2 * r2)
    b0, b2 = (3.0 * a0, 3.0 * a2)
    up = a0 * (u0 + e1 + d2) + a1 * (u1 + d3) + b2 * (d3 - u2)
    down = a2 * (u2 + e3 - d3) - a1 * (u1 + d2) - b0 * (u0 + d2)
    upper = h + up * inverse(6.0 * (a0 + a1 + b2))
    lower = h + down * inverse(6.0 * (a2 + a1 + b0))
    return (upper, lower)


def limited(face, lower_cell, upper_cell):
    out = []
    for c in range(7):
        value = face[c]
        if c in (0, 1, 5):
            value = jnp.maximum(value, 0.5 * jnp.minimum(lower_cell[c], upper_cell[c]))
        elif c == 6:
            value = jnp.maximum(value, 0.5 * jnp.minimum(lower_cell[c], upper_cell[c]))
            value = jnp.minimum(value, 0.5 + 0.5 * jnp.maximum(lower_cell[c], upper_cell[c]))
        out.append(value)
    return out


def side(w, normal):
    density = w[0] + w[1]
    gamma, stiff = mixture(w[6])
    momentum = [density * w[2], density * w[3], density * w[4]]
    energy = (
        gamma * w[5]
        + stiff
        + 0.5 * (momentum[0] * w[2] + momentum[1] * w[3] + momentum[2] * w[4])
    )
    vn = w[2 + normal]
    amounts = [w[0], w[1], *momentum, energy, w[6]]
    moved = [amount * vn for amount in amounts]
    moved[2 + normal] = moved[2 + normal] + w[5]
    moved[5] = moved[5] + w[5] * vn
    signal = jnp.abs(vn) + sound(density, w[5], gamma, stiff)
    return (amounts, moved, vn, signal)


def fluxes(left, right, lower_cell, upper_cell, normal):
    one = side(limited(left, lower_cell, upper_cell), normal)
    two = side(limited(right, lower_cell, upper_cell), normal)
    fastest = jnp.maximum(one[3], two[3])
    out = [
        (fl + fr) - fastest * (ur - ul)
        for ul, ur, fl, fr in zip(one[0], two[0], one[1], two[1])
    ]
    return out + [one[2] + two[2]]


def rolled(value, shift, axis):
    return pltpu.roll(value, shift % value.shape[axis], axis)


def along(w, axis, normal):
    upper, lower, before = ([], [], [])
    for c in range(7):
        h = w[c]
        g = rolled(h, 1, axis)
        d2 = h - g
        d1, d3, d4 = (rolled(d2, 1, axis), rolled(d2, -1, axis), rolled(d2, -2, axis))
        up, down = edges(h, d1, d2, d3, d4)
        upper.append(rolled(up, 1, axis))
        lower.append(down)
        before.append(g)
    return fluxes(upper, lower, before, w, normal)


def spread(flux, axis, keep=None):
    if keep is not None:
        flux = [jnp.where(keep, f, 0.0) for f in flux]
    return [rolled(f, -1, axis) - f for f in flux]


def folded(change, volume):
    return change[:6] + [change[6] - volume * change[7]]


def ring(stage, sizes):
    inner_s, inner_c, outer_s, outer_c = sizes
    s, c = (lax.axis_index("stream"), lax.axis_index("cross"))
    if stage == 0:
        base = s // inner_s * inner_s
        return inner_s, lambda k: (base + (s - base + k) % inner_s, c)
    if stage == 1:
        n = outer_s * inner_c
        place = s // inner_s * inner_c + c % inner_c

        def at(k):
            there = (place + k) % n
            return (
                there // inner_c * inner_s + s % inner_s,
                c // inner_c * inner_c + there % inner_c,
            )

        return n, at
    return outer_c, lambda k: (s, (c + k * inner_c) % (outer_c * inner_c))


def far_first(n):
    return sorted(range(1, n), key=lambda k: -min(k, n - k))


def send(source, target, send_sem, recv_sem, to):
    return pltpu.make_async_remote_copy(
        src_ref=source,
        dst_ref=target,
        send_sem=send_sem,
        recv_sem=recv_sem,
        device_id=to,
        device_id_type=MESH,
    )


def kernel(
    sizes,
    now_ref,
    base_ref,
    inflow_ref,
    part_ref,
    rate_ref,
    fast_ref,
    now,
    base,
    halo,
    inflow,
    prim,
    xr,
    flux_prev,
    acc,
    a_own,
    a_left,
    a_right,
    edge,
    rows,
    slots0,
    slots1,
    slots2,
    told,
    in_sems,
    halo_send,
    halo_recv,
    stage_send,
    stage_recv,
):
    size_s, size_c = (sizes[0] * sizes[2], sizes[1] * sizes[3])
    s, c = (lax.axis_index("stream"), lax.axis_index("cross"))
    left, right = (((s + size_s - 1) % size_s, c), ((s + 1) % size_s, c))
    below, above = ((s, (c + size_c - 1) % size_c), (s, (c + 1) % size_c))
    slots = (slots0, slots1, slots2)
    stages = [ring(k, sizes) for k in range(3)]
    inner_c, planes = (sizes[1], sizes[3])
    roots = max(1, planes // 3)
    plane = c // inner_c
    is_root = plane < roots

    load_base = pltpu.make_async_copy(base_ref, base, in_sems.at[0])
    load_now = pltpu.make_async_copy(now_ref, now, in_sems.at[1])
    load_inflow = pltpu.make_async_copy(inflow_ref, inflow, in_sems.at[2])
    load_base.start()
    load_now.start()
    load_inflow.start()

    barrier = pltpu.get_barrier_semaphore()

    def greet(there):
        pl.semaphore_signal(barrier, inc=1, device_id=there, device_id_type=MESH)

    for there in (left, right, below, above):
        greet(there)

    @pl.when(is_root)
    def _():
        for stage in (2, 1, 0):
            n, at = stages[stage]
            for k in far_first(n):
                greet(at(k))

    now_rows = now.reshape(7, 64, 128)
    halo_rows = halo.reshape(7, 64, 128)

    def across_rows(ref, y):
        return [ref[k, pl.ds(y, 8, stride=8), :] for k in range(7)]

    def all_of(ref, *index):
        return [ref[(k, *index)] for k in range(7)]

    def speed(y, most):
        w = primitive(all_of(base, y))
        gamma, stiff = mixture(w[6])
        swift = jnp.maximum(jnp.maximum(jnp.abs(w[2]), jnp.abs(w[3])), jnp.abs(w[4]))
        return jnp.maximum(most, swift + sound(w[0] + w[1], w[5], gamma, stiff))

    load_base.wait()
    most = lax.fori_loop(0, 8, speed, jnp.zeros((8, 128), jnp.float32))
    rows[2] = jnp.broadcast_to(jnp.max(most, keepdims=True), (1, 128))
    @pl.when(is_root)
    def _():
        pl.semaphore_wait(barrier, 4 + roots - 1 + stages[1][0] - 1 + stages[0][0] - 1)

    @pl.when(jnp.logical_not(is_root))
    def _():
        pl.semaphore_wait(barrier, 4 + roots)

    def stage_start(stage):
        n, at = stages[stage]
        for k in far_first(n):
            send(
                rows.at[stage],
                slots[stage].at[k - 1],
                stage_send.at[stage],
                stage_recv.at[stage],
                at(k),
            ).start()

    def stage_total(stage):
        n, at = stages[stage]
        return send(slots[stage], slots[stage], stage_send.at[stage], stage_recv.at[stage], at(1))

    def stage_end(stage):
        n, _ = stages[stage]
        stage_total(stage).wait_recv()
        value = rows[stage]
        for k in range(1, n):
            value = jnp.maximum(value, slots[stage][k - 1])
        return value

    def to_root(root):
        return send(
            rows.at[2],
            slots2.at[(root - plane + planes) % planes - 1],
            stage_send.at[2],
            stage_recv.at[2],
            (s, root * inner_c + c % inner_c),
        )

    for root in range(roots):

        @pl.when(plane != root)
        def _(root=root):
            to_root(root).start()

    load_now.wait()
    load_inflow.wait()

    lane = lax.broadcasted_iota(jnp.int32, (8, 128), 1)
    place = lane % 16
    group = lane // 16

    def pack(y, packed):
        packed = list(packed)
        for k, value in enumerate(across_rows(now_rows, y)):
            packed[k] = jnp.where(group == y, pltpu.roll(value, 16 * y + 5, 1), packed[k])
        return tuple(packed)

    packed = (jnp.zeros((8, 128), jnp.float32),) * 7
    for y in range(8):
        packed = pack(y, packed)
    for k in range(7):
        a_own[k] = packed[k]

    copies = [
        send(now.at[:, :, 0:3], halo.at[:, :, 0:3], halo_send.at[0], halo_recv.at[0], below),
        send(now.at[:, :, 5:8], halo.at[:, :, 5:8], halo_send.at[1], halo_recv.at[1], above),
        send(a_own, a_right, halo_send.at[2], halo_recv.at[2], left),
        send(a_own, a_left, halo_send.at[3], halo_recv.at[3], right),
    ]
    for copy in copies:
        copy.start()

    def own_prim(y, _):
        for k, value in enumerate(primitive(across_rows(now_rows, y))):
            prim[k, y + 3] = value
        return 0

    lax.fori_loop(0, 8, own_prim, 0)

    def local(y, _):
        w = all_of(prim, y + 3)
        across = folded(spread(along(w, 0, 2), 0), w[6])
        keep = (lane >= 3) & (lane <= 125)
        stream = folded(spread(along(w, 1, 0), 1, keep), w[6])
        for k in range(7):
            acc[k, y + 1] = across[k] + stream[k]
        return 0

    lax.fori_loop(0, 8, local, 0)

    def fixed_part(z, _):
        for k in range(7):
            part_ref[k, z] = base[k, z] * (1.0 / 3.0) + now[k, z] * (2.0 / 3.0)
        return 0

    lax.fori_loop(0, 8, fixed_part, 0)

    @pl.when(is_root)
    def _():
        rows[1] = stage_end(2)
        stage_start(1)
        rows[0] = stage_end(1)
        stage_start(0)

    for copy in copies:
        copy.wait_recv()

    @pl.when(s == 0)
    def _():
        for k in range(7):
            value = jnp.zeros((8, 128), jnp.float32)
            for layer in range(3):
                for y in range(8):
                    one = jnp.broadcast_to(inflow[k, layer][:, y : y + 1], (8, 128))
                    value = jnp.where((group == y) & (place == 2 + layer), one, value)
            a_left[k] = value

    @pl.when(s == size_s - 1)
    def _():
        for k in range(7):
            value = a_own[k]
            one, two, three = (rolled(value, 1, 1), rolled(value, 2, 1), rolled(value, 3, 1))
            a_right[k] = jnp.where(place == 5, one, jnp.where(place == 6, two, three))

    rim = []
    for k in range(7):
        own = a_own[k]
        late = rolled(jnp.where(place < 5, a_left[k], own), 6, 1)
        rim.append(jnp.where(place < 5, own, jnp.where(place < 8, a_right[k], late)))
    w = primitive(rim)
    keep = ((place >= 3) & (place <= 5)) | ((place >= 11) & (place <= 13))
    ends = folded(spread(along(w, 1, 0), 1, keep), w[6])
    for k in range(7):
        edge[k] = jnp.where(place < 5, ends[k], rolled(ends[k], -6, 1))

    def halo_prim(i, _):
        row = i + i // 3 * 8
        for k, value in enumerate(primitive(across_rows(halo_rows, (i + 5) % 8))):
            prim[k, row] = value
        return 0

    lax.fori_loop(0, 6, halo_prim, 0)

    def cell_edges(y):
        upper, lower = ([], [])
        for k in range(7):
            f, g, h, up, far = (prim[k, y + i] for i in range(1, 6))
            one, two = edges(h, g - f, h - g, up - h, far - up)
            upper.append(one)
            lower.append(two)
        return (upper, lower)

    for k, value in enumerate(cell_edges(-1)[0]):
        xr[k] = value
    for k in range(8):
        flux_prev[k] = jnp.zeros((8, 128), jnp.float32)
    for k in range(7):
        acc[k, 0] = jnp.zeros((8, 128), jnp.float32)

    def face(j, _):
        upper, lower = cell_edges(j)
        before = all_of(xr)
        for k in range(7):
            xr[k] = upper[k]
        lower_cell = all_of(prim, j + 2)
        flux = fluxes(before, lower, lower_cell, all_of(prim, j + 3), 1)
        change = [flux[k] - flux_prev[k] for k in range(8)]
        for k in range(8):
            flux_prev[k] = flux[k]
        for k, value in enumerate(folded(change, lower_cell[6])):
            acc[k, j] = acc[k, j] + value
        return 0

    lax.fori_loop(0, 9, face, 0)

    near = (lane >= 125) | (lane <= 2)
    for k in range(7):
        for y in range(8):
            extra = jnp.where(near, rolled(edge[k], 123 - 16 * y, 1), 0.0)
            rate_ref[k, pl.ds(y, 8, stride=8), :] = (acc[k, y + 1] + extra) * (-1.0 / 3.0)

    children = [
        send(
            rows.at[3],
            told.at[0],
            stage_send.at[3],
            stage_recv.at[3],
            (s, (c + k * roots * inner_c) % size_c),
        )
        for k in range(1, planes // roots)
    ]

    @pl.when(is_root)
    def _():
        rows[3] = stage_end(0)
        for copy in children:
            copy.start()
        fast_ref[...] = rows[3]

    @pl.when(jnp.logical_not(is_root))
    def _():
        children[0].wait_recv()
        fast_ref[...] = told[0]

    for copy in copies:
        copy.wait_send()

    def sent(count, stage):
        span = slots2.at[pl.ds(0, count)]
        send(span, span, stage_send.at[stage], stage_recv.at[stage], right).wait_send()

    @pl.when(is_root)
    def _():
        for stage in range(2):
            stage_total(stage).wait_send()
        if roots > 1:
            sent(roots - 1, 2)
        sent(planes // roots - 1, 3)

    @pl.when(jnp.logical_not(is_root))
    def _():
        sent(roots, 2)


def shards(sizes, state_now, state_base, inflow):
    size = jnp.float32
    n0, n1, n2 = (sizes[0], sizes[1] * sizes[2], sizes[3])
    inflow_t = jnp.transpose(inflow, (0, 3, 1, 2))
    part, rate, fast = pl.pallas_call(
        functools.partial(kernel, sizes),
        out_shape=(
            jax.ShapeDtypeStruct((7, 8, 8, 128), size),
            jax.ShapeDtypeStruct((7, 64, 128), size),
            jax.ShapeDtypeStruct((1, 128), size),
        ),
        in_specs=[pl.BlockSpec(memory_space=pltpu.HBM)] * 3,
        out_specs=(pl.BlockSpec(memory_space=pltpu.VMEM),) * 3,
        scratch_shapes=[
            pltpu.VMEM((7, 8, 8, 128), size),
            pltpu.VMEM((7, 8, 8, 128), size),
            pltpu.VMEM((7, 8, 8, 128), size),
            pltpu.VMEM((7, 3, 8, 8), size),
            pltpu.VMEM((7, 14, 8, 128), size),
            pltpu.VMEM((7, 8, 128), size),
            pltpu.VMEM((8, 8, 128), size),
            pltpu.VMEM((7, 9, 8, 128), size),
            pltpu.VMEM((7, 8, 128), size),
            pltpu.VMEM((7, 8, 128), size),
            pltpu.VMEM((7, 8, 128), size),
            pltpu.VMEM((7, 8, 128), size),
            pltpu.VMEM((4, 1, 128), size),
            pltpu.VMEM((n0 - 1, 1, 128), size),
            pltpu.VMEM((n1 - 1, 1, 128), size),
            pltpu.VMEM((n2 - 1, 1, 128), size),
            pltpu.VMEM((1, 1, 128), size),
            pltpu.SemaphoreType.DMA((3,)),
            pltpu.SemaphoreType.DMA((4,)),
            pltpu.SemaphoreType.DMA((4,)),
            pltpu.SemaphoreType.DMA((4,)),
            pltpu.SemaphoreType.DMA((4,)),
        ],
        compiler_params=pltpu.CompilerParams(
            collective_id=0, has_side_effects=True, vmem_limit_bytes=32 * 1024 * 1024
        ),
    )(
        pltpu.with_memory_space_constraint(state_now, pltpu.HBM),
        pltpu.with_memory_space_constraint(state_base, pltpu.HBM),
        pltpu.with_memory_space_constraint(inflow_t, pltpu.HBM),
    )
    return part + 0.3 / fast[0, 0] * rate.reshape(state_now.shape)


def solution(mesh):
    stream, cross = (mesh.shape["stream"], mesh.shape["cross"])
    sizes = (8, 4, 2, 12) if (stream, cross) == (16, 48) else (2, 2, stream // 2, cross // 2)
    return jax.shard_map(
        functools.partial(shards, sizes),
        mesh=mesh,
        in_specs=(
            P(None, None, "cross", "stream"),
            P(None, None, "cross", "stream"),
            P(None, None, "cross", None),
        ),
        out_specs=P(None, None, "cross", "stream"),
        check_vma=False,
    )
```

```python
import functools

import jax
import jax.numpy as jnp
from jax import lax
from jax.experimental import pallas as pl
from jax.experimental.pallas import tpu as pltpu
from jax.sharding import PartitionSpec as P

MESH = pl.DeviceIdType.MESH

gas_part = 1.0 / 0.4
liquid_part = 1.0 / 3.4
stiff_part = 4.4 * 0.6 / 3.4


def inverse(value):
    guess = pl.reciprocal(value, approx=True)
    return guess * (2.0 - value * guess)


def mixture(volume):
    rest = 1.0 - volume
    return (volume * gas_part + rest * liquid_part, rest * stiff_part)


def primitive(u):
    over = 1.0 / (u[0] + u[1])
    vx, vy, vz = (u[2] * over, u[3] * over, u[4] * over)
    kinetic = 0.5 * (u[2] * vx + u[3] * vy + u[4] * vz)
    gamma, stiff = mixture(u[6])
    return (u[0], u[1], vx, vy, vz, (u[5] - kinetic - stiff) / gamma, u[6])


def sound(density, pressure, gamma, stiff):
    return jnp.sqrt(((gamma + 1.0) * pressure + stiff) / (gamma * density))


def edges(h, d1, d2, d3, d4):
    e1, e2, e3 = (d2 - d1, d3 - d2, d4 - d3)
    u0 = e1 + d2 + d2
    u1 = d2 + d3
    u2 = e3 - d3 - d3
    third = 13.0 / 3.0
    top = 1e30
    s0 = jnp.minimum(third * (e1 * e1) + u0 * u0 + 4e-6, top)
    s1 = jnp.minimum(third * (e2 * e2) + u1 * u1 + 4e-6, top)
    s2 = jnp.minimum(third * (e3 * e3) + u2 * u2 + 4e-6, top)
    r0, r1, r2 = (inverse(s0), inverse(s1), inverse(s2))
    a0, a1, a2 = (r0 * r0, 6.0 * (r1 * r1), r2 * r2)
    b0, b2 = (3.0 * a0, 3.0 * a2)
    up = a0 * (u0 + e1 + d2) + a1 * (u1 + d3) + b2 * (d3 - u2)
    down = a2 * (u2 + e3 - d3) - a1 * (u1 + d2) - b0 * (u0 + d2)
    upper = h + up * inverse(6.0 * (a0 + a1 + b2))
    lower = h + down * inverse(6.0 * (a2 + a1 + b0))
    return (upper, lower)


def limited(face, lower_cell, upper_cell):
    out = []
    for c in range(7):
        value = face[c]
        if c in (0, 1, 5):
            value = jnp.maximum(value, 0.5 * jnp.minimum(lower_cell[c], upper_cell[c]))
        elif c == 6:
            value = jnp.maximum(value, 0.5 * jnp.minimum(lower_cell[c], upper_cell[c]))
            value = jnp.minimum(value, 0.5 + 0.5 * jnp.maximum(lower_cell[c], upper_cell[c]))
        out.append(value)
    return out


def side(w, normal):
    density = w[0] + w[1]
    gamma, stiff = mixture(w[6])
    momentum = [density * w[2], density * w[3], density * w[4]]
    energy = (
        gamma * w[5]
        + stiff
        + 0.5 * (momentum[0] * w[2] + momentum[1] * w[3] + momentum[2] * w[4])
    )
    vn = w[2 + normal]
    amounts = [w[0], w[1], *momentum, energy, w[6]]
    moved = [amount * vn for amount in amounts]
    moved[2 + normal] = moved[2 + normal] + w[5]
    moved[5] = moved[5] + w[5] * vn
    signal = jnp.abs(vn) + sound(density, w[5], gamma, stiff)
    return (amounts, moved, vn, signal)


def fluxes(left, right, lower_cell, upper_cell, normal):
    one = side(limited(left, lower_cell, upper_cell), normal)
    two = side(limited(right, lower_cell, upper_cell), normal)
    fastest = jnp.maximum(one[3], two[3])
    out = [
        (fl + fr) - fastest * (ur - ul)
        for ul, ur, fl, fr in zip(one[0], two[0], one[1], two[1])
    ]
    return out + [one[2] + two[2]]


def rolled(value, shift, axis):
    return pltpu.roll(value, shift % value.shape[axis], axis)


def along(w, axis, normal):
    upper, lower, before = ([], [], [])
    for c in range(7):
        h = w[c]
        g = rolled(h, 1, axis)
        d2 = h - g
        d1, d3, d4 = (rolled(d2, 1, axis), rolled(d2, -1, axis), rolled(d2, -2, axis))
        up, down = edges(h, d1, d2, d3, d4)
        upper.append(rolled(up, 1, axis))
        lower.append(down)
        before.append(g)
    return fluxes(upper, lower, before, w, normal)


def spread(flux, axis, keep=None):
    if keep is not None:
        flux = [jnp.where(keep, f, 0.0) for f in flux]
    return [rolled(f, -1, axis) - f for f in flux]


def folded(change, volume):
    return change[:6] + [change[6] - volume * change[7]]


def ring(stage, sizes):
    inner_s, inner_c, outer_s, outer_c = sizes
    s, c = (lax.axis_index("stream"), lax.axis_index("cross"))
    if stage == 0:
        base = s // inner_s * inner_s
        return inner_s, lambda k: (base + (s - base + k) % inner_s, c)
    if stage == 1:
        n = outer_s * inner_c
        place = s // inner_s * inner_c + c % inner_c

        def at(k):
            there = (place + k) % n
            return (
                there // inner_c * inner_s + s % inner_s,
                c // inner_c * inner_c + there % inner_c,
            )

        return n, at
    return outer_c, lambda k: (s, (c + k * inner_c) % (outer_c * inner_c))


def far_first(n):
    return sorted(range(1, n), key=lambda k: -min(k, n - k))


def send(source, target, send_sem, recv_sem, to):
    return pltpu.make_async_remote_copy(
        src_ref=source,
        dst_ref=target,
        send_sem=send_sem,
        recv_sem=recv_sem,
        device_id=to,
        device_id_type=MESH,
    )


def kernel(
    sizes,
    now_ref,
    base_ref,
    inflow_ref,
    part_ref,
    rate_ref,
    fast_ref,
    now,
    base,
    halo,
    inflow,
    prim,
    xr,
    flux_prev,
    acc,
    a_own,
    a_left,
    a_right,
    edge,
    rows,
    slots0,
    slots1,
    slots2,
    told,
    in_sems,
    halo_send,
    halo_recv,
    stage_send,
    stage_recv,
):
    size_s, size_c = (sizes[0] * sizes[2], sizes[1] * sizes[3])
    s, c = (lax.axis_index("stream"), lax.axis_index("cross"))
    left, right = (((s + size_s - 1) % size_s, c), ((s + 1) % size_s, c))
    below, above = ((s, (c + size_c - 1) % size_c), (s, (c + 1) % size_c))
    slots = (slots0, slots1, slots2)
    stages = [ring(k, sizes) for k in range(3)]
    inner_c, planes = (sizes[1], sizes[3])
    roots = max(1, planes // 3)
    plane = c // inner_c
    is_root = plane < roots

    load_base = pltpu.make_async_copy(base_ref, base, in_sems.at[0])
    load_now = pltpu.make_async_copy(now_ref, now, in_sems.at[1])
    load_inflow = pltpu.make_async_copy(inflow_ref, inflow, in_sems.at[2])
    load_base.start()
    load_now.start()
    load_inflow.start()

    barrier = pltpu.get_barrier_semaphore()

    def greet(there):
        pl.semaphore_signal(barrier, inc=1, device_id=there, device_id_type=MESH)

    first_s, last_s = (s % sizes[0] == 0, s % sizes[0] == sizes[0] - 1)
    first_c, last_c = (c % inner_c == 0, c % inner_c == inner_c - 1)
    flip = s // sizes[0] > 0
    answer_left = first_s
    answer_above = last_c & flip
    answer_below = first_c & jnp.logical_not(flip)
    greet(left)
    pl.when(jnp.logical_not(last_s))(lambda: greet(right))
    pl.when(jnp.logical_not(first_c & flip))(lambda: greet(below))
    pl.when(jnp.logical_not(last_c & jnp.logical_not(flip)))(lambda: greet(above))
    greeted = (
        1
        + jnp.where(answer_left, 0, 1)
        + jnp.where(answer_above, 0, 1)
        + jnp.where(answer_below, 0, 1)
    )

    @pl.when(is_root)
    def _():
        for stage in (2, 1, 0):
            n, at = stages[stage]
            for k in far_first(n):
                greet(at(k))

    now_rows = now.reshape(7, 64, 128)
    halo_rows = halo.reshape(7, 64, 128)

    def across_rows(ref, y):
        return [ref[k, pl.ds(y, 8, stride=8), :] for k in range(7)]

    def all_of(ref, *index):
        return [ref[(k, *index)] for k in range(7)]

    def speed(y, most):
        w = primitive(all_of(base, y))
        gamma, stiff = mixture(w[6])
        swift = jnp.maximum(jnp.maximum(jnp.abs(w[2]), jnp.abs(w[3])), jnp.abs(w[4]))
        return jnp.maximum(most, swift + sound(w[0] + w[1], w[5], gamma, stiff))

    load_base.wait()
    most = jnp.zeros((8, 128), jnp.float32)
    for y in range(8):
        most = speed(y, most)
    rows[2] = jnp.broadcast_to(jnp.max(most, keepdims=True), (1, 128))
    def stage_start(stage):
        n, at = stages[stage]
        for k in far_first(n):
            send(
                rows.at[stage],
                slots[stage].at[k - 1],
                stage_send.at[stage],
                stage_recv.at[stage],
                at(k),
            ).start()

    def stage_total(stage):
        n, at = stages[stage]
        return send(slots[stage], slots[stage], stage_send.at[stage], stage_recv.at[stage], at(1))

    def stage_end(stage):
        n, _ = stages[stage]
        stage_total(stage).wait_recv()
        value = rows[stage]
        for k in range(1, n):
            value = jnp.maximum(value, slots[stage][k - 1])
        return value

    def to_root(root):
        return send(
            rows.at[2],
            slots2.at[(root - plane + planes) % planes - 1],
            stage_send.at[2],
            stage_recv.at[2],
            (s, root * inner_c + c % inner_c),
        )

    load_now.wait()
    load_inflow.wait()

    lane = lax.broadcasted_iota(jnp.int32, (8, 128), 1)
    place = lane % 16
    group = lane // 16

    def pack(y, packed):
        packed = list(packed)
        for k, value in enumerate(across_rows(now_rows, y)):
            packed[k] = jnp.where(group == y, pltpu.roll(value, 16 * y + 5, 1), packed[k])
        return tuple(packed)

    packed = (jnp.zeros((8, 128), jnp.float32),) * 7
    for y in range(8):
        packed = pack(y, packed)
    for k in range(7):
        a_own[k] = packed[k]

    copies = [
        send(now.at[:, :, 0:3], halo.at[:, :, 0:3], halo_send.at[0], halo_recv.at[0], below),
        send(now.at[:, :, 5:8], halo.at[:, :, 5:8], halo_send.at[1], halo_recv.at[1], above),
        send(a_own, a_right, halo_send.at[2], halo_recv.at[2], left),
        send(a_own, a_left, halo_send.at[3], halo_recv.at[3], right),
    ]
    def own_prim(y, _):
        for k, value in enumerate(primitive(across_rows(now_rows, y))):
            prim[k, y + 3] = value
        return 0

    def local(y, _):
        w = all_of(prim, y + 3)
        across = folded(spread(along(w, 0, 2), 0), w[6])
        keep = (lane >= 3) & (lane <= 125)
        stream = folded(spread(along(w, 1, 0), 1, keep), w[6])
        for k in range(7):
            acc[k, y + 1] = across[k] + stream[k]
        return 0

    def fixed_part(z, _):
        for k in range(7):
            part_ref[k, z] = base[k, z] * (1.0 / 3.0) + now[k, z] * (2.0 / 3.0)
        return 0

    def at_home():
        lax.fori_loop(0, 8, own_prim, 0)
        lax.fori_loop(0, 8, local, 0)
        lax.fori_loop(0, 8, fixed_part, 0)

    pl.when(is_root)(at_home)

    @pl.when(is_root)
    def _():
        pl.semaphore_wait(barrier, greeted + roots - 1 + stages[1][0] - 1 + stages[0][0] - 1)

    @pl.when(jnp.logical_not(is_root))
    def _():
        pl.semaphore_wait(barrier, greeted + roots)

    for root in range(roots):

        @pl.when(plane != root)
        def _(root=root):
            to_root(root).start()

    copies[3].start()
    pl.when(jnp.logical_not(answer_left))(copies[2].start)
    pl.when(jnp.logical_not(answer_above))(copies[1].start)
    pl.when(jnp.logical_not(answer_below))(copies[0].start)

    pl.when(jnp.logical_not(is_root))(at_home)

    @pl.when(answer_below)
    def _():
        copies[1].wait_recv()
        copies[0].start()

    @pl.when(answer_above)
    def _():
        copies[0].wait_recv()
        copies[1].start()

    @pl.when(answer_left)
    def _():
        copies[3].wait_recv()
        copies[2].start()

    @pl.when(is_root)
    def _():
        rows[1] = stage_end(2)
        stage_start(1)

    @pl.when(is_root)
    def _():
        rows[0] = stage_end(1)
        stage_start(0)

    pl.when(jnp.logical_not(answer_below))(copies[1].wait_recv)
    pl.when(jnp.logical_not(answer_above))(copies[0].wait_recv)

    def halo_prim(i, _):
        row = i + i // 3 * 8
        for k, value in enumerate(primitive(across_rows(halo_rows, (i + 5) % 8))):
            prim[k, row] = value
        return 0

    lax.fori_loop(0, 6, halo_prim, 0)

    def cell_edges(y):
        upper, lower = ([], [])
        for k in range(7):
            f, g, h, up, far = (prim[k, y + i] for i in range(1, 6))
            one, two = edges(h, g - f, h - g, up - h, far - up)
            upper.append(one)
            lower.append(two)
        return (upper, lower)

    for k, value in enumerate(cell_edges(-1)[0]):
        xr[k] = value
    for k in range(8):
        flux_prev[k] = jnp.zeros((8, 128), jnp.float32)
    for k in range(7):
        acc[k, 0] = jnp.zeros((8, 128), jnp.float32)

    def face(j, _):
        upper, lower = cell_edges(j)
        before = all_of(xr)
        for k in range(7):
            xr[k] = upper[k]
        lower_cell = all_of(prim, j + 2)
        flux = fluxes(before, lower, lower_cell, all_of(prim, j + 3), 1)
        change = [flux[k] - flux_prev[k] for k in range(8)]
        for k in range(8):
            flux_prev[k] = flux[k]
        for k, value in enumerate(folded(change, lower_cell[6])):
            acc[k, j] = acc[k, j] + value
        return 0

    lax.fori_loop(0, 9, face, 0)

    copies[2].wait_recv()
    pl.when(jnp.logical_not(answer_left))(copies[3].wait_recv)

    @pl.when(s == 0)
    def _():
        for k in range(7):
            value = jnp.zeros((8, 128), jnp.float32)
            for layer in range(3):
                for y in range(8):
                    one = jnp.broadcast_to(inflow[k, layer][:, y : y + 1], (8, 128))
                    value = jnp.where((group == y) & (place == 2 + layer), one, value)
            a_left[k] = value

    @pl.when(s == size_s - 1)
    def _():
        for k in range(7):
            value = a_own[k]
            one, two, three = (rolled(value, 1, 1), rolled(value, 2, 1), rolled(value, 3, 1))
            a_right[k] = jnp.where(place == 5, one, jnp.where(place == 6, two, three))

    rim = []
    for k in range(7):
        own = a_own[k]
        late = rolled(jnp.where(place < 5, a_left[k], own), 6, 1)
        rim.append(jnp.where(place < 5, own, jnp.where(place < 8, a_right[k], late)))
    w = primitive(rim)
    keep = ((place >= 3) & (place <= 5)) | ((place >= 11) & (place <= 13))
    ends = folded(spread(along(w, 1, 0), 1, keep), w[6])
    for k in range(7):
        edge[k] = jnp.where(place < 5, ends[k], rolled(ends[k], -6, 1))

    near = (lane >= 125) | (lane <= 2)
    for k in range(7):
        for y in range(8):
            extra = jnp.where(near, rolled(edge[k], 123 - 16 * y, 1), 0.0)
            rate_ref[k, pl.ds(y, 8, stride=8), :] = (acc[k, y + 1] + extra) * (-1.0 / 3.0)

    children = [
        send(
            rows.at[3],
            told.at[0],
            stage_send.at[3],
            stage_recv.at[3],
            (s, (c + k * inner_c) % size_c),
        )
        for k in range(1, planes - roots + 1)
    ]

    @pl.when(is_root)
    def _():
        fastest = stage_end(0)
        rows[3] = fastest
        fast_ref[...] = fastest

    @pl.when(plane == roots - 1)
    def _():
        for copy in children:
            copy.start()

    @pl.when(jnp.logical_not(is_root))
    def _():
        children[0].wait_recv()
        fast_ref[...] = told[0]

    for copy in copies:
        copy.wait_send()

    def sent(count, stage):
        span = slots2.at[pl.ds(0, count)]
        send(span, span, stage_send.at[stage], stage_recv.at[stage], right).wait_send()

    @pl.when(is_root)
    def _():
        for stage in range(2):
            stage_total(stage).wait_send()
        if roots > 1:
            sent(roots - 1, 2)

    @pl.when(plane == roots - 1)
    def _():
        sent(planes - roots, 3)

    @pl.when(jnp.logical_not(is_root))
    def _():
        sent(roots, 2)


def shards(sizes, state_now, state_base, inflow):
    size = jnp.float32
    n0, n1, n2 = (sizes[0], sizes[1] * sizes[2], sizes[3])
    inflow_t = jnp.transpose(inflow, (0, 3, 1, 2))
    part, rate, fast = pl.pallas_call(
        functools.partial(kernel, sizes),
        out_shape=(
            jax.ShapeDtypeStruct((7, 8, 8, 128), size),
            jax.ShapeDtypeStruct((7, 64, 128), size),
            jax.ShapeDtypeStruct((1, 128), size),
        ),
        in_specs=[pl.BlockSpec(memory_space=pltpu.HBM)] * 3,
        out_specs=(pl.BlockSpec(memory_space=pltpu.VMEM),) * 3,
        scratch_shapes=[
            pltpu.VMEM((7, 8, 8, 128), size),
            pltpu.VMEM((7, 8, 8, 128), size),
            pltpu.VMEM((7, 8, 8, 128), size),
            pltpu.VMEM((7, 3, 8, 8), size),
            pltpu.VMEM((7, 14, 8, 128), size),
            pltpu.VMEM((7, 8, 128), size),
            pltpu.VMEM((8, 8, 128), size),
            pltpu.VMEM((7, 9, 8, 128), size),
            pltpu.VMEM((7, 8, 128), size),
            pltpu.VMEM((7, 8, 128), size),
            pltpu.VMEM((7, 8, 128), size),
            pltpu.VMEM((7, 8, 128), size),
            pltpu.VMEM((4, 1, 128), size),
            pltpu.VMEM((n0 - 1, 1, 128), size),
            pltpu.VMEM((n1 - 1, 1, 128), size),
            pltpu.VMEM((n2 - 1, 1, 128), size),
            pltpu.VMEM((1, 1, 128), size),
            pltpu.SemaphoreType.DMA((3,)),
            pltpu.SemaphoreType.DMA((4,)),
            pltpu.SemaphoreType.DMA((4,)),
            pltpu.SemaphoreType.DMA((4,)),
            pltpu.SemaphoreType.DMA((4,)),
        ],
        compiler_params=pltpu.CompilerParams(
            collective_id=0, has_side_effects=True, vmem_limit_bytes=32 * 1024 * 1024
        ),
    )(
        pltpu.with_memory_space_constraint(state_now, pltpu.HBM),
        pltpu.with_memory_space_constraint(state_base, pltpu.HBM),
        pltpu.with_memory_space_constraint(inflow_t, pltpu.HBM),
    )
    return part + 0.3 / fast[0, 0] * rate.reshape(state_now.shape)


def solution(mesh):
    stream, cross = (mesh.shape["stream"], mesh.shape["cross"])
    sizes = (8, 4, 2, 12) if (stream, cross) == (16, 48) else (2, 2, stream // 2, cross // 2)
    return jax.shard_map(
        functools.partial(shards, sizes),
        mesh=mesh,
        in_specs=(
            P(None, None, "cross", "stream"),
            P(None, None, "cross", "stream"),
            P(None, None, "cross", None),
        ),
        out_specs=P(None, None, "cross", "stream"),
        check_vma=False,
    )
```

```python
import functools

import jax
import jax.numpy as jnp
from jax import lax
from jax.experimental import pallas as pl
from jax.experimental.pallas import tpu as pltpu
from jax.sharding import PartitionSpec as P

MESH = pl.DeviceIdType.MESH

gas_part = 1.0 / 0.4
liquid_part = 1.0 / 3.4
stiff_part = 4.4 * 0.6 / 3.4


def inverse(value):
    guess = pl.reciprocal(value, approx=True)
    return guess * (2.0 - value * guess)


def mixture(volume):
    rest = 1.0 - volume
    return (volume * gas_part + rest * liquid_part, rest * stiff_part)


def primitive(u):
    over = 1.0 / (u[0] + u[1])
    vx, vy, vz = (u[2] * over, u[3] * over, u[4] * over)
    kinetic = 0.5 * (u[2] * vx + u[3] * vy + u[4] * vz)
    gamma, stiff = mixture(u[6])
    return (u[0], u[1], vx, vy, vz, (u[5] - kinetic - stiff) / gamma, u[6])


def sound(density, pressure, gamma, stiff):
    return jnp.sqrt(((gamma + 1.0) * pressure + stiff) / (gamma * density))


def edges(h, d1, d2, d3, d4):
    e1, e2, e3 = (d2 - d1, d3 - d2, d4 - d3)
    u0 = e1 + d2 + d2
    u1 = d2 + d3
    u2 = e3 - d3 - d3
    third = 13.0 / 3.0
    top = 1e30
    s0 = jnp.minimum(third * (e1 * e1) + u0 * u0 + 4e-6, top)
    s1 = jnp.minimum(third * (e2 * e2) + u1 * u1 + 4e-6, top)
    s2 = jnp.minimum(third * (e3 * e3) + u2 * u2 + 4e-6, top)
    r0, r1, r2 = (inverse(s0), inverse(s1), inverse(s2))
    a0, a1, a2 = (r0 * r0, 6.0 * (r1 * r1), r2 * r2)
    b0, b2 = (3.0 * a0, 3.0 * a2)
    up = a0 * (u0 + e1 + d2) + a1 * (u1 + d3) + b2 * (d3 - u2)
    down = a2 * (u2 + e3 - d3) - a1 * (u1 + d2) - b0 * (u0 + d2)
    upper = h + up * inverse(6.0 * (a0 + a1 + b2))
    lower = h + down * inverse(6.0 * (a2 + a1 + b0))
    return (upper, lower)


def limited(face, lower_cell, upper_cell):
    out = []
    for c in range(7):
        value = face[c]
        if c in (0, 1, 5):
            value = jnp.maximum(value, 0.5 * jnp.minimum(lower_cell[c], upper_cell[c]))
        elif c == 6:
            value = jnp.maximum(value, 0.5 * jnp.minimum(lower_cell[c], upper_cell[c]))
            value = jnp.minimum(value, 0.5 + 0.5 * jnp.maximum(lower_cell[c], upper_cell[c]))
        out.append(value)
    return out


def side(w, normal):
    density = w[0] + w[1]
    gamma, stiff = mixture(w[6])
    momentum = [density * w[2], density * w[3], density * w[4]]
    energy = (
        gamma * w[5]
        + stiff
        + 0.5 * (momentum[0] * w[2] + momentum[1] * w[3] + momentum[2] * w[4])
    )
    vn = w[2 + normal]
    amounts = [w[0], w[1], *momentum, energy, w[6]]
    moved = [amount * vn for amount in amounts]
    moved[2 + normal] = moved[2 + normal] + w[5]
    moved[5] = moved[5] + w[5] * vn
    signal = jnp.abs(vn) + sound(density, w[5], gamma, stiff)
    return (amounts, moved, vn, signal)


def fluxes(left, right, lower_cell, upper_cell, normal):
    one = side(limited(left, lower_cell, upper_cell), normal)
    two = side(limited(right, lower_cell, upper_cell), normal)
    fastest = jnp.maximum(one[3], two[3])
    out = [
        (fl + fr) - fastest * (ur - ul)
        for ul, ur, fl, fr in zip(one[0], two[0], one[1], two[1])
    ]
    return out + [one[2] + two[2]]


def rolled(value, shift, axis):
    return pltpu.roll(value, shift % value.shape[axis], axis)


def along(w, axis, normal):
    upper, lower, before = ([], [], [])
    for c in range(7):
        h = w[c]
        g = rolled(h, 1, axis)
        d2 = h - g
        d1, d3, d4 = (rolled(d2, 1, axis), rolled(d2, -1, axis), rolled(d2, -2, axis))
        up, down = edges(h, d1, d2, d3, d4)
        upper.append(rolled(up, 1, axis))
        lower.append(down)
        before.append(g)
    return fluxes(upper, lower, before, w, normal)


def spread(flux, axis, keep=None):
    if keep is not None:
        flux = [jnp.where(keep, f, 0.0) for f in flux]
    return [rolled(f, -1, axis) - f for f in flux]


def folded(change, volume):
    return change[:6] + [change[6] - volume * change[7]]


def ring(stage, sizes):
    inner_s, inner_c, outer_s, outer_c = sizes
    s, c = (lax.axis_index("stream"), lax.axis_index("cross"))
    if stage == 0:
        base = s // inner_s * inner_s
        return inner_s, lambda k: (base + (s - base + k) % inner_s, c)
    if stage == 1:
        n = outer_s * inner_c
        place = s // inner_s * inner_c + c % inner_c

        def at(k):
            there = (place + k) % n
            return (
                there // inner_c * inner_s + s % inner_s,
                c // inner_c * inner_c + there % inner_c,
            )

        return n, at
    return outer_c, lambda k: (s, (c + k * inner_c) % (outer_c * inner_c))


def far_first(n):
    return sorted(range(1, n), key=lambda k: -min(k, n - k))


def send(source, target, send_sem, recv_sem, to):
    return pltpu.make_async_remote_copy(
        src_ref=source,
        dst_ref=target,
        send_sem=send_sem,
        recv_sem=recv_sem,
        device_id=to,
        device_id_type=MESH,
    )


def kernel(
    sizes,
    now_ref,
    base_ref,
    inflow_ref,
    part_ref,
    rate_ref,
    step_ref,
    now,
    base,
    halo,
    inflow,
    prim,
    xr,
    flux_prev,
    acc,
    a_own,
    a_left,
    a_right,
    edge,
    rows,
    slots0,
    slots1,
    slots2,
    told,
    quick,
    in_sems,
    halo_send,
    halo_recv,
    stage_send,
    stage_recv,
):
    size_s, size_c = (sizes[0] * sizes[2], sizes[1] * sizes[3])
    s, c = (lax.axis_index("stream"), lax.axis_index("cross"))
    left, right = (((s + size_s - 1) % size_s, c), ((s + 1) % size_s, c))
    below, above = ((s, (c + size_c - 1) % size_c), (s, (c + 1) % size_c))
    slots = (slots0, slots1, slots2)
    stages = [ring(k, sizes) for k in range(3)]
    inner_c, planes = (sizes[1], sizes[3])
    roots = max(1, planes // 3)
    plane = c // inner_c
    is_root = plane < roots

    load_base = pltpu.make_async_copy(base_ref, base, in_sems.at[0])
    load_now = pltpu.make_async_copy(now_ref, now, in_sems.at[1])
    load_inflow = pltpu.make_async_copy(inflow_ref, inflow, in_sems.at[2])
    load_base.start()
    load_now.start()
    load_inflow.start()

    barrier = pltpu.get_barrier_semaphore()

    def greet(there):
        pl.semaphore_signal(barrier, inc=1, device_id=there, device_id_type=MESH)

    first_s, last_s = (s % sizes[0] == 0, s % sizes[0] == sizes[0] - 1)
    first_c, last_c = (c % inner_c == 0, c % inner_c == inner_c - 1)
    flip = s // sizes[0] > 0
    answer_left = first_s
    answer_above = last_c & flip
    answer_below = first_c & jnp.logical_not(flip)
    chief_s, chief_c = (1, 0)
    in_first = plane == 0
    is_chief = (s == chief_s) & (c == chief_c)
    serves_chief = in_first & jnp.logical_not(is_chief)
    beside_chief = serves_chief & (s // sizes[0] == chief_s // sizes[0]) & (c == chief_c)
    members = size_s * inner_c

    greet(left)
    pl.when(jnp.logical_not(last_s))(lambda: greet(right))
    pl.when(jnp.logical_not(first_c & flip))(lambda: greet(below))
    pl.when(jnp.logical_not(last_c & jnp.logical_not(flip)))(lambda: greet(above))

    @pl.when(is_chief)
    def _():
        def greet_member(k, _):
            pl.when(k != chief_s * inner_c + chief_c)(lambda: greet((k // inner_c, k % inner_c)))
            return 0

        lax.fori_loop(0, members, greet_member, 0)

    greeted = (
        1
        + jnp.where(serves_chief, 1, 0)
        + jnp.where(answer_left, 0, 1)
        + jnp.where(answer_above, 0, 1)
        + jnp.where(answer_below, 0, 1)
    )

    @pl.when(is_root)
    def _():
        for stage in (2, 1, 0):
            n, at = stages[stage]
            for k in far_first(n):
                greet(at(k))

    now_rows = now.reshape(7, 64, 128)
    halo_rows = halo.reshape(7, 64, 128)

    def across_rows(ref, y):
        return [ref[k, pl.ds(y, 8, stride=8), :] for k in range(7)]

    def all_of(ref, *index):
        return [ref[(k, *index)] for k in range(7)]

    def speed(y, most):
        w = primitive(all_of(base, y))
        gamma, stiff = mixture(w[6])
        swift = jnp.maximum(jnp.maximum(jnp.abs(w[2]), jnp.abs(w[3])), jnp.abs(w[4]))
        return jnp.maximum(most, swift + sound(w[0] + w[1], w[5], gamma, stiff))

    load_base.wait()
    most = jnp.zeros((8, 128), jnp.float32)
    for y in range(8):
        most = speed(y, most)
    rows[2] = jnp.broadcast_to(jnp.max(most, keepdims=True), (1, 128))
    def stage_start(stage):
        n, at = stages[stage]
        for k in far_first(n):
            copy = send(
                rows.at[stage],
                slots[stage].at[k - 1],
                stage_send.at[stage],
                stage_recv.at[stage],
                at(k),
            )
            if stage == 0:
                there_s, there_c = at(k)
                pl.when((there_s != chief_s) | (there_c != chief_c))(copy.start)
            else:
                copy.start()

    def stage_total(stage):
        n, at = stages[stage]
        return send(slots[stage], slots[stage], stage_send.at[stage], stage_recv.at[stage], at(1))

    def stage_end(stage):
        n, _ = stages[stage]
        stage_total(stage).wait_recv()
        value = rows[stage]
        for k in range(1, n):
            value = jnp.maximum(value, slots[stage][k - 1])
        return value

    def to_root(root):
        return send(
            rows.at[2],
            slots2.at[(root - plane + planes) % planes - 1],
            stage_send.at[2],
            stage_recv.at[2],
            (s, root * inner_c + c % inner_c),
        )

    @pl.when(jnp.logical_not(is_root))
    def _():
        pl.semaphore_wait(barrier, greeted + roots)
        for root in range(roots):
            to_root(root).start()

    load_now.wait()
    load_inflow.wait()

    lane = lax.broadcasted_iota(jnp.int32, (8, 128), 1)
    place = lane % 16
    group = lane // 16

    def pack(y, packed):
        packed = list(packed)
        for k, value in enumerate(across_rows(now_rows, y)):
            packed[k] = jnp.where(group == y, pltpu.roll(value, 16 * y + 5, 1), packed[k])
        return tuple(packed)

    packed = (jnp.zeros((8, 128), jnp.float32),) * 7
    for y in range(8):
        packed = pack(y, packed)
    for k in range(7):
        a_own[k] = packed[k]

    copies = [
        send(now.at[:, :, 0:3], halo.at[:, :, 0:3], halo_send.at[0], halo_recv.at[0], below),
        send(now.at[:, :, 5:8], halo.at[:, :, 5:8], halo_send.at[1], halo_recv.at[1], above),
        send(a_own, a_right, halo_send.at[2], halo_recv.at[2], left),
        send(a_own, a_left, halo_send.at[3], halo_recv.at[3], right),
    ]
    def own_prim(y, _):
        for k, value in enumerate(primitive(across_rows(now_rows, y))):
            prim[k, y + 3] = value
        return 0

    def local(y, _):
        w = all_of(prim, y + 3)
        across = folded(spread(along(w, 0, 2), 0), w[6])
        keep = (lane >= 3) & (lane <= 125)
        stream = folded(spread(along(w, 1, 0), 1, keep), w[6])
        for k in range(7):
            acc[k, y + 1] = across[k] + stream[k]
        return 0

    def fixed_part(z, _):
        for k in range(7):
            part_ref[k, z] = base[k, z] * (1.0 / 3.0) + now[k, z] * (2.0 / 3.0)
        return 0

    def at_home():
        lax.fori_loop(0, 8, own_prim, 0)
        lax.fori_loop(0, 8, local, 0)
        lax.fori_loop(0, 8, fixed_part, 0)

    pl.when(is_root)(at_home)

    @pl.when(is_root)
    def _():
        pl.semaphore_wait(barrier, greeted + roots - 1 + stages[1][0] - 1 + stages[0][0] - 1)
        for root in range(roots):
            pl.when(plane != root)(to_root(root).start)

    copies[3].start()
    pl.when(jnp.logical_not(answer_left))(copies[2].start)
    pl.when(jnp.logical_not(answer_above))(copies[1].start)
    pl.when(jnp.logical_not(answer_below))(copies[0].start)

    to_chief = send(
        rows.at[1],
        quick.at[s * inner_c + c % inner_c],
        stage_send.at[4],
        stage_recv.at[4],
        (chief_s, chief_c),
    )
    pl.when(jnp.logical_not(is_root))(at_home)

    @pl.when(is_root)
    def _():
        rows[1] = stage_end(2)
        pl.when(serves_chief)(to_chief.start)
        stage_start(1)

    @pl.when(answer_below)
    def _():
        copies[1].wait_recv()
        copies[0].start()

    @pl.when(answer_above)
    def _():
        copies[0].wait_recv()
        copies[1].start()

    @pl.when(answer_left)
    def _():
        copies[3].wait_recv()
        copies[2].start()

    @pl.when(is_root)
    def _():
        rows[0] = stage_end(1)
        stage_start(0)

    pl.when(jnp.logical_not(answer_below))(copies[1].wait_recv)
    pl.when(jnp.logical_not(answer_above))(copies[0].wait_recv)

    def halo_prim(i, _):
        row = i + i // 3 * 8
        for k, value in enumerate(primitive(across_rows(halo_rows, (i + 5) % 8))):
            prim[k, row] = value
        return 0

    lax.fori_loop(0, 6, halo_prim, 0)

    def cell_edges(y):
        upper, lower = ([], [])
        for k in range(7):
            f, g, h, up, far = (prim[k, y + i] for i in range(1, 6))
            one, two = edges(h, g - f, h - g, up - h, far - up)
            upper.append(one)
            lower.append(two)
        return (upper, lower)

    for k, value in enumerate(cell_edges(-1)[0]):
        xr[k] = value
    for k in range(8):
        flux_prev[k] = jnp.zeros((8, 128), jnp.float32)
    for k in range(7):
        acc[k, 0] = jnp.zeros((8, 128), jnp.float32)

    def face(j, _):
        upper, lower = cell_edges(j)
        before = all_of(xr)
        for k in range(7):
            xr[k] = upper[k]
        lower_cell = all_of(prim, j + 2)
        flux = fluxes(before, lower, lower_cell, all_of(prim, j + 3), 1)
        change = [flux[k] - flux_prev[k] for k in range(8)]
        for k in range(8):
            flux_prev[k] = flux[k]
        for k, value in enumerate(folded(change, lower_cell[6])):
            acc[k, j] = acc[k, j] + value
        return 0

    lax.fori_loop(0, 9, face, 0)

    copies[2].wait_recv()
    pl.when(jnp.logical_not(answer_left))(copies[3].wait_recv)

    @pl.when(s == 0)
    def _():
        for k in range(7):
            value = jnp.zeros((8, 128), jnp.float32)
            for layer in range(3):
                for y in range(8):
                    one = jnp.broadcast_to(inflow[k, layer][:, y : y + 1], (8, 128))
                    value = jnp.where((group == y) & (place == 2 + layer), one, value)
            a_left[k] = value

    @pl.when(s == size_s - 1)
    def _():
        for k in range(7):
            value = a_own[k]
            one, two, three = (rolled(value, 1, 1), rolled(value, 2, 1), rolled(value, 3, 1))
            a_right[k] = jnp.where(place == 5, one, jnp.where(place == 6, two, three))

    rim = []
    for k in range(7):
        own = a_own[k]
        late = rolled(jnp.where(place < 5, a_left[k], own), 6, 1)
        rim.append(jnp.where(place < 5, own, jnp.where(place < 8, a_right[k], late)))
    w = primitive(rim)
    keep = ((place >= 3) & (place <= 5)) | ((place >= 11) & (place <= 13))
    ends = folded(spread(along(w, 1, 0), 1, keep), w[6])
    for k in range(7):
        edge[k] = jnp.where(place < 5, ends[k], rolled(ends[k], -6, 1))

    near = (lane >= 125) | (lane <= 2)
    for k in range(7):
        for y in range(8):
            extra = jnp.where(near, rolled(edge[k], 123 - 16 * y, 1), 0.0)
            rate_ref[k, pl.ds(y, 8, stride=8), :] = (acc[k, y + 1] + extra) * (-1.0 / 3.0)

    children = [
        send(
            rows.at[3],
            told.at[0],
            stage_send.at[3],
            stage_recv.at[3],
            (s, (c + k * inner_c) % size_c),
        )
        for k in range(1, planes - roots + 1)
    ]

    @pl.when(is_root & jnp.logical_not(is_chief))
    def _():
        fastest = stage_end(0)
        rows[3] = fastest
        step_ref[...] = 0.3 / fastest

    @pl.when(is_chief)
    def _():
        span = quick.at[pl.ds(0, members - 1)]
        send(span, span, stage_send.at[4], stage_recv.at[4], right).wait_recv()
        fastest = rows[1]
        for k in range(members):
            if k != chief_s * inner_c + chief_c:
                fastest = jnp.maximum(fastest, quick[k])
        rows[3] = fastest
        step_ref[...] = 0.3 / fastest

    @pl.when(plane == roots - 1)
    def _():
        for copy in children:
            copy.start()

    @pl.when(jnp.logical_not(is_root))
    def _():
        children[0].wait_recv()
        step_ref[...] = 0.3 / told[0]

    for copy in copies:
        copy.wait_send()

    def sent(count, stage):
        span = slots2.at[pl.ds(0, count)]
        send(span, span, stage_send.at[stage], stage_recv.at[stage], right).wait_send()

    @pl.when(is_root)
    def _():
        stage_total(1).wait_send()
        if roots > 1:
            sent(roots - 1, 2)

    pl.when(is_root & jnp.logical_not(beside_chief))(stage_total(0).wait_send)

    @pl.when(beside_chief)
    def _():
        if sizes[0] > 2:
            span = slots0.at[pl.ds(0, sizes[0] - 2)]
            send(span, span, stage_send.at[0], stage_recv.at[0], right).wait_send()

    pl.when(serves_chief)(to_chief.wait_send)

    @pl.when(plane == roots - 1)
    def _():
        sent(planes - roots, 3)

    @pl.when(jnp.logical_not(is_root))
    def _():
        sent(roots, 2)


def shards(sizes, state_now, state_base, inflow):
    size = jnp.float32
    stream = sizes[0] * sizes[2]
    n0, n1, n2 = (sizes[0], sizes[1] * sizes[2], sizes[3])
    inflow_t = jnp.transpose(inflow, (0, 3, 1, 2))
    part, rate, step = pl.pallas_call(
        functools.partial(kernel, sizes),
        out_shape=(
            jax.ShapeDtypeStruct((7, 8, 8, 128), size),
            jax.ShapeDtypeStruct((7, 64, 128), size),
            jax.ShapeDtypeStruct((1, 128), size),
        ),
        in_specs=[pl.BlockSpec(memory_space=pltpu.HBM)] * 3,
        out_specs=(pl.BlockSpec(memory_space=pltpu.VMEM),) * 3,
        scratch_shapes=[
            pltpu.VMEM((7, 8, 8, 128), size),
            pltpu.VMEM((7, 8, 8, 128), size),
            pltpu.VMEM((7, 8, 8, 128), size),
            pltpu.VMEM((7, 3, 8, 8), size),
            pltpu.VMEM((7, 14, 8, 128), size),
            pltpu.VMEM((7, 8, 128), size),
            pltpu.VMEM((8, 8, 128), size),
            pltpu.VMEM((7, 9, 8, 128), size),
            pltpu.VMEM((7, 8, 128), size),
            pltpu.VMEM((7, 8, 128), size),
            pltpu.VMEM((7, 8, 128), size),
            pltpu.VMEM((7, 8, 128), size),
            pltpu.VMEM((4, 1, 128), size),
            pltpu.VMEM((n0 - 1, 1, 128), size),
            pltpu.VMEM((n1 - 1, 1, 128), size),
            pltpu.VMEM((n2 - 1, 1, 128), size),
            pltpu.VMEM((1, 1, 128), size),
            pltpu.VMEM((n1 // sizes[2] * stream, 1, 128), size),
            pltpu.SemaphoreType.DMA((3,)),
            pltpu.SemaphoreType.DMA((4,)),
            pltpu.SemaphoreType.DMA((4,)),
            pltpu.SemaphoreType.DMA((5,)),
            pltpu.SemaphoreType.DMA((5,)),
        ],
        compiler_params=pltpu.CompilerParams(
            collective_id=0, has_side_effects=True, vmem_limit_bytes=32 * 1024 * 1024
        ),
    )(
        pltpu.with_memory_space_constraint(state_now, pltpu.HBM),
        pltpu.with_memory_space_constraint(state_base, pltpu.HBM),
        pltpu.with_memory_space_constraint(inflow_t, pltpu.HBM),
    )
    return part + step.reshape(1, 1, 1, 128) * rate.reshape(state_now.shape)


def solution(mesh):
    stream, cross = (mesh.shape["stream"], mesh.shape["cross"])
    sizes = (8, 4, 2, 12) if (stream, cross) == (16, 48) else (2, 2, stream // 2, cross // 2)
    return jax.shard_map(
        functools.partial(shards, sizes),
        mesh=mesh,
        in_specs=(
            P(None, None, "cross", "stream"),
            P(None, None, "cross", "stream"),
            P(None, None, "cross", None),
        ),
        out_specs=P(None, None, "cross", "stream"),
        check_vma=False,
    )
```

```python
import functools

import jax
import jax.numpy as jnp
from jax import lax
from jax.experimental import pallas as pl
from jax.experimental.pallas import tpu as pltpu
from jax.sharding import PartitionSpec as P

MESH = pl.DeviceIdType.MESH

gas_part = 1.0 / 0.4
liquid_part = 1.0 / 3.4
stiff_part = 4.4 * 0.6 / 3.4


def inverse(value):
    guess = pl.reciprocal(value, approx=True)
    return guess * (2.0 - value * guess)


def mixture(volume):
    rest = 1.0 - volume
    return (volume * gas_part + rest * liquid_part, rest * stiff_part)


def primitive(u):
    over = 1.0 / (u[0] + u[1])
    vx, vy, vz = (u[2] * over, u[3] * over, u[4] * over)
    kinetic = 0.5 * (u[2] * vx + u[3] * vy + u[4] * vz)
    gamma, stiff = mixture(u[6])
    return (u[0], u[1], vx, vy, vz, (u[5] - kinetic - stiff) / gamma, u[6])


def sound(density, pressure, gamma, stiff):
    return jnp.sqrt(((gamma + 1.0) * pressure + stiff) / (gamma * density))


def edges(h, d1, d2, d3, d4):
    e1, e2, e3 = (d2 - d1, d3 - d2, d4 - d3)
    u0 = e1 + d2 + d2
    u1 = d2 + d3
    u2 = e3 - d3 - d3
    third = 13.0 / 3.0
    top = 1e30
    s0 = jnp.minimum(third * (e1 * e1) + u0 * u0 + 4e-6, top)
    s1 = jnp.minimum(third * (e2 * e2) + u1 * u1 + 4e-6, top)
    s2 = jnp.minimum(third * (e3 * e3) + u2 * u2 + 4e-6, top)
    r0, r1, r2 = (inverse(s0), inverse(s1), inverse(s2))
    a0, a1, a2 = (r0 * r0, 6.0 * (r1 * r1), r2 * r2)
    b0, b2 = (3.0 * a0, 3.0 * a2)
    up = a0 * (u0 + e1 + d2) + a1 * (u1 + d3) + b2 * (d3 - u2)
    down = a2 * (u2 + e3 - d3) - a1 * (u1 + d2) - b0 * (u0 + d2)
    upper = h + up * inverse(6.0 * (a0 + a1 + b2))
    lower = h + down * inverse(6.0 * (a2 + a1 + b0))
    return (upper, lower)


def limited(face, lower_cell, upper_cell):
    out = []
    for c in range(7):
        value = face[c]
        if c in (0, 1, 5):
            value = jnp.maximum(value, 0.5 * jnp.minimum(lower_cell[c], upper_cell[c]))
        elif c == 6:
            value = jnp.maximum(value, 0.5 * jnp.minimum(lower_cell[c], upper_cell[c]))
            value = jnp.minimum(value, 0.5 + 0.5 * jnp.maximum(lower_cell[c], upper_cell[c]))
        out.append(value)
    return out


def side(w, normal):
    density = w[0] + w[1]
    gamma, stiff = mixture(w[6])
    momentum = [density * w[2], density * w[3], density * w[4]]
    energy = (
        gamma * w[5]
        + stiff
        + 0.5 * (momentum[0] * w[2] + momentum[1] * w[3] + momentum[2] * w[4])
    )
    vn = w[2 + normal]
    amounts = [w[0], w[1], *momentum, energy, w[6]]
    moved = [amount * vn for amount in amounts]
    moved[2 + normal] = moved[2 + normal] + w[5]
    moved[5] = moved[5] + w[5] * vn
    signal = jnp.abs(vn) + sound(density, w[5], gamma, stiff)
    return (amounts, moved, vn, signal)


def fluxes(left, right, lower_cell, upper_cell, normal):
    one = side(limited(left, lower_cell, upper_cell), normal)
    two = side(limited(right, lower_cell, upper_cell), normal)
    fastest = jnp.maximum(one[3], two[3])
    out = [
        (fl + fr) - fastest * (ur - ul)
        for ul, ur, fl, fr in zip(one[0], two[0], one[1], two[1])
    ]
    return out + [one[2] + two[2]]


def rolled(value, shift, axis):
    return pltpu.roll(value, shift % value.shape[axis], axis)


def along(w, axis, normal):
    upper, lower, before = ([], [], [])
    for c in range(7):
        h = w[c]
        g = rolled(h, 1, axis)
        d2 = h - g
        d1, d3, d4 = (rolled(d2, 1, axis), rolled(d2, -1, axis), rolled(d2, -2, axis))
        up, down = edges(h, d1, d2, d3, d4)
        upper.append(rolled(up, 1, axis))
        lower.append(down)
        before.append(g)
    return fluxes(upper, lower, before, w, normal)


def spread(flux, axis, keep=None):
    if keep is not None:
        flux = [jnp.where(keep, f, 0.0) for f in flux]
    return [rolled(f, -1, axis) - f for f in flux]


def folded(change, volume):
    return change[:6] + [change[6] - volume * change[7]]


def in_plane(sizes):
    inner_s, inner_c, outer_s, _ = sizes
    s, c = (lax.axis_index("stream"), lax.axis_index("cross"))
    length = outer_s * inner_c
    x, y = (s % inner_s, s // inner_s * inner_c + c % inner_c)
    offsets = [(i, j) for i in range(inner_s) for j in range(length) if i or j]

    def distance(offset):
        i, j = offset
        return min(i, inner_s - i) / 2 + min(j, length - j)

    there = []
    for i, j in sorted(offsets, key=lambda offset: -distance(offset)):
        y_there = (y + j) % length
        there.append(
            (
                y_there // inner_c * inner_s + (x + i) % inner_s,
                c // inner_c * inner_c + y_there % inner_c,
            )
        )
    return there


def along_z(sizes):
    _, inner_c, _, planes = sizes
    s, c = (lax.axis_index("stream"), lax.axis_index("cross"))
    offsets = sorted(range(1, planes), key=lambda k: -min(k, planes - k))
    return [(s, (c + k * inner_c) % (planes * inner_c)) for k in offsets]


def send(source, target, send_sem, recv_sem, to):
    return pltpu.make_async_remote_copy(
        src_ref=source,
        dst_ref=target,
        send_sem=send_sem,
        recv_sem=recv_sem,
        device_id=to,
        device_id_type=MESH,
    )


def kernel(
    sizes,
    now_ref,
    base_ref,
    inflow_ref,
    part_ref,
    rate_ref,
    step_ref,
    now,
    base,
    halo,
    inflow,
    prim,
    xr,
    flux_prev,
    acc,
    a_own,
    a_left,
    a_right,
    edge,
    rows,
    slots_z,
    slots_p,
    told,
    in_sems,
    halo_send,
    halo_recv,
    stage_send,
    stage_recv,
):
    size_s, size_c = (sizes[0] * sizes[2], sizes[1] * sizes[3])
    s, c = (lax.axis_index("stream"), lax.axis_index("cross"))
    left, right = (((s + size_s - 1) % size_s, c), ((s + 1) % size_s, c))
    below, above = ((s, (c + size_c - 1) % size_c), (s, (c + 1) % size_c))
    mates, others = (in_plane(sizes), along_z(sizes))
    inner_c, planes = (sizes[1], sizes[3])
    roots = max(1, planes // 3)
    plane = c // inner_c
    is_root = plane < roots

    load_base = pltpu.make_async_copy(base_ref, base, in_sems.at[0])
    load_now = pltpu.make_async_copy(now_ref, now, in_sems.at[1])
    load_inflow = pltpu.make_async_copy(inflow_ref, inflow, in_sems.at[2])
    load_base.start()
    load_now.start()
    load_inflow.start()

    barrier = pltpu.get_barrier_semaphore()

    def greet(there):
        pl.semaphore_signal(barrier, inc=1, device_id=there, device_id_type=MESH)

    first_s, last_s = (s % sizes[0] == 0, s % sizes[0] == sizes[0] - 1)
    first_c, last_c = (c % inner_c == 0, c % inner_c == inner_c - 1)
    flip = s // sizes[0] > 0
    answer_left = first_s
    answer_above = last_c & flip
    answer_below = first_c & jnp.logical_not(flip)
    greet(left)
    pl.when(jnp.logical_not(last_s))(lambda: greet(right))
    pl.when(jnp.logical_not(first_c & flip))(lambda: greet(below))
    pl.when(jnp.logical_not(last_c & jnp.logical_not(flip)))(lambda: greet(above))
    greeted = (
        1
        + jnp.where(answer_left, 0, 1)
        + jnp.where(answer_above, 0, 1)
        + jnp.where(answer_below, 0, 1)
    )

    @pl.when(is_root)
    def _():
        for there in others + mates:
            greet(there)

    now_rows = now.reshape(7, 64, 128)
    halo_rows = halo.reshape(7, 64, 128)

    def across_rows(ref, y):
        return [ref[k, pl.ds(y, 8, stride=8), :] for k in range(7)]

    def all_of(ref, *index):
        return [ref[(k, *index)] for k in range(7)]

    def speed(y, most):
        w = primitive(all_of(base, y))
        gamma, stiff = mixture(w[6])
        swift = jnp.maximum(jnp.maximum(jnp.abs(w[2]), jnp.abs(w[3])), jnp.abs(w[4]))
        return jnp.maximum(most, swift + sound(w[0] + w[1], w[5], gamma, stiff))

    load_base.wait()
    most = jnp.zeros((8, 128), jnp.float32)
    for y in range(8):
        most = speed(y, most)
    rows[0] = jnp.broadcast_to(jnp.max(most, keepdims=True), (1, 128))
    def arrived(slots, stage, own):
        send(slots, slots, stage_send.at[stage], stage_recv.at[stage], right).wait_recv()
        for k in range(slots.shape[0]):
            own = jnp.maximum(own, slots[k])
        return own

    def to_root(root):
        return send(
            rows.at[0],
            slots_z.at[(root - plane + planes) % planes - 1],
            stage_send.at[0],
            stage_recv.at[0],
            (s, root * inner_c + c % inner_c),
        )

    @pl.when(jnp.logical_not(is_root))
    def _():
        pl.semaphore_wait(barrier, greeted + roots)
        for root in range(roots):
            to_root(root).start()

    load_now.wait()
    load_inflow.wait()

    lane = lax.broadcasted_iota(jnp.int32, (8, 128), 1)
    place = lane % 16
    group = lane // 16

    def pack(y, packed):
        packed = list(packed)
        for k, value in enumerate(across_rows(now_rows, y)):
            packed[k] = jnp.where(group == y, pltpu.roll(value, 16 * y + 5, 1), packed[k])
        return tuple(packed)

    packed = (jnp.zeros((8, 128), jnp.float32),) * 7
    for y in range(8):
        packed = pack(y, packed)
    for k in range(7):
        a_own[k] = packed[k]

    copies = [
        send(now.at[:, :, 0:3], halo.at[:, :, 0:3], halo_send.at[0], halo_recv.at[0], below),
        send(now.at[:, :, 5:8], halo.at[:, :, 5:8], halo_send.at[1], halo_recv.at[1], above),
        send(a_own, a_right, halo_send.at[2], halo_recv.at[2], left),
        send(a_own, a_left, halo_send.at[3], halo_recv.at[3], right),
    ]
    def own_prim(y, _):
        for k, value in enumerate(primitive(across_rows(now_rows, y))):
            prim[k, y + 3] = value
        return 0

    def local(y, _):
        w = all_of(prim, y + 3)
        across = folded(spread(along(w, 0, 2), 0), w[6])
        keep = (lane >= 3) & (lane <= 125)
        stream = folded(spread(along(w, 1, 0), 1, keep), w[6])
        for k in range(7):
            acc[k, y + 1] = across[k] + stream[k]
        return 0

    def fixed_part(z, _):
        for k in range(7):
            part_ref[k, z] = base[k, z] * (1.0 / 3.0) + now[k, z] * (2.0 / 3.0)
        return 0

    def at_home():
        lax.fori_loop(0, 8, own_prim, 0)
        lax.fori_loop(0, 8, local, 0)
        lax.fori_loop(0, 8, fixed_part, 0)

    pl.when(is_root)(at_home)

    @pl.when(is_root)
    def _():
        pl.semaphore_wait(barrier, greeted + roots - 1 + len(mates))
        for root in range(roots):
            pl.when(plane != root)(to_root(root).start)

    copies[3].start()
    pl.when(jnp.logical_not(answer_left))(copies[2].start)
    pl.when(jnp.logical_not(answer_above))(copies[1].start)
    pl.when(jnp.logical_not(answer_below))(copies[0].start)

    pl.when(jnp.logical_not(is_root))(at_home)

    @pl.when(is_root)
    def _():
        rows[1] = arrived(slots_z, 0, rows[0])
        for k, there in enumerate(mates):
            send(rows.at[1], slots_p.at[k], stage_send.at[1], stage_recv.at[1], there).start()

    @pl.when(answer_below)
    def _():
        copies[1].wait_recv()
        copies[0].start()

    @pl.when(answer_above)
    def _():
        copies[0].wait_recv()
        copies[1].start()

    @pl.when(answer_left)
    def _():
        copies[3].wait_recv()
        copies[2].start()

    pl.when(jnp.logical_not(answer_below))(copies[1].wait_recv)
    pl.when(jnp.logical_not(answer_above))(copies[0].wait_recv)

    def halo_prim(i, _):
        row = i + i // 3 * 8
        for k, value in enumerate(primitive(across_rows(halo_rows, (i + 5) % 8))):
            prim[k, row] = value
        return 0

    lax.fori_loop(0, 6, halo_prim, 0)

    def cell_edges(y):
        upper, lower = ([], [])
        for k in range(7):
            f, g, h, up, far = (prim[k, y + i] for i in range(1, 6))
            one, two = edges(h, g - f, h - g, up - h, far - up)
            upper.append(one)
            lower.append(two)
        return (upper, lower)

    for k, value in enumerate(cell_edges(-1)[0]):
        xr[k] = value
    for k in range(8):
        flux_prev[k] = jnp.zeros((8, 128), jnp.float32)
    for k in range(7):
        acc[k, 0] = jnp.zeros((8, 128), jnp.float32)

    def face(j, _):
        upper, lower = cell_edges(j)
        before = all_of(xr)
        for k in range(7):
            xr[k] = upper[k]
        lower_cell = all_of(prim, j + 2)
        flux = fluxes(before, lower, lower_cell, all_of(prim, j + 3), 1)
        change = [flux[k] - flux_prev[k] for k in range(8)]
        for k in range(8):
            flux_prev[k] = flux[k]
        for k, value in enumerate(folded(change, lower_cell[6])):
            acc[k, j] = acc[k, j] + value
        return 0

    lax.fori_loop(0, 9, face, 0)

    copies[2].wait_recv()
    pl.when(jnp.logical_not(answer_left))(copies[3].wait_recv)

    @pl.when(s == 0)
    def _():
        for k in range(7):
            value = jnp.zeros((8, 128), jnp.float32)
            for layer in range(3):
                for y in range(8):
                    one = jnp.broadcast_to(inflow[k, layer][:, y : y + 1], (8, 128))
                    value = jnp.where((group == y) & (place == 2 + layer), one, value)
            a_left[k] = value

    @pl.when(s == size_s - 1)
    def _():
        for k in range(7):
            value = a_own[k]
            one, two, three = (rolled(value, 1, 1), rolled(value, 2, 1), rolled(value, 3, 1))
            a_right[k] = jnp.where(place == 5, one, jnp.where(place == 6, two, three))

    rim = []
    for k in range(7):
        own = a_own[k]
        late = rolled(jnp.where(place < 5, a_left[k], own), 6, 1)
        rim.append(jnp.where(place < 5, own, jnp.where(place < 8, a_right[k], late)))
    w = primitive(rim)
    keep = ((place >= 3) & (place <= 5)) | ((place >= 11) & (place <= 13))
    ends = folded(spread(along(w, 1, 0), 1, keep), w[6])
    for k in range(7):
        edge[k] = jnp.where(place < 5, ends[k], rolled(ends[k], -6, 1))

    near = (lane >= 125) | (lane <= 2)
    for k in range(7):
        for y in range(8):
            extra = jnp.where(near, rolled(edge[k], 123 - 16 * y, 1), 0.0)
            rate_ref[k, pl.ds(y, 8, stride=8), :] = (acc[k, y + 1] + extra) * (-1.0 / 3.0)

    children = [
        send(
            rows.at[2],
            told.at[0],
            stage_send.at[2],
            stage_recv.at[2],
            (s, (c + k * inner_c) % size_c),
        )
        for k in range(1, planes - roots + 1)
    ]

    @pl.when(is_root)
    def _():
        fastest = arrived(slots_p, 1, rows[1])
        rows[2] = fastest
        step_ref[...] = 0.3 / fastest

    @pl.when(plane == roots - 1)
    def _():
        for copy in children:
            copy.start()

    @pl.when(jnp.logical_not(is_root))
    def _():
        children[0].wait_recv()
        step_ref[...] = 0.3 / told[0]

    for copy in copies:
        copy.wait_send()

    def sent(slots, stage):
        send(slots, slots, stage_send.at[stage], stage_recv.at[stage], right).wait_send()

    @pl.when(is_root)
    def _():
        sent(slots_p, 1)
        if roots > 1:
            sent(slots_z.at[pl.ds(0, roots - 1)], 0)

    @pl.when(plane == roots - 1)
    def _():
        sent(slots_z.at[pl.ds(0, planes - roots)], 2)

    @pl.when(jnp.logical_not(is_root))
    def _():
        sent(slots_z.at[pl.ds(0, roots)], 0)


def shards(sizes, state_now, state_base, inflow):
    size = jnp.float32
    inflow_t = jnp.transpose(inflow, (0, 3, 1, 2))
    part, rate, step = pl.pallas_call(
        functools.partial(kernel, sizes),
        out_shape=(
            jax.ShapeDtypeStruct((7, 8, 8, 128), size),
            jax.ShapeDtypeStruct((7, 64, 128), size),
            jax.ShapeDtypeStruct((1, 128), size),
        ),
        in_specs=[pl.BlockSpec(memory_space=pltpu.HBM)] * 3,
        out_specs=(pl.BlockSpec(memory_space=pltpu.VMEM),) * 3,
        scratch_shapes=[
            pltpu.VMEM((7, 8, 8, 128), size),
            pltpu.VMEM((7, 8, 8, 128), size),
            pltpu.VMEM((7, 8, 8, 128), size),
            pltpu.VMEM((7, 3, 8, 8), size),
            pltpu.VMEM((7, 14, 8, 128), size),
            pltpu.VMEM((7, 8, 128), size),
            pltpu.VMEM((8, 8, 128), size),
            pltpu.VMEM((7, 9, 8, 128), size),
            pltpu.VMEM((7, 8, 128), size),
            pltpu.VMEM((7, 8, 128), size),
            pltpu.VMEM((7, 8, 128), size),
            pltpu.VMEM((7, 8, 128), size),
            pltpu.VMEM((3, 1, 128), size),
            pltpu.VMEM((sizes[3] - 1, 1, 128), size),
            pltpu.VMEM((sizes[0] * sizes[1] * sizes[2] - 1, 1, 128), size),
            pltpu.VMEM((1, 1, 128), size),
            pltpu.SemaphoreType.DMA((3,)),
            pltpu.SemaphoreType.DMA((4,)),
            pltpu.SemaphoreType.DMA((4,)),
            pltpu.SemaphoreType.DMA((3,)),
            pltpu.SemaphoreType.DMA((3,)),
        ],
        compiler_params=pltpu.CompilerParams(
            collective_id=0, has_side_effects=True, vmem_limit_bytes=32 * 1024 * 1024
        ),
    )(
        pltpu.with_memory_space_constraint(state_now, pltpu.HBM),
        pltpu.with_memory_space_constraint(state_base, pltpu.HBM),
        pltpu.with_memory_space_constraint(inflow_t, pltpu.HBM),
    )
    return part + step.reshape(1, 1, 1, 128) * rate.reshape(state_now.shape)


def solution(mesh):
    stream, cross = (mesh.shape["stream"], mesh.shape["cross"])
    sizes = (8, 4, 2, 12) if (stream, cross) == (16, 48) else (2, 2, stream // 2, cross // 2)
    return jax.shard_map(
        functools.partial(shards, sizes),
        mesh=mesh,
        in_specs=(
            P(None, None, "cross", "stream"),
            P(None, None, "cross", "stream"),
            P(None, None, "cross", None),
        ),
        out_specs=P(None, None, "cross", "stream"),
        check_vma=False,
    )
```

```python
import functools

import jax
import jax.numpy as jnp
from jax import lax
from jax.experimental import pallas as pl
from jax.experimental.pallas import tpu as pltpu
from jax.sharding import PartitionSpec as P

MESH = pl.DeviceIdType.MESH

gas_part = 1.0 / 0.4
liquid_part = 1.0 / 3.4
stiff_part = 4.4 * 0.6 / 3.4


def inverse(value):
    guess = pl.reciprocal(value, approx=True)
    return guess * (2.0 - value * guess)


def mixture(volume):
    rest = 1.0 - volume
    return (volume * gas_part + rest * liquid_part, rest * stiff_part)


def primitive(u):
    over = 1.0 / (u[0] + u[1])
    vx, vy, vz = (u[2] * over, u[3] * over, u[4] * over)
    kinetic = 0.5 * (u[2] * vx + u[3] * vy + u[4] * vz)
    gamma, stiff = mixture(u[6])
    return (u[0], u[1], vx, vy, vz, (u[5] - kinetic - stiff) / gamma, u[6])


def sound(density, pressure, gamma, stiff):
    return jnp.sqrt(((gamma + 1.0) * pressure + stiff) / (gamma * density))


def edges(h, d1, d2, d3, d4):
    e1, e2, e3 = (d2 - d1, d3 - d2, d4 - d3)
    u0 = e1 + d2 + d2
    u1 = d2 + d3
    u2 = e3 - d3 - d3
    third = 13.0 / 3.0
    top = 1e30
    s0 = jnp.minimum(third * (e1 * e1) + u0 * u0 + 4e-6, top)
    s1 = jnp.minimum(third * (e2 * e2) + u1 * u1 + 4e-6, top)
    s2 = jnp.minimum(third * (e3 * e3) + u2 * u2 + 4e-6, top)
    r0, r1, r2 = (inverse(s0), inverse(s1), inverse(s2))
    a0, a1, a2 = (r0 * r0, 6.0 * (r1 * r1), r2 * r2)
    b0, b2 = (3.0 * a0, 3.0 * a2)
    up = a0 * (u0 + e1 + d2) + a1 * (u1 + d3) + b2 * (d3 - u2)
    down = a2 * (u2 + e3 - d3) - a1 * (u1 + d2) - b0 * (u0 + d2)
    upper = h + up * inverse(6.0 * (a0 + a1 + b2))
    lower = h + down * inverse(6.0 * (a2 + a1 + b0))
    return (upper, lower)


def limited(face, lower_cell, upper_cell):
    out = []
    for c in range(7):
        value = face[c]
        if c in (0, 1, 5):
            value = jnp.maximum(value, 0.5 * jnp.minimum(lower_cell[c], upper_cell[c]))
        elif c == 6:
            value = jnp.maximum(value, 0.5 * jnp.minimum(lower_cell[c], upper_cell[c]))
            value = jnp.minimum(value, 0.5 + 0.5 * jnp.maximum(lower_cell[c], upper_cell[c]))
        out.append(value)
    return out


def side(w, normal):
    density = w[0] + w[1]
    gamma, stiff = mixture(w[6])
    momentum = [density * w[2], density * w[3], density * w[4]]
    energy = (
        gamma * w[5]
        + stiff
        + 0.5 * (momentum[0] * w[2] + momentum[1] * w[3] + momentum[2] * w[4])
    )
    vn = w[2 + normal]
    amounts = [w[0], w[1], *momentum, energy, w[6]]
    moved = [amount * vn for amount in amounts]
    moved[2 + normal] = moved[2 + normal] + w[5]
    moved[5] = moved[5] + w[5] * vn
    signal = jnp.abs(vn) + sound(density, w[5], gamma, stiff)
    return (amounts, moved, vn, signal)


def fluxes(left, right, lower_cell, upper_cell, normal):
    one = side(limited(left, lower_cell, upper_cell), normal)
    two = side(limited(right, lower_cell, upper_cell), normal)
    fastest = jnp.maximum(one[3], two[3])
    out = [
        (fl + fr) - fastest * (ur - ul)
        for ul, ur, fl, fr in zip(one[0], two[0], one[1], two[1])
    ]
    return out + [one[2] + two[2]]


def rolled(value, shift, axis):
    return pltpu.roll(value, shift % value.shape[axis], axis)


def along(w, axis, normal):
    upper, lower, before = ([], [], [])
    for c in range(7):
        h = w[c]
        g = rolled(h, 1, axis)
        d2 = h - g
        d1, d3, d4 = (rolled(d2, 1, axis), rolled(d2, -1, axis), rolled(d2, -2, axis))
        up, down = edges(h, d1, d2, d3, d4)
        upper.append(rolled(up, 1, axis))
        lower.append(down)
        before.append(g)
    return fluxes(upper, lower, before, w, normal)


def spread(flux, axis, keep=None):
    if keep is not None:
        flux = [jnp.where(keep, f, 0.0) for f in flux]
    return [rolled(f, -1, axis) - f for f in flux]


def folded(change, volume):
    return change[:6] + [change[6] - volume * change[7]]


def in_plane(sizes):
    inner_s, inner_c, outer_s, _ = sizes
    s, c = (lax.axis_index("stream"), lax.axis_index("cross"))
    length = outer_s * inner_c
    x, y = (s % inner_s, s // inner_s * inner_c + c % inner_c)
    offsets = [(i, j) for i in range(inner_s) for j in range(length) if i or j]

    def distance(offset):
        i, j = offset
        return min(i, inner_s - i) / 2 + min(j, length - j)

    there = []
    for i, j in sorted(offsets, key=lambda offset: -distance(offset)):
        y_there = (y + j) % length
        there.append(
            (
                y_there // inner_c * inner_s + (x + i) % inner_s,
                c // inner_c * inner_c + y_there % inner_c,
            )
        )
    return there


def along_z(sizes):
    _, inner_c, _, planes = sizes
    s, c = (lax.axis_index("stream"), lax.axis_index("cross"))
    offsets = sorted(range(1, planes), key=lambda k: -min(k, planes - k))
    return [(s, (c + k * inner_c) % (planes * inner_c)) for k in offsets]


def send(source, target, send_sem, recv_sem, to):
    return pltpu.make_async_remote_copy(
        src_ref=source,
        dst_ref=target,
        send_sem=send_sem,
        recv_sem=recv_sem,
        device_id=to,
        device_id_type=MESH,
    )


def kernel(
    sizes,
    now_ref,
    base_ref,
    inflow_ref,
    part_ref,
    rate_ref,
    step_ref,
    now,
    base,
    halo,
    inflow,
    prim,
    xr,
    flux_prev,
    acc,
    a_own,
    a_left,
    a_right,
    edge,
    rows,
    slots_z,
    slots_p,
    told,
    in_sems,
    halo_send,
    halo_recv,
    stage_send,
    stage_recv,
):
    load_base = pltpu.make_async_copy(base_ref, base, in_sems.at[0])
    load_now = pltpu.make_async_copy(now_ref, now, in_sems.at[1])
    load_inflow = pltpu.make_async_copy(inflow_ref, inflow, in_sems.at[2])
    load_base.start()
    load_now.start()
    load_inflow.start()

    size_s, size_c = (sizes[0] * sizes[2], sizes[1] * sizes[3])
    s, c = (lax.axis_index("stream"), lax.axis_index("cross"))
    left, right = (((s + size_s - 1) % size_s, c), ((s + 1) % size_s, c))
    below, above = ((s, (c + size_c - 1) % size_c), (s, (c + 1) % size_c))
    inner_c, planes = (sizes[1], sizes[3])
    roots = max(1, planes // 3)
    plane = c // inner_c
    is_root = plane < roots

    barrier = pltpu.get_barrier_semaphore()

    def greet(there):
        pl.semaphore_signal(barrier, inc=1, device_id=there, device_id_type=MESH)

    first_s, last_s = (s % sizes[0] == 0, s % sizes[0] == sizes[0] - 1)
    first_c, last_c = (c % inner_c == 0, c % inner_c == inner_c - 1)
    flip = s // sizes[0] > 0
    answer_left = first_s
    answer_above = last_c & flip & (plane != planes - 1)
    answer_below = first_c & (jnp.logical_not(flip) | (plane == 0))
    greet(left)
    pl.when(jnp.logical_not(last_s))(lambda: greet(right))
    pl.when(jnp.logical_not(first_c) | answer_below)(lambda: greet(below))
    pl.when(jnp.logical_not(last_c) | answer_above)(lambda: greet(above))
    greeted = (
        1
        + jnp.where(answer_left, 0, 1)
        + jnp.where(answer_above, 0, 1)
        + jnp.where(answer_below, 0, 1)
    )

    @pl.when(is_root)
    def _():
        for there in along_z(sizes) + in_plane(sizes):
            greet(there)

    now_rows = now.reshape(7, 64, 128)
    halo_rows = halo.reshape(7, 64, 128)

    def across_rows(ref, y):
        return [ref[k, pl.ds(y, 8, stride=8), :] for k in range(7)]

    def all_of(ref, *index):
        return [ref[(k, *index)] for k in range(7)]

    def speed(y, most):
        w = primitive(all_of(base, y))
        gamma, stiff = mixture(w[6])
        swift = jnp.maximum(jnp.maximum(jnp.abs(w[2]), jnp.abs(w[3])), jnp.abs(w[4]))
        return jnp.maximum(most, swift + sound(w[0] + w[1], w[5], gamma, stiff))

    load_base.wait()
    most = jnp.zeros((8, 128), jnp.float32)
    for y in range(8):
        most = speed(y, most)
    rows[0] = jnp.broadcast_to(jnp.max(most, keepdims=True), (1, 128))
    def arrived(slots, stage, own):
        send(slots, slots, stage_send.at[stage], stage_recv.at[stage], right).wait_recv()
        for k in range(slots.shape[0]):
            own = jnp.maximum(own, slots[k])
        return own

    def to_root(root):
        return send(
            rows.at[0],
            slots_z.at[(root - plane + planes) % planes - 1],
            stage_send.at[0],
            stage_recv.at[0],
            (s, root * inner_c + c % inner_c),
        )

    @pl.when(jnp.logical_not(is_root))
    def _():
        pl.semaphore_wait(barrier, greeted + roots)
        for root in range(roots):
            to_root(root).start()

    load_now.wait()
    load_inflow.wait()

    lane = lax.broadcasted_iota(jnp.int32, (8, 128), 1)
    place = lane % 16
    group = lane // 16

    def pack(y, packed):
        packed = list(packed)
        for k, value in enumerate(across_rows(now_rows, y)):
            packed[k] = jnp.where(group == y, pltpu.roll(value, 16 * y + 5, 1), packed[k])
        return tuple(packed)

    packed = (jnp.zeros((8, 128), jnp.float32),) * 7
    for y in range(8):
        packed = pack(y, packed)
    for k in range(7):
        a_own[k] = packed[k]

    copies = [
        send(now.at[:, :, 0:3], halo.at[:, :, 0:3], halo_send.at[0], halo_recv.at[0], below),
        send(now.at[:, :, 5:8], halo.at[:, :, 5:8], halo_send.at[1], halo_recv.at[1], above),
        send(a_own, a_right, halo_send.at[2], halo_recv.at[2], left),
        send(a_own, a_left, halo_send.at[3], halo_recv.at[3], right),
    ]
    def own_prim(y, _):
        for k, value in enumerate(primitive(across_rows(now_rows, y))):
            prim[k, y + 3] = value
        return 0

    def local(y, _):
        w = all_of(prim, y + 3)
        across = folded(spread(along(w, 0, 2), 0), w[6])
        keep = (lane >= 3) & (lane <= 125)
        stream = folded(spread(along(w, 1, 0), 1, keep), w[6])
        for k in range(7):
            acc[k, y + 1] = across[k] + stream[k]
        return 0

    def fixed_part(z, _):
        for k in range(7):
            part_ref[k, z] = base[k, z] * (1.0 / 3.0) + now[k, z] * (2.0 / 3.0)
        return 0

    def at_home():
        lax.fori_loop(0, 8, own_prim, 0)
        lax.fori_loop(0, 8, local, 0)
        lax.fori_loop(0, 8, fixed_part, 0)

    pl.when(is_root)(at_home)

    @pl.when(is_root)
    def _():
        pl.semaphore_wait(barrier, greeted + roots - 1 + slots_p.shape[0])
        for root in range(roots):
            pl.when(plane != root)(to_root(root).start)

    copies[3].start()
    pl.when(jnp.logical_not(answer_left))(copies[2].start)
    pl.when(jnp.logical_not(answer_above))(copies[1].start)
    pl.when(jnp.logical_not(answer_below))(copies[0].start)

    pl.when(jnp.logical_not(is_root))(at_home)

    @pl.when(is_root)
    def _():
        rows[1] = arrived(slots_z, 0, rows[0])
        for k, there in enumerate(in_plane(sizes)):
            send(rows.at[1], slots_p.at[k], stage_send.at[1], stage_recv.at[1], there).start()

    @pl.when(answer_below)
    def _():
        copies[1].wait_recv()
        copies[0].start()

    @pl.when(answer_above)
    def _():
        copies[0].wait_recv()
        copies[1].start()

    @pl.when(answer_left)
    def _():
        copies[3].wait_recv()
        copies[2].start()

    pl.when(jnp.logical_not(answer_below))(copies[1].wait_recv)
    pl.when(jnp.logical_not(answer_above))(copies[0].wait_recv)

    def halo_prim(i, _):
        row = i + i // 3 * 8
        for k, value in enumerate(primitive(across_rows(halo_rows, (i + 5) % 8))):
            prim[k, row] = value
        return 0

    lax.fori_loop(0, 6, halo_prim, 0)

    def cell_edges(y):
        upper, lower = ([], [])
        for k in range(7):
            f, g, h, up, far = (prim[k, y + i] for i in range(1, 6))
            one, two = edges(h, g - f, h - g, up - h, far - up)
            upper.append(one)
            lower.append(two)
        return (upper, lower)

    for k, value in enumerate(cell_edges(-1)[0]):
        xr[k] = value
    for k in range(8):
        flux_prev[k] = jnp.zeros((8, 128), jnp.float32)
    for k in range(7):
        acc[k, 0] = jnp.zeros((8, 128), jnp.float32)

    def face(j, _):
        upper, lower = cell_edges(j)
        before = all_of(xr)
        for k in range(7):
            xr[k] = upper[k]
        lower_cell = all_of(prim, j + 2)
        flux = fluxes(before, lower, lower_cell, all_of(prim, j + 3), 1)
        change = [flux[k] - flux_prev[k] for k in range(8)]
        for k in range(8):
            flux_prev[k] = flux[k]
        for k, value in enumerate(folded(change, lower_cell[6])):
            acc[k, j] = acc[k, j] + value
        return 0

    lax.fori_loop(0, 9, face, 0)

    copies[2].wait_recv()
    pl.when(jnp.logical_not(answer_left))(copies[3].wait_recv)

    @pl.when(s == 0)
    def _():
        for k in range(7):
            value = jnp.zeros((8, 128), jnp.float32)
            for layer in range(3):
                for y in range(8):
                    one = jnp.broadcast_to(inflow[k, layer][:, y : y + 1], (8, 128))
                    value = jnp.where((group == y) & (place == 2 + layer), one, value)
            a_left[k] = value

    @pl.when(s == size_s - 1)
    def _():
        for k in range(7):
            value = a_own[k]
            one, two, three = (rolled(value, 1, 1), rolled(value, 2, 1), rolled(value, 3, 1))
            a_right[k] = jnp.where(place == 5, one, jnp.where(place == 6, two, three))

    rim = []
    for k in range(7):
        own = a_own[k]
        late = rolled(jnp.where(place < 5, a_left[k], own), 6, 1)
        rim.append(jnp.where(place < 5, own, jnp.where(place < 8, a_right[k], late)))
    w = primitive(rim)
    keep = ((place >= 3) & (place <= 5)) | ((place >= 11) & (place <= 13))
    ends = folded(spread(along(w, 1, 0), 1, keep), w[6])
    for k in range(7):
        edge[k] = jnp.where(place < 5, ends[k], rolled(ends[k], -6, 1))

    near = (lane >= 125) | (lane <= 2)
    for k in range(7):
        for y in range(8):
            extra = jnp.where(near, rolled(edge[k], 123 - 16 * y, 1), 0.0)
            rate_ref[k, pl.ds(y, 8, stride=8), :] = (acc[k, y + 1] + extra) * (-1.0 / 3.0)

    children = [
        send(
            rows.at[2],
            told.at[0],
            stage_send.at[2],
            stage_recv.at[2],
            (s, (c + k * inner_c) % size_c),
        )
        for k in range(1, planes - roots + 1)
    ]

    for copy in copies:
        copy.wait_send()

    def sent(slots, stage):
        send(slots, slots, stage_send.at[stage], stage_recv.at[stage], right).wait_send()

    @pl.when(is_root)
    def _():
        sent(slots_p, 1)
        if roots > 1:
            sent(slots_z.at[pl.ds(0, roots - 1)], 0)

    @pl.when(jnp.logical_not(is_root))
    def _():
        sent(slots_z.at[pl.ds(0, roots)], 0)

    @pl.when(is_root)
    def _():
        fastest = arrived(slots_p, 1, rows[1])
        rows[2] = fastest
        step_ref[...] = 0.3 / fastest

    @pl.when(plane == roots - 1)
    def _():
        for copy in children:
            copy.start()

    @pl.when(jnp.logical_not(is_root))
    def _():
        children[0].wait_recv()
        step_ref[...] = 0.3 / told[0]

    @pl.when(plane == roots - 1)
    def _():
        sent(slots_z.at[pl.ds(0, planes - roots)], 2)


def shards(sizes, state_now, state_base, inflow):
    size = jnp.float32
    inflow_t = jnp.transpose(inflow, (0, 3, 1, 2))
    part, rate, step = pl.pallas_call(
        functools.partial(kernel, sizes),
        out_shape=(
            jax.ShapeDtypeStruct((7, 8, 8, 128), size),
            jax.ShapeDtypeStruct((7, 64, 128), size),
            jax.ShapeDtypeStruct((1, 128), size),
        ),
        in_specs=[pl.BlockSpec(memory_space=pltpu.HBM)] * 3,
        out_specs=(pl.BlockSpec(memory_space=pltpu.VMEM),) * 3,
        scratch_shapes=[
            pltpu.VMEM((7, 8, 8, 128), size),
            pltpu.VMEM((7, 8, 8, 128), size),
            pltpu.VMEM((7, 8, 8, 128), size),
            pltpu.VMEM((7, 3, 8, 8), size),
            pltpu.VMEM((7, 14, 8, 128), size),
            pltpu.VMEM((7, 8, 128), size),
            pltpu.VMEM((8, 8, 128), size),
            pltpu.VMEM((7, 9, 8, 128), size),
            pltpu.VMEM((7, 8, 128), size),
            pltpu.VMEM((7, 8, 128), size),
            pltpu.VMEM((7, 8, 128), size),
            pltpu.VMEM((7, 8, 128), size),
            pltpu.VMEM((3, 1, 128), size),
            pltpu.VMEM((sizes[3] - 1, 1, 128), size),
            pltpu.VMEM((sizes[0] * sizes[1] * sizes[2] - 1, 1, 128), size),
            pltpu.VMEM((1, 1, 128), size),
            pltpu.SemaphoreType.DMA((3,)),
            pltpu.SemaphoreType.DMA((4,)),
            pltpu.SemaphoreType.DMA((4,)),
            pltpu.SemaphoreType.DMA((3,)),
            pltpu.SemaphoreType.DMA((3,)),
        ],
        compiler_params=pltpu.CompilerParams(
            collective_id=0, has_side_effects=True, vmem_limit_bytes=32 * 1024 * 1024
        ),
    )(
        pltpu.with_memory_space_constraint(state_now, pltpu.HBM),
        pltpu.with_memory_space_constraint(state_base, pltpu.HBM),
        pltpu.with_memory_space_constraint(inflow_t, pltpu.HBM),
    )
    return part + step.reshape(1, 1, 1, 128) * rate.reshape(state_now.shape)


def solution(mesh):
    stream, cross = (mesh.shape["stream"], mesh.shape["cross"])
    sizes = (8, 4, 2, 12) if (stream, cross) == (16, 48) else (2, 2, stream // 2, cross // 2)
    return jax.shard_map(
        functools.partial(shards, sizes),
        mesh=mesh,
        in_specs=(
            P(None, None, "cross", "stream"),
            P(None, None, "cross", "stream"),
            P(None, None, "cross", None),
        ),
        out_specs=P(None, None, "cross", "stream"),
        check_vma=False,
    )
```

```python
import functools

import jax
import jax.numpy as jnp
from jax import lax
from jax.experimental import pallas as pl
from jax.experimental.pallas import tpu as pltpu
from jax.sharding import PartitionSpec as P

MESH = pl.DeviceIdType.MESH

gas_part = 1.0 / 0.4
liquid_part = 1.0 / 3.4
stiff_part = 4.4 * 0.6 / 3.4


def inverse(value):
    guess = pl.reciprocal(value, approx=True)
    return guess * (2.0 - value * guess)


def mixture(volume):
    rest = 1.0 - volume
    return (volume * gas_part + rest * liquid_part, rest * stiff_part)


def primitive(u):
    over = 1.0 / (u[0] + u[1])
    vx, vy, vz = (u[2] * over, u[3] * over, u[4] * over)
    kinetic = 0.5 * (u[2] * vx + u[3] * vy + u[4] * vz)
    gamma, stiff = mixture(u[6])
    return (u[0], u[1], vx, vy, vz, (u[5] - kinetic - stiff) / gamma, u[6])


def sound(density, pressure, gamma, stiff):
    return jnp.sqrt(((gamma + 1.0) * pressure + stiff) / (gamma * density))


def edges(h, d1, d2, d3, d4):
    e1, e2, e3 = (d2 - d1, d3 - d2, d4 - d3)
    u0 = e1 + d2 + d2
    u1 = d2 + d3
    u2 = e3 - d3 - d3
    third = 13.0 / 3.0
    top = 1e30
    s0 = jnp.minimum(third * (e1 * e1) + u0 * u0 + 4e-6, top)
    s1 = jnp.minimum(third * (e2 * e2) + u1 * u1 + 4e-6, top)
    s2 = jnp.minimum(third * (e3 * e3) + u2 * u2 + 4e-6, top)
    r0, r1, r2 = (inverse(s0), inverse(s1), inverse(s2))
    a0, a1, a2 = (r0 * r0, 6.0 * (r1 * r1), r2 * r2)
    b0, b2 = (3.0 * a0, 3.0 * a2)
    up = a0 * (u0 + e1 + d2) + a1 * (u1 + d3) + b2 * (d3 - u2)
    down = a2 * (u2 + e3 - d3) - a1 * (u1 + d2) - b0 * (u0 + d2)
    upper = h + up * inverse(6.0 * (a0 + a1 + b2))
    lower = h + down * inverse(6.0 * (a2 + a1 + b0))
    return (upper, lower)


def limited(face, lower_cell, upper_cell):
    out = []
    for c in range(7):
        value = face[c]
        if c in (0, 1, 5):
            value = jnp.maximum(value, 0.5 * jnp.minimum(lower_cell[c], upper_cell[c]))
        elif c == 6:
            value = jnp.maximum(value, 0.5 * jnp.minimum(lower_cell[c], upper_cell[c]))
            value = jnp.minimum(value, 0.5 + 0.5 * jnp.maximum(lower_cell[c], upper_cell[c]))
        out.append(value)
    return out


def side(w, normal):
    density = w[0] + w[1]
    gamma, stiff = mixture(w[6])
    momentum = [density * w[2], density * w[3], density * w[4]]
    energy = (
        gamma * w[5]
        + stiff
        + 0.5 * (momentum[0] * w[2] + momentum[1] * w[3] + momentum[2] * w[4])
    )
    vn = w[2 + normal]
    amounts = [w[0], w[1], *momentum, energy, w[6]]
    moved = [amount * vn for amount in amounts]
    moved[2 + normal] = moved[2 + normal] + w[5]
    moved[5] = moved[5] + w[5] * vn
    signal = jnp.abs(vn) + sound(density, w[5], gamma, stiff)
    return (amounts, moved, vn, signal)


def fluxes(left, right, lower_cell, upper_cell, normal):
    one = side(limited(left, lower_cell, upper_cell), normal)
    two = side(limited(right, lower_cell, upper_cell), normal)
    fastest = jnp.maximum(one[3], two[3])
    out = [
        (fl + fr) - fastest * (ur - ul)
        for ul, ur, fl, fr in zip(one[0], two[0], one[1], two[1])
    ]
    return out + [one[2] + two[2]]


def rolled(value, shift, axis):
    return pltpu.roll(value, shift % value.shape[axis], axis)


def along(w, axis, normal):
    upper, lower, before = ([], [], [])
    for c in range(7):
        h = w[c]
        g = rolled(h, 1, axis)
        d2 = h - g
        d1, d3, d4 = (rolled(d2, 1, axis), rolled(d2, -1, axis), rolled(d2, -2, axis))
        up, down = edges(h, d1, d2, d3, d4)
        upper.append(rolled(up, 1, axis))
        lower.append(down)
        before.append(g)
    return fluxes(upper, lower, before, w, normal)


def spread(flux, axis, keep=None):
    if keep is not None:
        flux = [jnp.where(keep, f, 0.0) for f in flux]
    return [rolled(f, -1, axis) - f for f in flux]


def folded(change, volume):
    return change[:6] + [change[6] - volume * change[7]]


def in_plane(sizes):
    inner_s, inner_c, outer_s, _ = sizes
    s, c = (lax.axis_index("stream"), lax.axis_index("cross"))
    length = outer_s * inner_c
    x, y = (s % inner_s, s // inner_s * inner_c + c % inner_c)
    offsets = [(i, j) for i in range(inner_s) for j in range(length) if i or j]

    def distance(offset):
        i, j = offset
        return min(i, inner_s - i) / 2 + min(j, length - j)

    there = []
    for i, j in sorted(offsets, key=lambda offset: -distance(offset)):
        y_there = (y + j) % length
        there.append(
            (
                y_there // inner_c * inner_s + (x + i) % inner_s,
                c // inner_c * inner_c + y_there % inner_c,
            )
        )
    return there


def core_mate(s):
    return s // 2 * 2 + 1 - s % 2


def along_z(sizes):
    _, inner_c, _, planes = sizes
    s, c = (lax.axis_index("stream"), lax.axis_index("cross"))
    offsets = sorted(range(1, planes), key=lambda k: -min(k, planes - k))
    return [(core_mate(s), (c + k * inner_c) % (planes * inner_c)) for k in offsets]


def send(source, target, send_sem, recv_sem, to):
    return pltpu.make_async_remote_copy(
        src_ref=source,
        dst_ref=target,
        send_sem=send_sem,
        recv_sem=recv_sem,
        device_id=to,
        device_id_type=MESH,
    )


def kernel(
    sizes,
    now_ref,
    base_ref,
    inflow_ref,
    part_ref,
    rate_ref,
    step_ref,
    now,
    base,
    halo,
    inflow,
    prim,
    xr,
    flux_prev,
    acc,
    a_own,
    a_left,
    a_right,
    edge,
    rows,
    slots_z,
    slots_p,
    told,
    in_sems,
    halo_send,
    halo_recv,
    stage_send,
    stage_recv,
):
    load_base = pltpu.make_async_copy(base_ref, base, in_sems.at[0])
    load_now = pltpu.make_async_copy(now_ref, now, in_sems.at[1])
    load_inflow = pltpu.make_async_copy(inflow_ref, inflow, in_sems.at[2])
    load_base.start()
    load_now.start()
    load_inflow.start()

    size_s, size_c = (sizes[0] * sizes[2], sizes[1] * sizes[3])
    s, c = (lax.axis_index("stream"), lax.axis_index("cross"))
    left, right = (((s + size_s - 1) % size_s, c), ((s + 1) % size_s, c))
    below, above = ((s, (c + size_c - 1) % size_c), (s, (c + 1) % size_c))
    inner_c, planes = (sizes[1], sizes[3])
    roots = max(1, planes // 3)
    plane = c // inner_c
    is_root = plane < roots

    barrier = pltpu.get_barrier_semaphore()

    def greet(there):
        pl.semaphore_signal(barrier, inc=1, device_id=there, device_id_type=MESH)

    first_s, last_s = (s % sizes[0] == 0, s % sizes[0] == sizes[0] - 1)
    first_c, last_c = (c % inner_c == 0, c % inner_c == inner_c - 1)
    flip = s // sizes[0] > 0
    answer_left = first_s
    leftmost, rightmost = (s == 0, s == size_s - 1)
    answer_above = last_c & flip & (plane != planes - 1)
    answer_below = first_c & (jnp.logical_not(flip) | (plane == 0))
    pl.when(jnp.logical_not(first_c) | answer_below)(lambda: greet(below))
    pl.when(jnp.logical_not(last_c) | answer_above)(lambda: greet(above))
    pl.when(s > 0)(lambda: greet(left))
    pl.when(jnp.logical_not(last_s))(lambda: greet(right))
    greeted = (
        jnp.where(s < size_s - 1, 1, 0)
        + jnp.where(answer_left, 0, 1)
        + jnp.where(answer_above, 0, 1)
        + jnp.where(answer_below, 0, 1)
    )

    @pl.when(is_root)
    def _():
        for there in along_z(sizes) + in_plane(sizes):
            greet(there)

    now_rows = now.reshape(7, 64, 128)
    halo_rows = halo.reshape(7, 64, 128)

    def across_rows(ref, y):
        return [ref[k, pl.ds(y, 8, stride=8), :] for k in range(7)]

    def all_of(ref, *index):
        return [ref[(k, *index)] for k in range(7)]

    def speed(y, most):
        w = primitive(all_of(base, y))
        gamma, stiff = mixture(w[6])
        swift = jnp.maximum(jnp.maximum(jnp.abs(w[2]), jnp.abs(w[3])), jnp.abs(w[4]))
        return jnp.maximum(most, swift + sound(w[0] + w[1], w[5], gamma, stiff))

    load_base.wait()
    most = jnp.zeros((8, 128), jnp.float32)
    for y in range(8):
        most = speed(y, most)
    rows[0] = jnp.broadcast_to(jnp.max(most, keepdims=True), (1, 128))
    def arrived(slots, stage, own):
        send(slots, slots, stage_send.at[stage], stage_recv.at[stage], right).wait_recv()
        values = [own] + [slots[k] for k in range(slots.shape[0])]
        while len(values) > 1:
            pairs = [jnp.maximum(*values[k : k + 2]) for k in range(0, len(values) - 1, 2)]
            values = pairs + values[2 * len(pairs) :]
        return values[0]

    def to_root(root):
        return send(
            rows.at[0],
            slots_z.at[(root - plane + planes) % planes - 1],
            stage_send.at[0],
            stage_recv.at[0],
            (core_mate(s), root * inner_c + c % inner_c),
        )

    @pl.when(jnp.logical_not(is_root))
    def _():
        pl.semaphore_wait(barrier, greeted + roots)
        for root in range(roots):
            to_root(root).start()

    load_now.wait()
    load_inflow.wait()

    lane = lax.broadcasted_iota(jnp.int32, (8, 128), 1)
    place = lane % 16
    group = lane // 16

    def pack(y, packed):
        packed = list(packed)
        for k, value in enumerate(across_rows(now_rows, y)):
            packed[k] = jnp.where(group == y, pltpu.roll(value, 16 * y + 5, 1), packed[k])
        return tuple(packed)

    packed = (jnp.zeros((8, 128), jnp.float32),) * 7
    for y in range(8):
        packed = pack(y, packed)
    for k in range(7):
        a_own[k] = packed[k]

    copies = [
        send(now.at[:, :, 0:3], halo.at[:, :, 0:3], halo_send.at[0], halo_recv.at[0], below),
        send(now.at[:, :, 5:8], halo.at[:, :, 5:8], halo_send.at[1], halo_recv.at[1], above),
        send(a_own, a_right, halo_send.at[2], halo_recv.at[2], left),
        send(a_own, a_left, halo_send.at[3], halo_recv.at[3], right),
    ]
    def own_prim(y, _):
        for k, value in enumerate(primitive(across_rows(now_rows, y))):
            prim[k, y + 3] = value
        return 0

    def local(y, _):
        w = all_of(prim, y + 3)
        across = folded(spread(along(w, 0, 2), 0), w[6])
        keep = (lane >= 3) & (lane <= 125)
        stream = folded(spread(along(w, 1, 0), 1, keep), w[6])
        for k in range(7):
            acc[k, y + 1] = across[k] + stream[k]
        return 0

    def fixed_part(z, _):
        for k in range(7):
            part_ref[k, z] = base[k, z] * (1.0 / 3.0) + now[k, z] * (2.0 / 3.0)
        return 0

    def at_home():
        lax.fori_loop(0, 8, own_prim, 0)
        lax.fori_loop(0, 8, local, 0)
        lax.fori_loop(0, 8, fixed_part, 0)

    pl.when(is_root)(at_home)

    @pl.when(is_root)
    def _():
        pl.semaphore_wait(barrier, greeted + roots - 1 + slots_p.shape[0])
        for root in range(roots):
            pl.when(plane != root)(to_root(root).start)

    pl.when(jnp.logical_not(rightmost))(copies[3].start)
    pl.when(jnp.logical_not(answer_left))(copies[2].start)
    pl.when(jnp.logical_not(answer_above))(copies[1].start)
    pl.when(jnp.logical_not(answer_below))(copies[0].start)

    pl.when(jnp.logical_not(is_root))(at_home)

    @pl.when(is_root)
    def _():
        rows[1] = arrived(slots_z, 0, rows[0])
        for k, there in enumerate(in_plane(sizes)):
            send(rows.at[1], slots_p.at[k], stage_send.at[1], stage_recv.at[1], there).start()

    @pl.when(answer_below)
    def _():
        copies[1].wait_recv()
        copies[0].start()

    @pl.when(answer_above)
    def _():
        copies[0].wait_recv()
        copies[1].start()

    @pl.when(answer_left & jnp.logical_not(leftmost))
    def _():
        copies[3].wait_recv()
        copies[2].start()

    pl.when(jnp.logical_not(answer_below))(copies[1].wait_recv)
    pl.when(jnp.logical_not(answer_above))(copies[0].wait_recv)

    def halo_prim(i, _):
        row = i + i // 3 * 8
        for k, value in enumerate(primitive(across_rows(halo_rows, (i + 5) % 8))):
            prim[k, row] = value
        return 0

    lax.fori_loop(0, 6, halo_prim, 0)

    def cell_edges(y):
        upper, lower = ([], [])
        for k in range(7):
            f, g, h, up, far = (prim[k, y + i] for i in range(1, 6))
            one, two = edges(h, g - f, h - g, up - h, far - up)
            upper.append(one)
            lower.append(two)
        return (upper, lower)

    for k, value in enumerate(cell_edges(-1)[0]):
        xr[k] = value
    for k in range(8):
        flux_prev[k] = jnp.zeros((8, 128), jnp.float32)
    for k in range(7):
        acc[k, 0] = jnp.zeros((8, 128), jnp.float32)

    def face(j, _):
        upper, lower = cell_edges(j)
        before = all_of(xr)
        for k in range(7):
            xr[k] = upper[k]
        lower_cell = all_of(prim, j + 2)
        flux = fluxes(before, lower, lower_cell, all_of(prim, j + 3), 1)
        change = [flux[k] - flux_prev[k] for k in range(8)]
        for k in range(8):
            flux_prev[k] = flux[k]
        for k, value in enumerate(folded(change, lower_cell[6])):
            acc[k, j] = acc[k, j] + value
        return 0

    lax.fori_loop(0, 9, face, 0)

    pl.when(jnp.logical_not(rightmost))(copies[2].wait_recv)
    pl.when(jnp.logical_not(answer_left))(copies[3].wait_recv)

    @pl.when(s == 0)
    def _():
        for k in range(7):
            value = jnp.zeros((8, 128), jnp.float32)
            for layer in range(3):
                for y in range(8):
                    one = jnp.broadcast_to(inflow[k, layer][:, y : y + 1], (8, 128))
                    value = jnp.where((group == y) & (place == 2 + layer), one, value)
            a_left[k] = value

    @pl.when(s == size_s - 1)
    def _():
        for k in range(7):
            value = a_own[k]
            one, two, three = (rolled(value, 1, 1), rolled(value, 2, 1), rolled(value, 3, 1))
            a_right[k] = jnp.where(place == 5, one, jnp.where(place == 6, two, three))

    rim = []
    for k in range(7):
        own = a_own[k]
        late = rolled(jnp.where(place < 5, a_left[k], own), 6, 1)
        rim.append(jnp.where(place < 5, own, jnp.where(place < 8, a_right[k], late)))
    w = primitive(rim)
    keep = ((place >= 3) & (place <= 5)) | ((place >= 11) & (place <= 13))
    ends = folded(spread(along(w, 1, 0), 1, keep), w[6])
    for k in range(7):
        edge[k] = jnp.where(place < 5, ends[k], rolled(ends[k], -6, 1))

    near = (lane >= 125) | (lane <= 2)
    for k in range(7):
        for y in range(8):
            extra = jnp.where(near, rolled(edge[k], 123 - 16 * y, 1), 0.0)
            rate_ref[k, pl.ds(y, 8, stride=8), :] = (acc[k, y + 1] + extra) * (-1.0 / 3.0)

    children = [
        send(
            rows.at[2],
            told.at[0],
            stage_send.at[2],
            stage_recv.at[2],
            (core_mate(s), (c + k * inner_c) % size_c),
        )
        for k in range(1, planes - roots + 1)
    ]

    copies[0].wait_send()
    copies[1].wait_send()
    pl.when(jnp.logical_not(leftmost))(copies[2].wait_send)
    pl.when(jnp.logical_not(rightmost))(copies[3].wait_send)

    def sent(slots, stage):
        send(slots, slots, stage_send.at[stage], stage_recv.at[stage], right).wait_send()

    @pl.when(is_root)
    def _():
        sent(slots_p, 1)
        if roots > 1:
            sent(slots_z.at[pl.ds(0, roots - 1)], 0)

    @pl.when(jnp.logical_not(is_root))
    def _():
        sent(slots_z.at[pl.ds(0, roots)], 0)

    @pl.when(is_root)
    def _():
        fastest = arrived(slots_p, 1, rows[1])
        rows[2] = fastest
        step_ref[...] = 0.3 / fastest

    @pl.when(plane == roots - 1)
    def _():
        for copy in children:
            copy.start()

    @pl.when(jnp.logical_not(is_root))
    def _():
        children[0].wait_recv()
        step_ref[...] = 0.3 / told[0]

    @pl.when(plane == roots - 1)
    def _():
        sent(slots_z.at[pl.ds(0, planes - roots)], 2)


def shards(sizes, state_now, state_base, inflow):
    size = jnp.float32
    inflow_t = jnp.transpose(inflow, (0, 3, 1, 2))
    part, rate, step = pl.pallas_call(
        functools.partial(kernel, sizes),
        out_shape=(
            jax.ShapeDtypeStruct((7, 8, 8, 128), size),
            jax.ShapeDtypeStruct((7, 64, 128), size),
            jax.ShapeDtypeStruct((1, 128), size),
        ),
        in_specs=[pl.BlockSpec(memory_space=pltpu.HBM)] * 3,
        out_specs=(pl.BlockSpec(memory_space=pltpu.VMEM),) * 3,
        scratch_shapes=[
            pltpu.VMEM((7, 8, 8, 128), size),
            pltpu.VMEM((7, 8, 8, 128), size),
            pltpu.VMEM((7, 8, 8, 128), size),
            pltpu.VMEM((7, 3, 8, 8), size),
            pltpu.VMEM((7, 14, 8, 128), size),
            pltpu.VMEM((7, 8, 128), size),
            pltpu.VMEM((8, 8, 128), size),
            pltpu.VMEM((7, 9, 8, 128), size),
            pltpu.VMEM((7, 8, 128), size),
            pltpu.VMEM((7, 8, 128), size),
            pltpu.VMEM((7, 8, 128), size),
            pltpu.VMEM((7, 8, 128), size),
            pltpu.VMEM((3, 1, 128), size),
            pltpu.VMEM((sizes[3] - 1, 1, 128), size),
            pltpu.VMEM((sizes[0] * sizes[1] * sizes[2] - 1, 1, 128), size),
            pltpu.VMEM((1, 1, 128), size),
            pltpu.SemaphoreType.DMA((3,)),
            pltpu.SemaphoreType.DMA((4,)),
            pltpu.SemaphoreType.DMA((4,)),
            pltpu.SemaphoreType.DMA((3,)),
            pltpu.SemaphoreType.DMA((3,)),
        ],
        compiler_params=pltpu.CompilerParams(
            collective_id=0, has_side_effects=True, vmem_limit_bytes=32 * 1024 * 1024
        ),
    )(
        pltpu.with_memory_space_constraint(state_now, pltpu.HBM),
        pltpu.with_memory_space_constraint(state_base, pltpu.HBM),
        pltpu.with_memory_space_constraint(inflow_t, pltpu.HBM),
    )
    return part + step.reshape(1, 1, 1, 128) * rate.reshape(state_now.shape)


def solution(mesh):
    stream, cross = (mesh.shape["stream"], mesh.shape["cross"])
    sizes = (8, 4, 2, 12) if (stream, cross) == (16, 48) else (2, 2, stream // 2, cross // 2)
    return jax.shard_map(
        functools.partial(shards, sizes),
        mesh=mesh,
        in_specs=(
            P(None, None, "cross", "stream"),
            P(None, None, "cross", "stream"),
            P(None, None, "cross", None),
        ),
        out_specs=P(None, None, "cross", "stream"),
        check_vma=False,
    )
```

```python
import functools

import jax
import jax.numpy as jnp
from jax import lax
from jax.experimental import pallas as pl
from jax.experimental.pallas import tpu as pltpu
from jax.sharding import PartitionSpec as P

MESH = pl.DeviceIdType.MESH

gas_part = 1.0 / 0.4
liquid_part = 1.0 / 3.4
stiff_part = 4.4 * 0.6 / 3.4


def inverse(value):
    guess = pl.reciprocal(value, approx=True)
    return guess * (2.0 - value * guess)


def mixture(volume):
    rest = 1.0 - volume
    return (volume * gas_part + rest * liquid_part, rest * stiff_part)


def primitive(u):
    over = 1.0 / (u[0] + u[1])
    vx, vy, vz = (u[2] * over, u[3] * over, u[4] * over)
    kinetic = 0.5 * (u[2] * vx + u[3] * vy + u[4] * vz)
    gamma, stiff = mixture(u[6])
    return (u[0], u[1], vx, vy, vz, (u[5] - kinetic - stiff) / gamma, u[6])


def sound(density, pressure, gamma, stiff):
    return jnp.sqrt(((gamma + 1.0) * pressure + stiff) / (gamma * density))


def edges(h, d1, d2, d3, d4):
    e1, e2, e3 = (d2 - d1, d3 - d2, d4 - d3)
    u0 = e1 + d2 + d2
    u1 = d2 + d3
    u2 = e3 - d3 - d3
    third = 13.0 / 3.0
    top = 1e30
    s0 = jnp.minimum(third * (e1 * e1) + u0 * u0 + 4e-6, top)
    s1 = jnp.minimum(third * (e2 * e2) + u1 * u1 + 4e-6, top)
    s2 = jnp.minimum(third * (e3 * e3) + u2 * u2 + 4e-6, top)
    r0, r1, r2 = (inverse(s0), inverse(s1), inverse(s2))
    a0, a1, a2 = (r0 * r0, 6.0 * (r1 * r1), r2 * r2)
    b0, b2 = (3.0 * a0, 3.0 * a2)
    up = a0 * (u0 + e1 + d2) + a1 * (u1 + d3) + b2 * (d3 - u2)
    down = a2 * (u2 + e3 - d3) - a1 * (u1 + d2) - b0 * (u0 + d2)
    upper = h + up * inverse(6.0 * (a0 + a1 + b2))
    lower = h + down * inverse(6.0 * (a2 + a1 + b0))
    return (upper, lower)


def limited(face, lower_cell, upper_cell):
    out = []
    for c in range(7):
        value = face[c]
        if c in (0, 1, 5):
            value = jnp.maximum(value, 0.5 * jnp.minimum(lower_cell[c], upper_cell[c]))
        elif c == 6:
            value = jnp.maximum(value, 0.5 * jnp.minimum(lower_cell[c], upper_cell[c]))
            value = jnp.minimum(value, 0.5 + 0.5 * jnp.maximum(lower_cell[c], upper_cell[c]))
        out.append(value)
    return out


def side(w, normal):
    density = w[0] + w[1]
    gamma, stiff = mixture(w[6])
    momentum = [density * w[2], density * w[3], density * w[4]]
    energy = (
        gamma * w[5]
        + stiff
        + 0.5 * (momentum[0] * w[2] + momentum[1] * w[3] + momentum[2] * w[4])
    )
    vn = w[2 + normal]
    amounts = [w[0], w[1], *momentum, energy, w[6]]
    moved = [amount * vn for amount in amounts]
    moved[2 + normal] = moved[2 + normal] + w[5]
    moved[5] = moved[5] + w[5] * vn
    signal = jnp.abs(vn) + sound(density, w[5], gamma, stiff)
    return (amounts, moved, vn, signal)


def fluxes(left, right, lower_cell, upper_cell, normal):
    one = side(limited(left, lower_cell, upper_cell), normal)
    two = side(limited(right, lower_cell, upper_cell), normal)
    fastest = jnp.maximum(one[3], two[3])
    out = [
        (fl + fr) - fastest * (ur - ul)
        for ul, ur, fl, fr in zip(one[0], two[0], one[1], two[1])
    ]
    return out + [one[2] + two[2]]


def rolled(value, shift, axis):
    return pltpu.roll(value, shift % value.shape[axis], axis)


def along(w, axis, normal):
    upper, lower, before = ([], [], [])
    for c in range(7):
        h = w[c]
        g = rolled(h, 1, axis)
        d2 = h - g
        d1, d3, d4 = (rolled(d2, 1, axis), rolled(d2, -1, axis), rolled(d2, -2, axis))
        up, down = edges(h, d1, d2, d3, d4)
        upper.append(rolled(up, 1, axis))
        lower.append(down)
        before.append(g)
    return fluxes(upper, lower, before, w, normal)


def spread(flux, axis, keep=None):
    if keep is not None:
        flux = [jnp.where(keep, f, 0.0) for f in flux]
    return [rolled(f, -1, axis) - f for f in flux]


def folded(change, volume):
    return change[:6] + [change[6] - volume * change[7]]


def in_plane(sizes):
    inner_s, inner_c, outer_s, _ = sizes
    s, c = (lax.axis_index("stream"), lax.axis_index("cross"))
    length = outer_s * inner_c
    x, y = (s % inner_s, s // inner_s * inner_c + c % inner_c)
    offsets = [(i, j) for i in range(inner_s) for j in range(length) if i or j]

    def distance(offset):
        i, j = offset
        return (min(i, inner_s - i) + 1) // 2 + min(j, length - j)

    there = []
    for i, j in sorted(offsets, key=lambda offset: -distance(offset)):
        y_there = (y + j) % length
        there.append(
            (
                y_there // inner_c * inner_s + (x + i) % inner_s,
                c // inner_c * inner_c + y_there % inner_c,
            )
        )
    return there


def core_mate(s):
    return s // 2 * 2 + 1 - s % 2


def along_z(sizes):
    _, inner_c, _, planes = sizes
    s, c = (lax.axis_index("stream"), lax.axis_index("cross"))
    offsets = sorted(range(1, planes), key=lambda k: -min(k, planes - k))
    return [(core_mate(s), (c + k * inner_c) % (planes * inner_c)) for k in offsets]


def send(source, target, send_sem, recv_sem, to):
    return pltpu.make_async_remote_copy(
        src_ref=source,
        dst_ref=target,
        send_sem=send_sem,
        recv_sem=recv_sem,
        device_id=to,
        device_id_type=MESH,
    )


def kernel(
    sizes,
    now_ref,
    base_ref,
    inflow_ref,
    part_ref,
    rate_ref,
    step_ref,
    now,
    base,
    halo,
    inflow,
    prim,
    xr,
    flux_prev,
    acc,
    a_own,
    a_left,
    a_right,
    edge,
    rows,
    slots_z,
    slots_p,
    told,
    in_sems,
    halo_send,
    halo_recv,
    stage_send,
    stage_recv,
):
    load_base = pltpu.make_async_copy(base_ref, base, in_sems.at[0])
    load_now = pltpu.make_async_copy(now_ref, now, in_sems.at[1])
    load_inflow = pltpu.make_async_copy(inflow_ref, inflow, in_sems.at[2])
    load_base.start()
    load_now.start()
    load_inflow.start()

    size_s, size_c = (sizes[0] * sizes[2], sizes[1] * sizes[3])
    s, c = (lax.axis_index("stream"), lax.axis_index("cross"))
    left, right = (((s + size_s - 1) % size_s, c), ((s + 1) % size_s, c))
    below, above = ((s, (c + size_c - 1) % size_c), (s, (c + 1) % size_c))
    inner_c, planes = (sizes[1], sizes[3])
    roots = max(1, planes // 3)
    plane = c // inner_c
    is_root = plane < roots

    barrier = pltpu.get_barrier_semaphore()

    def greet(there):
        pl.semaphore_signal(barrier, inc=1, device_id=there, device_id_type=MESH)

    first_s, last_s = (s % sizes[0] == 0, s % sizes[0] == sizes[0] - 1)
    first_c, last_c = (c % inner_c == 0, c % inner_c == inner_c - 1)
    flip = s // sizes[0] > 0
    answer_left = first_s
    leftmost, rightmost = (s == 0, s == size_s - 1)
    answer_above = last_c & flip & (plane != planes - 1)
    answer_below = first_c & (jnp.logical_not(flip) | (plane == 0))
    pl.when(jnp.logical_not(first_c) | answer_below)(lambda: greet(below))
    pl.when(jnp.logical_not(last_c) | answer_above)(lambda: greet(above))
    pl.when(s > 0)(lambda: greet(left))
    pl.when(jnp.logical_not(last_s))(lambda: greet(right))
    greeted = (
        jnp.where(s < size_s - 1, 1, 0)
        + jnp.where(answer_left, 0, 1)
        + jnp.where(answer_above, 0, 1)
        + jnp.where(answer_below, 0, 1)
    )

    @pl.when(is_root)
    def _():
        for there in along_z(sizes) + in_plane(sizes):
            greet(there)

    now_rows = now.reshape(7, 64, 128)
    halo_rows = halo.reshape(7, 64, 128)

    def across_rows(ref, y):
        return [ref[k, pl.ds(y, 8, stride=8), :] for k in range(7)]

    def all_of(ref, *index):
        return [ref[(k, *index)] for k in range(7)]

    def speed(y, most):
        w = primitive(all_of(base, y))
        gamma, stiff = mixture(w[6])
        swift = jnp.maximum(jnp.maximum(jnp.abs(w[2]), jnp.abs(w[3])), jnp.abs(w[4]))
        return jnp.maximum(most, swift + sound(w[0] + w[1], w[5], gamma, stiff))

    load_base.wait()
    most = jnp.zeros((8, 128), jnp.float32)
    for y in range(8):
        most = speed(y, most)
    rows[0] = jnp.broadcast_to(jnp.max(most, keepdims=True), (1, 128))
    def arrived(slots, stage, own):
        send(slots, slots, stage_send.at[stage], stage_recv.at[stage], right).wait_recv()
        values = [own] + [slots[k] for k in range(slots.shape[0])]
        while len(values) > 1:
            pairs = [jnp.maximum(*values[k : k + 2]) for k in range(0, len(values) - 1, 2)]
            values = pairs + values[2 * len(pairs) :]
        return values[0]

    def to_root(root):
        return send(
            rows.at[0],
            slots_z.at[(root - plane + planes) % planes - 1],
            stage_send.at[0],
            stage_recv.at[0],
            (core_mate(s), root * inner_c + c % inner_c),
        )

    @pl.when(jnp.logical_not(is_root))
    def _():
        pl.semaphore_wait(barrier, greeted + roots)
        for root in range(roots):
            to_root(root).start()

    load_now.wait()
    load_inflow.wait()

    lane = lax.broadcasted_iota(jnp.int32, (8, 128), 1)
    place = lane % 16
    group = lane // 16

    def pack(y, packed):
        packed = list(packed)
        for k, value in enumerate(across_rows(now_rows, y)):
            packed[k] = jnp.where(group == y, pltpu.roll(value, 16 * y + 5, 1), packed[k])
        return tuple(packed)

    packed = (jnp.zeros((8, 128), jnp.float32),) * 7
    for y in range(8):
        packed = pack(y, packed)
    for k in range(7):
        a_own[k] = packed[k]

    copies = [
        send(now.at[:, :, 0:3], halo.at[:, :, 0:3], halo_send.at[0], halo_recv.at[0], below),
        send(now.at[:, :, 5:8], halo.at[:, :, 5:8], halo_send.at[1], halo_recv.at[1], above),
        send(a_own, a_right, halo_send.at[2], halo_recv.at[2], left),
        send(a_own, a_left, halo_send.at[3], halo_recv.at[3], right),
    ]
    def own_prim(y, _):
        for k, value in enumerate(primitive(across_rows(now_rows, y))):
            prim[k, y + 3] = value
        return 0

    def local(y, _):
        w = all_of(prim, y + 3)
        across = folded(spread(along(w, 0, 2), 0), w[6])
        keep = (lane >= 3) & (lane <= 125)
        stream = folded(spread(along(w, 1, 0), 1, keep), w[6])
        for k in range(7):
            acc[k, y + 1] = across[k] + stream[k]
        return 0

    def fixed_part(z, _):
        for k in range(7):
            part_ref[k, z] = base[k, z] * (1.0 / 3.0) + now[k, z] * (2.0 / 3.0)
        return 0

    def at_home():
        lax.fori_loop(0, 8, own_prim, 0)
        lax.fori_loop(0, 8, local, 0)
        lax.fori_loop(0, 8, fixed_part, 0)

    pl.when(is_root)(at_home)

    @pl.when(is_root)
    def _():
        pl.semaphore_wait(barrier, greeted + roots - 1 + slots_p.shape[0])
        for root in range(roots):
            pl.when(plane != root)(to_root(root).start)

    pl.when(jnp.logical_not(rightmost))(copies[3].start)
    pl.when(jnp.logical_not(answer_left))(copies[2].start)
    pl.when(jnp.logical_not(answer_above))(copies[1].start)
    pl.when(jnp.logical_not(answer_below))(copies[0].start)

    pl.when(jnp.logical_not(is_root))(at_home)

    @pl.when(is_root)
    def _():
        rows[1] = arrived(slots_z, 0, rows[0])
        for k, there in enumerate(in_plane(sizes)):
            send(rows.at[1], slots_p.at[k], stage_send.at[1], stage_recv.at[1], there).start()

    @pl.when(answer_below)
    def _():
        copies[1].wait_recv()
        copies[0].start()

    @pl.when(answer_above)
    def _():
        copies[0].wait_recv()
        copies[1].start()

    @pl.when(answer_left & jnp.logical_not(leftmost))
    def _():
        copies[3].wait_recv()
        copies[2].start()

    pl.when(jnp.logical_not(answer_below))(copies[1].wait_recv)
    pl.when(jnp.logical_not(answer_above))(copies[0].wait_recv)

    def halo_prim(i, _):
        row = i + i // 3 * 8
        for k, value in enumerate(primitive(across_rows(halo_rows, (i + 5) % 8))):
            prim[k, row] = value
        return 0

    lax.fori_loop(0, 6, halo_prim, 0)

    def cell_edges(y):
        upper, lower = ([], [])
        for k in range(7):
            f, g, h, up, far = (prim[k, y + i] for i in range(1, 6))
            one, two = edges(h, g - f, h - g, up - h, far - up)
            upper.append(one)
            lower.append(two)
        return (upper, lower)

    for k, value in enumerate(cell_edges(-1)[0]):
        xr[k] = value
    for k in range(8):
        flux_prev[k] = jnp.zeros((8, 128), jnp.float32)
    for k in range(7):
        acc[k, 0] = jnp.zeros((8, 128), jnp.float32)

    def face(j, _):
        upper, lower = cell_edges(j)
        before = all_of(xr)
        for k in range(7):
            xr[k] = upper[k]
        lower_cell = all_of(prim, j + 2)
        flux = fluxes(before, lower, lower_cell, all_of(prim, j + 3), 1)
        change = [flux[k] - flux_prev[k] for k in range(8)]
        for k in range(8):
            flux_prev[k] = flux[k]
        for k, value in enumerate(folded(change, lower_cell[6])):
            acc[k, j] = acc[k, j] + value
        return 0

    lax.fori_loop(0, 9, face, 0)

    pl.when(jnp.logical_not(rightmost))(copies[2].wait_recv)
    pl.when(jnp.logical_not(answer_left))(copies[3].wait_recv)

    @pl.when(s == 0)
    def _():
        for k in range(7):
            value = jnp.zeros((8, 128), jnp.float32)
            for layer in range(3):
                for y in range(8):
                    one = jnp.broadcast_to(inflow[k, layer][:, y : y + 1], (8, 128))
                    value = jnp.where((group == y) & (place == 2 + layer), one, value)
            a_left[k] = value

    @pl.when(s == size_s - 1)
    def _():
        for k in range(7):
            value = a_own[k]
            one, two, three = (rolled(value, 1, 1), rolled(value, 2, 1), rolled(value, 3, 1))
            a_right[k] = jnp.where(place == 5, one, jnp.where(place == 6, two, three))

    rim = []
    for k in range(7):
        own = a_own[k]
        late = rolled(jnp.where(place < 5, a_left[k], own), 6, 1)
        rim.append(jnp.where(place < 5, own, jnp.where(place < 8, a_right[k], late)))
    w = primitive(rim)
    keep = ((place >= 3) & (place <= 5)) | ((place >= 11) & (place <= 13))
    ends = folded(spread(along(w, 1, 0), 1, keep), w[6])
    for k in range(7):
        edge[k] = jnp.where(place < 5, ends[k], rolled(ends[k], -6, 1))

    near = (lane >= 125) | (lane <= 2)
    for k in range(7):
        for y in range(8):
            extra = jnp.where(near, rolled(edge[k], 123 - 16 * y, 1), 0.0)
            rate_ref[k, pl.ds(y, 8, stride=8), :] = (acc[k, y + 1] + extra) * (-1.0 / 3.0)

    children = [
        send(
            rows.at[2],
            told.at[0],
            stage_send.at[2],
            stage_recv.at[2],
            (core_mate(s), (c + k * inner_c) % size_c),
        )
        for k in range(1, planes - roots + 1)
    ]

    copies[0].wait_send()
    copies[1].wait_send()
    pl.when(jnp.logical_not(leftmost))(copies[2].wait_send)
    pl.when(jnp.logical_not(rightmost))(copies[3].wait_send)

    def sent(slots, stage):
        send(slots, slots, stage_send.at[stage], stage_recv.at[stage], right).wait_send()

    @pl.when(is_root)
    def _():
        sent(slots_p, 1)
        if roots > 1:
            sent(slots_z.at[pl.ds(0, roots - 1)], 0)

    @pl.when(jnp.logical_not(is_root))
    def _():
        sent(slots_z.at[pl.ds(0, roots)], 0)

    @pl.when(is_root)
    def _():
        fastest = arrived(slots_p, 1, rows[1])
        rows[2] = fastest
        step_ref[...] = 0.3 / fastest

    @pl.when(plane == roots - 1)
    def _():
        for copy in children:
            copy.start()

    @pl.when(jnp.logical_not(is_root))
    def _():
        children[0].wait_recv()
        step_ref[...] = 0.3 / told[0]

    @pl.when(plane == roots - 1)
    def _():
        sent(slots_z.at[pl.ds(0, planes - roots)], 2)


def shards(sizes, state_now, state_base, inflow):
    size = jnp.float32
    inflow_t = jnp.transpose(inflow, (0, 3, 1, 2))
    part, rate, step = pl.pallas_call(
        functools.partial(kernel, sizes),
        out_shape=(
            jax.ShapeDtypeStruct((7, 8, 8, 128), size),
            jax.ShapeDtypeStruct((7, 64, 128), size),
            jax.ShapeDtypeStruct((1, 128), size),
        ),
        in_specs=[pl.BlockSpec(memory_space=pltpu.HBM)] * 3,
        out_specs=(pl.BlockSpec(memory_space=pltpu.VMEM),) * 3,
        scratch_shapes=[
            pltpu.VMEM((7, 8, 8, 128), size),
            pltpu.VMEM((7, 8, 8, 128), size),
            pltpu.VMEM((7, 8, 8, 128), size),
            pltpu.VMEM((7, 3, 8, 8), size),
            pltpu.VMEM((7, 14, 8, 128), size),
            pltpu.VMEM((7, 8, 128), size),
            pltpu.VMEM((8, 8, 128), size),
            pltpu.VMEM((7, 9, 8, 128), size),
            pltpu.VMEM((7, 8, 128), size),
            pltpu.VMEM((7, 8, 128), size),
            pltpu.VMEM((7, 8, 128), size),
            pltpu.VMEM((7, 8, 128), size),
            pltpu.VMEM((3, 1, 128), size),
            pltpu.VMEM((sizes[3] - 1, 1, 128), size),
            pltpu.VMEM((sizes[0] * sizes[1] * sizes[2] - 1, 1, 128), size),
            pltpu.VMEM((1, 1, 128), size),
            pltpu.SemaphoreType.DMA((3,)),
            pltpu.SemaphoreType.DMA((4,)),
            pltpu.SemaphoreType.DMA((4,)),
            pltpu.SemaphoreType.DMA((3,)),
            pltpu.SemaphoreType.DMA((3,)),
        ],
        compiler_params=pltpu.CompilerParams(
            collective_id=0, has_side_effects=True, vmem_limit_bytes=32 * 1024 * 1024
        ),
    )(
        pltpu.with_memory_space_constraint(state_now, pltpu.HBM),
        pltpu.with_memory_space_constraint(state_base, pltpu.HBM),
        pltpu.with_memory_space_constraint(inflow_t, pltpu.HBM),
    )
    return part + step.reshape(1, 1, 1, 128) * rate.reshape(state_now.shape)


def solution(mesh):
    stream, cross = (mesh.shape["stream"], mesh.shape["cross"])
    sizes = (8, 4, 2, 12) if (stream, cross) == (16, 48) else (2, 2, stream // 2, cross // 2)
    return jax.shard_map(
        functools.partial(shards, sizes),
        mesh=mesh,
        in_specs=(
            P(None, None, "cross", "stream"),
            P(None, None, "cross", "stream"),
            P(None, None, "cross", None),
        ),
        out_specs=P(None, None, "cross", "stream"),
        check_vma=False,
    )
```

```python
import functools

import jax
import jax.numpy as jnp
from jax import lax
from jax.experimental import pallas as pl
from jax.experimental.pallas import tpu as pltpu
from jax.sharding import PartitionSpec as P

MESH = pl.DeviceIdType.MESH

gas_part = 1.0 / 0.4
liquid_part = 1.0 / 3.4
stiff_part = 4.4 * 0.6 / 3.4


def inverse(value):
    guess = pl.reciprocal(value, approx=True)
    return guess * (2.0 - value * guess)


def mixture(volume):
    rest = 1.0 - volume
    return (volume * gas_part + rest * liquid_part, rest * stiff_part)


def primitive(u):
    over = 1.0 / (u[0] + u[1])
    vx, vy, vz = (u[2] * over, u[3] * over, u[4] * over)
    kinetic = 0.5 * (u[2] * vx + u[3] * vy + u[4] * vz)
    gamma, stiff = mixture(u[6])
    return (u[0], u[1], vx, vy, vz, (u[5] - kinetic - stiff) / gamma, u[6])


def sound(density, pressure, gamma, stiff):
    return jnp.sqrt(((gamma + 1.0) * pressure + stiff) / (gamma * density))


def edges(h, d1, d2, d3, d4):
    e1, e2, e3 = (d2 - d1, d3 - d2, d4 - d3)
    u0 = e1 + d2 + d2
    u1 = d2 + d3
    u2 = e3 - d3 - d3
    third = 13.0 / 3.0
    top = 1e30
    s0 = jnp.minimum(third * (e1 * e1) + u0 * u0 + 4e-6, top)
    s1 = jnp.minimum(third * (e2 * e2) + u1 * u1 + 4e-6, top)
    s2 = jnp.minimum(third * (e3 * e3) + u2 * u2 + 4e-6, top)
    r0, r1, r2 = (inverse(s0), inverse(s1), inverse(s2))
    a0, a1, a2 = (r0 * r0, 6.0 * (r1 * r1), r2 * r2)
    b0, b2 = (3.0 * a0, 3.0 * a2)
    up = a0 * (u0 + e1 + d2) + a1 * (u1 + d3) + b2 * (d3 - u2)
    down = a2 * (u2 + e3 - d3) - a1 * (u1 + d2) - b0 * (u0 + d2)
    upper = h + up * inverse(6.0 * (a0 + a1 + b2))
    lower = h + down * inverse(6.0 * (a2 + a1 + b0))
    return (upper, lower)


def limited(face, lower_cell, upper_cell):
    out = []
    for c in range(7):
        value = face[c]
        if c in (0, 1, 5):
            value = jnp.maximum(value, 0.5 * jnp.minimum(lower_cell[c], upper_cell[c]))
        elif c == 6:
            value = jnp.maximum(value, 0.5 * jnp.minimum(lower_cell[c], upper_cell[c]))
            value = jnp.minimum(value, 0.5 + 0.5 * jnp.maximum(lower_cell[c], upper_cell[c]))
        out.append(value)
    return out


def side(w, normal):
    density = w[0] + w[1]
    gamma, stiff = mixture(w[6])
    momentum = [density * w[2], density * w[3], density * w[4]]
    energy = (
        gamma * w[5]
        + stiff
        + 0.5 * (momentum[0] * w[2] + momentum[1] * w[3] + momentum[2] * w[4])
    )
    vn = w[2 + normal]
    amounts = [w[0], w[1], *momentum, energy, w[6]]
    moved = [amount * vn for amount in amounts]
    moved[2 + normal] = moved[2 + normal] + w[5]
    moved[5] = moved[5] + w[5] * vn
    signal = jnp.abs(vn) + sound(density, w[5], gamma, stiff)
    return (amounts, moved, vn, signal)


def fluxes(left, right, lower_cell, upper_cell, normal):
    one = side(limited(left, lower_cell, upper_cell), normal)
    two = side(limited(right, lower_cell, upper_cell), normal)
    fastest = jnp.maximum(one[3], two[3])
    out = [
        (fl + fr) - fastest * (ur - ul)
        for ul, ur, fl, fr in zip(one[0], two[0], one[1], two[1])
    ]
    return out + [one[2] + two[2]]


def rolled(value, shift, axis):
    return pltpu.roll(value, shift % value.shape[axis], axis)


def along(w, axis, normal):
    upper, lower, before = ([], [], [])
    for c in range(7):
        h = w[c]
        g = rolled(h, 1, axis)
        d2 = h - g
        d1, d3, d4 = (rolled(d2, 1, axis), rolled(d2, -1, axis), rolled(d2, -2, axis))
        up, down = edges(h, d1, d2, d3, d4)
        upper.append(rolled(up, 1, axis))
        lower.append(down)
        before.append(g)
    return fluxes(upper, lower, before, w, normal)


def spread(flux, axis, keep=None):
    if keep is not None:
        flux = [jnp.where(keep, f, 0.0) for f in flux]
    return [rolled(f, -1, axis) - f for f in flux]


def folded(change, volume):
    return change[:6] + [change[6] - volume * change[7]]


def in_plane(sizes):
    inner_s, inner_c, outer_s, _ = sizes
    s, c = (lax.axis_index("stream"), lax.axis_index("cross"))
    length = outer_s * inner_c
    x, y = (s % inner_s, s // inner_s * inner_c + c % inner_c)
    offsets = [(i, j) for i in range(inner_s) for j in range(length) if i or j]

    def distance(offset):
        i, j = offset
        return (min(i, inner_s - i) + 1) // 2 + min(j, length - j)

    there = []
    for i, j in sorted(offsets, key=lambda offset: -distance(offset)):
        y_there = (y + j) % length
        there.append(
            (
                y_there // inner_c * inner_s + (x + i) % inner_s,
                c // inner_c * inner_c + y_there % inner_c,
            )
        )
    return there


def core_mate(s):
    return s // 2 * 2 + 1 - s % 2


def along_z(sizes):
    _, inner_c, _, planes = sizes
    s, c = (lax.axis_index("stream"), lax.axis_index("cross"))
    offsets = sorted(range(1, planes), key=lambda k: -min(k, planes - k))
    return [(core_mate(s), (c + k * inner_c) % (planes * inner_c)) for k in offsets]


def send(source, target, send_sem, recv_sem, to):
    return pltpu.make_async_remote_copy(
        src_ref=source,
        dst_ref=target,
        send_sem=send_sem,
        recv_sem=recv_sem,
        device_id=to,
        device_id_type=MESH,
    )


def kernel(
    sizes,
    now_ref,
    base_ref,
    inflow_ref,
    part_ref,
    rate_ref,
    step_ref,
    now,
    base,
    halo,
    inflow,
    prim,
    xr,
    flux_prev,
    acc,
    a_own,
    a_left,
    a_right,
    edge,
    rows,
    slots_z,
    slots_p,
    told,
    in_sems,
    halo_send,
    halo_recv,
    stage_send,
    stage_recv,
):
    load_base = pltpu.make_async_copy(base_ref, base, in_sems.at[0])
    load_now = pltpu.make_async_copy(now_ref, now, in_sems.at[1])
    load_inflow = pltpu.make_async_copy(inflow_ref, inflow, in_sems.at[2])
    load_base.start()

    size_s, size_c = (sizes[0] * sizes[2], sizes[1] * sizes[3])
    s, c = (lax.axis_index("stream"), lax.axis_index("cross"))
    left, right = (((s + size_s - 1) % size_s, c), ((s + 1) % size_s, c))
    below, above = ((s, (c + size_c - 1) % size_c), (s, (c + 1) % size_c))
    inner_c, planes = (sizes[1], sizes[3])
    roots = max(1, planes // 3)
    plane = c // inner_c
    is_root = plane < roots

    barrier = pltpu.get_barrier_semaphore()

    def greet(there):
        pl.semaphore_signal(barrier, inc=1, device_id=there, device_id_type=MESH)

    first_s, last_s = (s % sizes[0] == 0, s % sizes[0] == sizes[0] - 1)
    first_c, last_c = (c % inner_c == 0, c % inner_c == inner_c - 1)
    flip = s // sizes[0] > 0
    answer_left = first_s
    leftmost, rightmost = (s == 0, s == size_s - 1)
    answer_above = last_c & flip & (plane != planes - 1)
    answer_below = first_c & (jnp.logical_not(flip) | (plane == 0))
    pl.when(jnp.logical_not(first_c) | answer_below)(lambda: greet(below))
    pl.when(jnp.logical_not(last_c) | answer_above)(lambda: greet(above))
    pl.when(s > 0)(lambda: greet(left))
    pl.when(jnp.logical_not(last_s))(lambda: greet(right))
    greeted = (
        jnp.where(s < size_s - 1, 1, 0)
        + jnp.where(answer_left, 0, 1)
        + jnp.where(answer_above, 0, 1)
        + jnp.where(answer_below, 0, 1)
    )

    @pl.when(is_root)
    def _():
        for there in along_z(sizes) + in_plane(sizes):
            greet(there)

    now_rows = now.reshape(7, 64, 128)
    halo_rows = halo.reshape(7, 64, 128)

    def across_rows(ref, y):
        return [ref[k, pl.ds(y, 8, stride=8), :] for k in range(7)]

    def all_of(ref, *index):
        return [ref[(k, *index)] for k in range(7)]

    def speed(y, most):
        w = primitive(all_of(base, y))
        gamma, stiff = mixture(w[6])
        swift = jnp.maximum(jnp.maximum(jnp.abs(w[2]), jnp.abs(w[3])), jnp.abs(w[4]))
        return jnp.maximum(most, swift + sound(w[0] + w[1], w[5], gamma, stiff))

    load_base.wait()
    load_now.start()
    load_inflow.start()
    most = jnp.zeros((8, 128), jnp.float32)
    for y in range(8):
        most = speed(y, most)
    rows[0] = jnp.broadcast_to(jnp.max(most, keepdims=True), (1, 128))
    def arrived(slots, stage, own):
        send(slots, slots, stage_send.at[stage], stage_recv.at[stage], right).wait_recv()
        values = [own] + [slots[k] for k in range(slots.shape[0])]
        while len(values) > 1:
            pairs = [jnp.maximum(*values[k : k + 2]) for k in range(0, len(values) - 1, 2)]
            values = pairs + values[2 * len(pairs) :]
        return values[0]

    def to_root(root):
        return send(
            rows.at[0],
            slots_z.at[(root - plane + planes) % planes - 1],
            stage_send.at[0],
            stage_recv.at[0],
            (core_mate(s), root * inner_c + c % inner_c),
        )

    @pl.when(jnp.logical_not(is_root))
    def _():
        pl.semaphore_wait(barrier, greeted + roots)
        for root in range(roots):
            to_root(root).start()

    load_now.wait()
    load_inflow.wait()

    lane = lax.broadcasted_iota(jnp.int32, (8, 128), 1)
    place = lane % 16
    group = lane // 16

    def pack(y, packed):
        packed = list(packed)
        for k, value in enumerate(across_rows(now_rows, y)):
            packed[k] = jnp.where(group == y, pltpu.roll(value, 16 * y + 5, 1), packed[k])
        return tuple(packed)

    packed = (jnp.zeros((8, 128), jnp.float32),) * 7
    for y in range(8):
        packed = pack(y, packed)
    for k in range(7):
        a_own[k] = packed[k]

    copies = [
        send(now.at[:, :, 0:3], halo.at[:, :, 0:3], halo_send.at[0], halo_recv.at[0], below),
        send(now.at[:, :, 5:8], halo.at[:, :, 5:8], halo_send.at[1], halo_recv.at[1], above),
        send(a_own, a_right, halo_send.at[2], halo_recv.at[2], left),
        send(a_own, a_left, halo_send.at[3], halo_recv.at[3], right),
    ]
    def own_prim(y, _):
        for k, value in enumerate(primitive(across_rows(now_rows, y))):
            prim[k, y + 3] = value
        return 0

    def local(y, _):
        w = all_of(prim, y + 3)
        across = folded(spread(along(w, 0, 2), 0), w[6])
        keep = (lane >= 3) & (lane <= 125)
        stream = folded(spread(along(w, 1, 0), 1, keep), w[6])
        for k in range(7):
            acc[k, y + 1] = across[k] + stream[k]
        return 0

    def fixed_part(z, _):
        for k in range(7):
            part_ref[k, z] = base[k, z] * (1.0 / 3.0) + now[k, z] * (2.0 / 3.0)
        return 0

    def at_home():
        lax.fori_loop(0, 8, own_prim, 0)
        lax.fori_loop(0, 8, local, 0)
        lax.fori_loop(0, 8, fixed_part, 0)

    pl.when(is_root)(at_home)

    @pl.when(is_root)
    def _():
        pl.semaphore_wait(barrier, greeted + roots - 1 + slots_p.shape[0])
        for root in range(roots):
            pl.when(plane != root)(to_root(root).start)

    pl.when(jnp.logical_not(rightmost))(copies[3].start)
    pl.when(jnp.logical_not(answer_left))(copies[2].start)
    pl.when(jnp.logical_not(answer_above))(copies[1].start)
    pl.when(jnp.logical_not(answer_below))(copies[0].start)

    pl.when(jnp.logical_not(is_root))(at_home)

    @pl.when(is_root)
    def _():
        rows[1] = arrived(slots_z, 0, rows[0])
        for k, there in enumerate(in_plane(sizes)):
            send(rows.at[1], slots_p.at[k], stage_send.at[1], stage_recv.at[1], there).start()

    @pl.when(answer_below)
    def _():
        copies[1].wait_recv()
        copies[0].start()

    @pl.when(answer_above)
    def _():
        copies[0].wait_recv()
        copies[1].start()

    @pl.when(answer_left & jnp.logical_not(leftmost))
    def _():
        copies[3].wait_recv()
        copies[2].start()

    pl.when(jnp.logical_not(answer_below))(copies[1].wait_recv)
    pl.when(jnp.logical_not(answer_above))(copies[0].wait_recv)

    def halo_prim(i, _):
        row = i + i // 3 * 8
        for k, value in enumerate(primitive(across_rows(halo_rows, (i + 5) % 8))):
            prim[k, row] = value
        return 0

    lax.fori_loop(0, 6, halo_prim, 0)

    def cell_edges(y):
        upper, lower = ([], [])
        for k in range(7):
            f, g, h, up, far = (prim[k, y + i] for i in range(1, 6))
            one, two = edges(h, g - f, h - g, up - h, far - up)
            upper.append(one)
            lower.append(two)
        return (upper, lower)

    for k, value in enumerate(cell_edges(-1)[0]):
        xr[k] = value
    for k in range(8):
        flux_prev[k] = jnp.zeros((8, 128), jnp.float32)
    for k in range(7):
        acc[k, 0] = jnp.zeros((8, 128), jnp.float32)

    def face(j, _):
        upper, lower = cell_edges(j)
        before = all_of(xr)
        for k in range(7):
            xr[k] = upper[k]
        lower_cell = all_of(prim, j + 2)
        flux = fluxes(before, lower, lower_cell, all_of(prim, j + 3), 1)
        change = [flux[k] - flux_prev[k] for k in range(8)]
        for k in range(8):
            flux_prev[k] = flux[k]
        for k, value in enumerate(folded(change, lower_cell[6])):
            acc[k, j] = acc[k, j] + value
        return 0

    lax.fori_loop(0, 9, face, 0)

    pl.when(jnp.logical_not(rightmost))(copies[2].wait_recv)
    pl.when(jnp.logical_not(answer_left))(copies[3].wait_recv)

    @pl.when(s == 0)
    def _():
        for k in range(7):
            value = jnp.zeros((8, 128), jnp.float32)
            for layer in range(3):
                for y in range(8):
                    one = jnp.broadcast_to(inflow[k, layer][:, y : y + 1], (8, 128))
                    value = jnp.where((group == y) & (place == 2 + layer), one, value)
            a_left[k] = value

    @pl.when(s == size_s - 1)
    def _():
        for k in range(7):
            value = a_own[k]
            one, two, three = (rolled(value, 1, 1), rolled(value, 2, 1), rolled(value, 3, 1))
            a_right[k] = jnp.where(place == 5, one, jnp.where(place == 6, two, three))

    rim = []
    for k in range(7):
        own = a_own[k]
        late = rolled(jnp.where(place < 5, a_left[k], own), 6, 1)
        rim.append(jnp.where(place < 5, own, jnp.where(place < 8, a_right[k], late)))
    w = primitive(rim)
    keep = ((place >= 3) & (place <= 5)) | ((place >= 11) & (place <= 13))
    ends = folded(spread(along(w, 1, 0), 1, keep), w[6])
    for k in range(7):
        edge[k] = jnp.where(place < 5, ends[k], rolled(ends[k], -6, 1))

    near = (lane >= 125) | (lane <= 2)
    for k in range(7):
        for y in range(8):
            extra = jnp.where(near, rolled(edge[k], 123 - 16 * y, 1), 0.0)
            rate_ref[k, pl.ds(y, 8, stride=8), :] = (acc[k, y + 1] + extra) * (-1.0 / 3.0)

    children = [
        send(
            rows.at[2],
            told.at[0],
            stage_send.at[2],
            stage_recv.at[2],
            (core_mate(s), (c + k * inner_c) % size_c),
        )
        for k in range(1, planes - roots + 1)
    ]

    copies[0].wait_send()
    copies[1].wait_send()
    pl.when(jnp.logical_not(leftmost))(copies[2].wait_send)
    pl.when(jnp.logical_not(rightmost))(copies[3].wait_send)

    def sent(slots, stage):
        send(slots, slots, stage_send.at[stage], stage_recv.at[stage], right).wait_send()

    @pl.when(is_root)
    def _():
        sent(slots_p, 1)
        if roots > 1:
            sent(slots_z.at[pl.ds(0, roots - 1)], 0)

    @pl.when(jnp.logical_not(is_root))
    def _():
        sent(slots_z.at[pl.ds(0, roots)], 0)

    @pl.when(is_root)
    def _():
        fastest = arrived(slots_p, 1, rows[1])
        rows[2] = fastest
        step_ref[...] = 0.3 / fastest

    @pl.when(plane == roots - 1)
    def _():
        for copy in children:
            copy.start()

    @pl.when(jnp.logical_not(is_root))
    def _():
        children[0].wait_recv()
        step_ref[...] = 0.3 / told[0]

    @pl.when(plane == roots - 1)
    def _():
        sent(slots_z.at[pl.ds(0, planes - roots)], 2)


def shards(sizes, state_now, state_base, inflow):
    size = jnp.float32
    inflow_t = jnp.transpose(inflow, (0, 3, 1, 2))
    part, rate, step = pl.pallas_call(
        functools.partial(kernel, sizes),
        out_shape=(
            jax.ShapeDtypeStruct((7, 8, 8, 128), size),
            jax.ShapeDtypeStruct((7, 64, 128), size),
            jax.ShapeDtypeStruct((1, 128), size),
        ),
        in_specs=[pl.BlockSpec(memory_space=pltpu.HBM)] * 3,
        out_specs=(pl.BlockSpec(memory_space=pltpu.VMEM),) * 3,
        scratch_shapes=[
            pltpu.VMEM((7, 8, 8, 128), size),
            pltpu.VMEM((7, 8, 8, 128), size),
            pltpu.VMEM((7, 8, 8, 128), size),
            pltpu.VMEM((7, 3, 8, 8), size),
            pltpu.VMEM((7, 14, 8, 128), size),
            pltpu.VMEM((7, 8, 128), size),
            pltpu.VMEM((8, 8, 128), size),
            pltpu.VMEM((7, 9, 8, 128), size),
            pltpu.VMEM((7, 8, 128), size),
            pltpu.VMEM((7, 8, 128), size),
            pltpu.VMEM((7, 8, 128), size),
            pltpu.VMEM((7, 8, 128), size),
            pltpu.VMEM((3, 1, 128), size),
            pltpu.VMEM((sizes[3] - 1, 1, 128), size),
            pltpu.VMEM((sizes[0] * sizes[1] * sizes[2] - 1, 1, 128), size),
            pltpu.VMEM((1, 1, 128), size),
            pltpu.SemaphoreType.DMA((3,)),
            pltpu.SemaphoreType.DMA((4,)),
            pltpu.SemaphoreType.DMA((4,)),
            pltpu.SemaphoreType.DMA((3,)),
            pltpu.SemaphoreType.DMA((3,)),
        ],
        compiler_params=pltpu.CompilerParams(
            collective_id=0, has_side_effects=True, vmem_limit_bytes=32 * 1024 * 1024
        ),
    )(
        pltpu.with_memory_space_constraint(state_now, pltpu.HBM),
        pltpu.with_memory_space_constraint(state_base, pltpu.HBM),
        pltpu.with_memory_space_constraint(inflow_t, pltpu.HBM),
    )
    return part + step.reshape(1, 1, 1, 128) * rate.reshape(state_now.shape)


def solution(mesh):
    stream, cross = (mesh.shape["stream"], mesh.shape["cross"])
    sizes = (8, 4, 2, 12) if (stream, cross) == (16, 48) else (2, 2, stream // 2, cross // 2)
    return jax.shard_map(
        functools.partial(shards, sizes),
        mesh=mesh,
        in_specs=(
            P(None, None, "cross", "stream"),
            P(None, None, "cross", "stream"),
            P(None, None, "cross", None),
        ),
        out_specs=P(None, None, "cross", "stream"),
        check_vma=False,
    )
```

```python
import functools

import jax
import jax.numpy as jnp
from jax import lax
from jax.experimental import pallas as pl
from jax.experimental.pallas import tpu as pltpu
from jax.sharding import PartitionSpec as P

MESH = pl.DeviceIdType.MESH

gas_part = 1.0 / 0.4
liquid_part = 1.0 / 3.4
stiff_part = 4.4 * 0.6 / 3.4


def inverse(value):
    guess = pl.reciprocal(value, approx=True)
    return guess * (2.0 - value * guess)


def mixture(volume):
    rest = 1.0 - volume
    return (volume * gas_part + rest * liquid_part, rest * stiff_part)


def primitive(u):
    over = 1.0 / (u[0] + u[1])
    vx, vy, vz = (u[2] * over, u[3] * over, u[4] * over)
    kinetic = 0.5 * (u[2] * vx + u[3] * vy + u[4] * vz)
    gamma, stiff = mixture(u[6])
    return (u[0], u[1], vx, vy, vz, (u[5] - kinetic - stiff) / gamma, u[6])


def sound(density, pressure, gamma, stiff):
    return jnp.sqrt(((gamma + 1.0) * pressure + stiff) / (gamma * density))


def edges(h, d1, d2, d3, d4):
    e1, e2, e3 = (d2 - d1, d3 - d2, d4 - d3)
    u0 = e1 + d2 + d2
    u1 = d2 + d3
    u2 = e3 - d3 - d3
    third = 13.0 / 3.0
    top = 1e30
    s0 = jnp.minimum(third * (e1 * e1) + u0 * u0 + 4e-6, top)
    s1 = jnp.minimum(third * (e2 * e2) + u1 * u1 + 4e-6, top)
    s2 = jnp.minimum(third * (e3 * e3) + u2 * u2 + 4e-6, top)
    r0, r1, r2 = (inverse(s0), inverse(s1), inverse(s2))
    a0, a1, a2 = (r0 * r0, 6.0 * (r1 * r1), r2 * r2)
    b0, b2 = (3.0 * a0, 3.0 * a2)
    up = a0 * (u0 + e1 + d2) + a1 * (u1 + d3) + b2 * (d3 - u2)
    down = a2 * (u2 + e3 - d3) - a1 * (u1 + d2) - b0 * (u0 + d2)
    upper = h + up * inverse(6.0 * (a0 + a1 + b2))
    lower = h + down * inverse(6.0 * (a2 + a1 + b0))
    return (upper, lower)


def limited(face, lower_cell, upper_cell):
    out = []
    for c in range(7):
        value = face[c]
        if c in (0, 1, 5):
            value = jnp.maximum(value, 0.5 * jnp.minimum(lower_cell[c], upper_cell[c]))
        elif c == 6:
            value = jnp.maximum(value, 0.5 * jnp.minimum(lower_cell[c], upper_cell[c]))
            value = jnp.minimum(value, 0.5 + 0.5 * jnp.maximum(lower_cell[c], upper_cell[c]))
        out.append(value)
    return out


def side(w, normal):
    density = w[0] + w[1]
    gamma, stiff = mixture(w[6])
    momentum = [density * w[2], density * w[3], density * w[4]]
    energy = (
        gamma * w[5]
        + stiff
        + 0.5 * (momentum[0] * w[2] + momentum[1] * w[3] + momentum[2] * w[4])
    )
    vn = w[2 + normal]
    amounts = [w[0], w[1], *momentum, energy, w[6]]
    moved = [amount * vn for amount in amounts]
    moved[2 + normal] = moved[2 + normal] + w[5]
    moved[5] = moved[5] + w[5] * vn
    signal = jnp.abs(vn) + sound(density, w[5], gamma, stiff)
    return (amounts, moved, vn, signal)


def fluxes(left, right, lower_cell, upper_cell, normal):
    one = side(limited(left, lower_cell, upper_cell), normal)
    two = side(limited(right, lower_cell, upper_cell), normal)
    fastest = jnp.maximum(one[3], two[3])
    out = [
        (fl + fr) - fastest * (ur - ul)
        for ul, ur, fl, fr in zip(one[0], two[0], one[1], two[1])
    ]
    return out + [one[2] + two[2]]


def rolled(value, shift, axis):
    return pltpu.roll(value, shift % value.shape[axis], axis)


def along(w, axis, normal):
    upper, lower, before = ([], [], [])
    for c in range(7):
        h = w[c]
        g = rolled(h, 1, axis)
        d2 = h - g
        d1, d3, d4 = (rolled(d2, 1, axis), rolled(d2, -1, axis), rolled(d2, -2, axis))
        up, down = edges(h, d1, d2, d3, d4)
        upper.append(rolled(up, 1, axis))
        lower.append(down)
        before.append(g)
    return fluxes(upper, lower, before, w, normal)


def spread(flux, axis, keep=None):
    if keep is not None:
        flux = [jnp.where(keep, f, 0.0) for f in flux]
    return [rolled(f, -1, axis) - f for f in flux]


def folded(change, volume):
    return change[:6] + [change[6] - volume * change[7]]


def in_plane(sizes):
    inner_s, inner_c, outer_s, _ = sizes
    s, c = (lax.axis_index("stream"), lax.axis_index("cross"))
    length = outer_s * inner_c
    x, y = (s % inner_s, s // inner_s * inner_c + c % inner_c)
    offsets = [(i, j) for i in range(inner_s) for j in range(length) if i or j]

    def distance(offset):
        i, j = offset
        return (min(i, inner_s - i) + 1) // 2 + min(j, length - j)

    there = []
    for i, j in sorted(offsets, key=lambda offset: -distance(offset)):
        y_there = (y + j) % length
        there.append(
            (
                y_there // inner_c * inner_s + (x + i) % inner_s,
                c // inner_c * inner_c + y_there % inner_c,
            )
        )
    return there


def core_mate(s):
    return s // 2 * 2 + 1 - s % 2


def along_z(sizes):
    _, inner_c, _, planes = sizes
    s, c = (lax.axis_index("stream"), lax.axis_index("cross"))
    offsets = sorted(range(1, planes), key=lambda k: -min(k, planes - k))
    return [(core_mate(s), (c + k * inner_c) % (planes * inner_c)) for k in offsets]


def send(source, target, send_sem, recv_sem, to):
    return pltpu.make_async_remote_copy(
        src_ref=source,
        dst_ref=target,
        send_sem=send_sem,
        recv_sem=recv_sem,
        device_id=to,
        device_id_type=MESH,
    )


def kernel(
    sizes,
    now_ref,
    base_ref,
    inflow_ref,
    part_ref,
    rate_ref,
    step_ref,
    now,
    base,
    halo,
    inflow,
    prim,
    xr,
    flux_prev,
    acc,
    a_own,
    a_left,
    a_right,
    edge,
    rows,
    slots_z,
    slots_p,
    told,
    in_sems,
    halo_send,
    halo_recv,
    stage_send,
    stage_recv,
):
    load_base = pltpu.make_async_copy(base_ref, base, in_sems.at[0])
    load_now = pltpu.make_async_copy(now_ref, now, in_sems.at[1])
    load_inflow = pltpu.make_async_copy(inflow_ref, inflow, in_sems.at[2])
    load_base.start()

    size_s, size_c = (sizes[0] * sizes[2], sizes[1] * sizes[3])
    s, c = (lax.axis_index("stream"), lax.axis_index("cross"))
    left, right = (((s + size_s - 1) % size_s, c), ((s + 1) % size_s, c))
    below, above = ((s, (c + size_c - 1) % size_c), (s, (c + 1) % size_c))
    inner_c, planes = (sizes[1], sizes[3])
    roots = max(1, planes // 4)
    plane = c // inner_c
    is_root = plane < roots

    barrier = pltpu.get_barrier_semaphore()

    def greet(there):
        pl.semaphore_signal(barrier, inc=1, device_id=there, device_id_type=MESH)

    first_s, last_s = (s % sizes[0] == 0, s % sizes[0] == sizes[0] - 1)
    first_c, last_c = (c % inner_c == 0, c % inner_c == inner_c - 1)
    flip = s // sizes[0] > 0
    answer_left = first_s
    leftmost, rightmost = (s == 0, s == size_s - 1)
    answer_above = last_c & flip & (plane != planes - 1)
    answer_below = first_c & (jnp.logical_not(flip) | (plane == 0))
    pl.when(jnp.logical_not(first_c) | answer_below)(lambda: greet(below))
    pl.when(jnp.logical_not(last_c) | answer_above)(lambda: greet(above))
    pl.when(s > 0)(lambda: greet(left))
    pl.when(jnp.logical_not(last_s))(lambda: greet(right))
    greeted = (
        jnp.where(s < size_s - 1, 1, 0)
        + jnp.where(answer_left, 0, 1)
        + jnp.where(answer_above, 0, 1)
        + jnp.where(answer_below, 0, 1)
    )

    @pl.when(is_root)
    def _():
        for there in along_z(sizes) + in_plane(sizes):
            greet(there)

    now_rows = now.reshape(7, 64, 128)
    halo_rows = halo.reshape(7, 64, 128)

    def across_rows(ref, y):
        return [ref[k, pl.ds(y, 8, stride=8), :] for k in range(7)]

    def all_of(ref, *index):
        return [ref[(k, *index)] for k in range(7)]

    def speed(y, most):
        w = primitive(all_of(base, y))
        gamma, stiff = mixture(w[6])
        swift = jnp.maximum(jnp.maximum(jnp.abs(w[2]), jnp.abs(w[3])), jnp.abs(w[4]))
        return jnp.maximum(most, swift + sound(w[0] + w[1], w[5], gamma, stiff))

    load_base.wait()
    load_now.start()
    load_inflow.start()
    most = jnp.zeros((8, 128), jnp.float32)
    for y in range(8):
        most = speed(y, most)
    rows[0] = jnp.broadcast_to(jnp.max(most, keepdims=True), (1, 128))
    def arrived(slots, stage, own):
        send(slots, slots, stage_send.at[stage], stage_recv.at[stage], right).wait_recv()
        values = [own] + [slots[k] for k in range(slots.shape[0])]
        while len(values) > 1:
            pairs = [jnp.maximum(*values[k : k + 2]) for k in range(0, len(values) - 1, 2)]
            values = pairs + values[2 * len(pairs) :]
        return values[0]

    def to_root(root):
        return send(
            rows.at[0],
            slots_z.at[(root - plane + planes) % planes - 1],
            stage_send.at[0],
            stage_recv.at[0],
            (core_mate(s), root * inner_c + c % inner_c),
        )

    @pl.when(jnp.logical_not(is_root))
    def _():
        pl.semaphore_wait(barrier, greeted + roots)
        for root in range(roots):
            to_root(root).start()

    load_now.wait()
    load_inflow.wait()

    lane = lax.broadcasted_iota(jnp.int32, (8, 128), 1)
    place = lane % 16
    group = lane // 16

    def pack(y, packed):
        packed = list(packed)
        for k, value in enumerate(across_rows(now_rows, y)):
            packed[k] = jnp.where(group == y, pltpu.roll(value, 16 * y + 5, 1), packed[k])
        return tuple(packed)

    packed = (jnp.zeros((8, 128), jnp.float32),) * 7
    for y in range(8):
        packed = pack(y, packed)
    for k in range(7):
        a_own[k] = packed[k]

    copies = [
        send(now.at[:, :, 0:3], halo.at[:, :, 0:3], halo_send.at[0], halo_recv.at[0], below),
        send(now.at[:, :, 5:8], halo.at[:, :, 5:8], halo_send.at[1], halo_recv.at[1], above),
        send(a_own, a_right, halo_send.at[2], halo_recv.at[2], left),
        send(a_own, a_left, halo_send.at[3], halo_recv.at[3], right),
    ]
    def own_prim(y, _):
        for k, value in enumerate(primitive(across_rows(now_rows, y))):
            prim[k, y + 3] = value
        return 0

    def local(y, _):
        w = all_of(prim, y + 3)
        across = folded(spread(along(w, 0, 2), 0), w[6])
        keep = (lane >= 3) & (lane <= 125)
        stream = folded(spread(along(w, 1, 0), 1, keep), w[6])
        for k in range(7):
            acc[k, y + 1] = across[k] + stream[k]
        return 0

    def fixed_part(z, _):
        for k in range(7):
            part_ref[k, z] = base[k, z] * (1.0 / 3.0) + now[k, z] * (2.0 / 3.0)
        return 0

    def at_home():
        lax.fori_loop(0, 8, own_prim, 0)
        lax.fori_loop(0, 8, local, 0)
        lax.fori_loop(0, 8, fixed_part, 0)

    pl.when(is_root)(at_home)

    @pl.when(is_root)
    def _():
        pl.semaphore_wait(barrier, greeted + roots - 1 + slots_p.shape[0])
        for root in range(roots):
            pl.when(plane != root)(to_root(root).start)

    pl.when(jnp.logical_not(rightmost))(copies[3].start)
    pl.when(jnp.logical_not(answer_left))(copies[2].start)
    pl.when(jnp.logical_not(answer_above))(copies[1].start)
    pl.when(jnp.logical_not(answer_below))(copies[0].start)

    pl.when(jnp.logical_not(is_root))(at_home)

    @pl.when(is_root)
    def _():
        rows[1] = arrived(slots_z, 0, rows[0])
        for k, there in enumerate(in_plane(sizes)):
            send(rows.at[1], slots_p.at[k], stage_send.at[1], stage_recv.at[1], there).start()

    @pl.when(answer_below)
    def _():
        copies[1].wait_recv()
        copies[0].start()

    @pl.when(answer_above)
    def _():
        copies[0].wait_recv()
        copies[1].start()

    @pl.when(answer_left & jnp.logical_not(leftmost))
    def _():
        copies[3].wait_recv()
        copies[2].start()

    pl.when(jnp.logical_not(answer_below))(copies[1].wait_recv)
    pl.when(jnp.logical_not(answer_above))(copies[0].wait_recv)

    def halo_prim(i, _):
        row = i + i // 3 * 8
        for k, value in enumerate(primitive(across_rows(halo_rows, (i + 5) % 8))):
            prim[k, row] = value
        return 0

    lax.fori_loop(0, 6, halo_prim, 0)

    def cell_edges(y):
        upper, lower = ([], [])
        for k in range(7):
            f, g, h, up, far = (prim[k, y + i] for i in range(1, 6))
            one, two = edges(h, g - f, h - g, up - h, far - up)
            upper.append(one)
            lower.append(two)
        return (upper, lower)

    for k, value in enumerate(cell_edges(-1)[0]):
        xr[k] = value
    for k in range(8):
        flux_prev[k] = jnp.zeros((8, 128), jnp.float32)
    for k in range(7):
        acc[k, 0] = jnp.zeros((8, 128), jnp.float32)

    def face(j, _):
        upper, lower = cell_edges(j)
        before = all_of(xr)
        for k in range(7):
            xr[k] = upper[k]
        lower_cell = all_of(prim, j + 2)
        flux = fluxes(before, lower, lower_cell, all_of(prim, j + 3), 1)
        change = [flux[k] - flux_prev[k] for k in range(8)]
        for k in range(8):
            flux_prev[k] = flux[k]
        for k, value in enumerate(folded(change, lower_cell[6])):
            acc[k, j] = acc[k, j] + value
        return 0

    lax.fori_loop(0, 9, face, 0)

    pl.when(jnp.logical_not(rightmost))(copies[2].wait_recv)
    pl.when(jnp.logical_not(answer_left))(copies[3].wait_recv)

    @pl.when(s == 0)
    def _():
        for k in range(7):
            value = jnp.zeros((8, 128), jnp.float32)
            for layer in range(3):
                for y in range(8):
                    one = jnp.broadcast_to(inflow[k, layer][:, y : y + 1], (8, 128))
                    value = jnp.where((group == y) & (place == 2 + layer), one, value)
            a_left[k] = value

    @pl.when(s == size_s - 1)
    def _():
        for k in range(7):
            value = a_own[k]
            one, two, three = (rolled(value, 1, 1), rolled(value, 2, 1), rolled(value, 3, 1))
            a_right[k] = jnp.where(place == 5, one, jnp.where(place == 6, two, three))

    rim = []
    for k in range(7):
        own = a_own[k]
        late = rolled(jnp.where(place < 5, a_left[k], own), 6, 1)
        rim.append(jnp.where(place < 5, own, jnp.where(place < 8, a_right[k], late)))
    w = primitive(rim)
    keep = ((place >= 3) & (place <= 5)) | ((place >= 11) & (place <= 13))
    ends = folded(spread(along(w, 1, 0), 1, keep), w[6])
    for k in range(7):
        edge[k] = jnp.where(place < 5, ends[k], rolled(ends[k], -6, 1))

    near = (lane >= 125) | (lane <= 2)
    for k in range(7):
        for y in range(8):
            extra = jnp.where(near, rolled(edge[k], 123 - 16 * y, 1), 0.0)
            rate_ref[k, pl.ds(y, 8, stride=8), :] = (acc[k, y + 1] + extra) * (-1.0 / 3.0)

    children = [
        send(
            rows.at[2],
            told.at[0],
            stage_send.at[2],
            stage_recv.at[2],
            (core_mate(s), (c + k * inner_c) % size_c),
        )
        for k in range(1, planes - roots + 1)
    ]

    copies[0].wait_send()
    copies[1].wait_send()
    pl.when(jnp.logical_not(leftmost))(copies[2].wait_send)
    pl.when(jnp.logical_not(rightmost))(copies[3].wait_send)

    def sent(slots, stage):
        send(slots, slots, stage_send.at[stage], stage_recv.at[stage], right).wait_send()

    @pl.when(is_root)
    def _():
        sent(slots_p, 1)
        if roots > 1:
            sent(slots_z.at[pl.ds(0, roots - 1)], 0)

    @pl.when(jnp.logical_not(is_root))
    def _():
        sent(slots_z.at[pl.ds(0, roots)], 0)

    @pl.when(is_root)
    def _():
        fastest = arrived(slots_p, 1, rows[1])
        rows[2] = fastest
        step_ref[...] = 0.3 / fastest

    @pl.when(plane == roots - 1)
    def _():
        for copy in children:
            copy.start()

    @pl.when(jnp.logical_not(is_root))
    def _():
        children[0].wait_recv()
        step_ref[...] = 0.3 / told[0]

    @pl.when(plane == roots - 1)
    def _():
        sent(slots_z.at[pl.ds(0, planes - roots)], 2)


def shards(sizes, state_now, state_base, inflow):
    size = jnp.float32
    inflow_t = jnp.transpose(inflow, (0, 3, 1, 2))
    part, rate, step = pl.pallas_call(
        functools.partial(kernel, sizes),
        out_shape=(
            jax.ShapeDtypeStruct((7, 8, 8, 128), size),
            jax.ShapeDtypeStruct((7, 64, 128), size),
            jax.ShapeDtypeStruct((1, 128), size),
        ),
        in_specs=[pl.BlockSpec(memory_space=pltpu.HBM)] * 3,
        out_specs=(pl.BlockSpec(memory_space=pltpu.VMEM),) * 3,
        scratch_shapes=[
            pltpu.VMEM((7, 8, 8, 128), size),
            pltpu.VMEM((7, 8, 8, 128), size),
            pltpu.VMEM((7, 8, 8, 128), size),
            pltpu.VMEM((7, 3, 8, 8), size),
            pltpu.VMEM((7, 14, 8, 128), size),
            pltpu.VMEM((7, 8, 128), size),
            pltpu.VMEM((8, 8, 128), size),
            pltpu.VMEM((7, 9, 8, 128), size),
            pltpu.VMEM((7, 8, 128), size),
            pltpu.VMEM((7, 8, 128), size),
            pltpu.VMEM((7, 8, 128), size),
            pltpu.VMEM((7, 8, 128), size),
            pltpu.VMEM((3, 1, 128), size),
            pltpu.VMEM((sizes[3] - 1, 1, 128), size),
            pltpu.VMEM((sizes[0] * sizes[1] * sizes[2] - 1, 1, 128), size),
            pltpu.VMEM((1, 1, 128), size),
            pltpu.SemaphoreType.DMA((3,)),
            pltpu.SemaphoreType.DMA((4,)),
            pltpu.SemaphoreType.DMA((4,)),
            pltpu.SemaphoreType.DMA((3,)),
            pltpu.SemaphoreType.DMA((3,)),
        ],
        compiler_params=pltpu.CompilerParams(
            collective_id=0, has_side_effects=True, vmem_limit_bytes=32 * 1024 * 1024
        ),
    )(
        pltpu.with_memory_space_constraint(state_now, pltpu.HBM),
        pltpu.with_memory_space_constraint(state_base, pltpu.HBM),
        pltpu.with_memory_space_constraint(inflow_t, pltpu.HBM),
    )
    return part + step.reshape(1, 1, 1, 128) * rate.reshape(state_now.shape)


def solution(mesh):
    stream, cross = (mesh.shape["stream"], mesh.shape["cross"])
    sizes = (8, 4, 2, 12) if (stream, cross) == (16, 48) else (2, 2, stream // 2, cross // 2)
    return jax.shard_map(
        functools.partial(shards, sizes),
        mesh=mesh,
        in_specs=(
            P(None, None, "cross", "stream"),
            P(None, None, "cross", "stream"),
            P(None, None, "cross", None),
        ),
        out_specs=P(None, None, "cross", "stream"),
        check_vma=False,
    )
```
